32 devices in a mesh: groups: 2 (over y), ep: 4 (over x, core), tp: 4 (over z).
Axes of the slice: x: 2, y: 2, z: 4, core: 2. Of those that a mesh axis runs over, the one named last changes fastest.
Arguments:
- hidden_in: bfloat16 [32, 4, 3584], P(('groups', 'ep', 'tp')), parts along dimension 0, may hold values from -12 to 12
- queries: bfloat16 [32, 4, 128, 576], P(('groups', 'ep', 'tp')), parts along dimension 0, may hold values from -100 to 100
- kv_cache: bfloat16 [32, 2048, 576], P(('groups', 'ep', 'tp')), parts along dimension 0, may hold values from -6 to 6
- new_kv: bfloat16 [32, 4, 576], P(('groups', 'ep', 'tp')), parts along dimension 0, may hold values from -8 to 8
- lengths: int32 [32], P(('groups', 'ep', 'tp')), parts along dimension 0, may hold values from 128 to 2048, as said below
- expert_ids: int32 [32, 4, 2], P(('groups', 'ep')), parts along dimension 0, may hold values from 0 to 3, all different within a row; in each aligned block of 16 rows (0 to 15, 16 to 31, ..., all dimensions but the last counted through in order) at most 12 rows name the same one
- value_up: bfloat16 [128, 512, 128], P(('ep', 'tp')), may hold values from -3 to 3
- out_proj: bfloat16 [128, 128, 3584], P(('ep', 'tp')), may hold values from -0.046875 to 0.046875
- norm_gain: bfloat16 [3584], replicated, may hold values from 0.099609375 to 1.8984375
- router: bfloat16 [3584, 4], replicated, may hold values from -0.09375 to 0.09375
- expert_in: bfloat16 [4, 2, 3584, 2048], P('ep', None, None, 'tp'), may hold values from -0.09375 to 0.09375
- expert_out: bfloat16 [4, 2048, 3584], P('ep', 'tp'), may hold values from -0.125 to 0.125
- shared_in: bfloat16 [2, 3584, 1024], P(None, None, 'tp'), may hold values from -0.09375 to 0.09375
- shared_out: bfloat16 [1024, 3584], P('tp'), may hold values from -0.1875 to 0.1875
Outputs:
- layer_out: bfloat16 [32, 4, 3584], P(('groups', 'ep', 'tp')), parts along dimension 0
The draws below stay inside these ranges and needn't reach their ends.
There are 2 independent parts, one for each index of `groups`. The reference program is written for one: setup_inputs(seed, part) draws one part's arguments, and reference() takes and returns one part's arrays. A program takes and returns all parts, laid end to end along the dimension named above; an argument that names none is the same for every part. Nothing has to cross between parts.
Inputs may be any that keep to these rules, and one draw needn't show every extreme that they name: `expert_ids`: each row and step names 2 distinct experts; within the rows of one index of ep, over all 4 steps, no expert is named more than 12 times, and in every draw some expert is named exactly 12 times there. `lengths`: some row uses all 2048 cached positions.
All inputs are finite; a program needn't handle non-finite values.
Results may differ from the reference program's by a relative error of at most 0.014.
Values may be sent and summed in bfloat16 or wider, within the bound.
No kernel may reach another device: no remote copies, remote signals or barrier semaphores. Data moves between devices by JAX's collectives and lax.ppermute only.
A program may use at most 64 MiB of HBM per device.

```python
import math
import jax
import jax.numpy as jnp
import numpy as np
from jax import lax

D = 3584
HEADS = 128
LAT = 512
VHEAD = 128
MOE_FF = 2048
SH_FF = 1024
STEPS = 4
CTX = 2048
KV = 576
EXPERTS = 4
TOP = 2
ROWS_EP = 4
ROWS = 16
CAP = 12


def align_draws(key):
    key_fresh = jax.random.fold_in(key, 11)
    key_query = jax.random.fold_in(key, 13)
    fresh = jax.random.normal(key_fresh, (ROWS, STEPS, KV), jnp.float32)
    query_all = 0.5 * jax.random.normal(key_query, (ROWS, STEPS, HEADS, KV), jnp.float32)
    return (fresh, query_all)


def draw_queries(key, part):
    return align_draws(key)[1].astype(jnp.bfloat16)


def draw_new_kv(key, part):
    return align_draws(key)[0].astype(jnp.bfloat16)


def draw_lengths(key, part):
    key_base = jax.random.fold_in(key, 21)
    key_index = jax.random.fold_in(key, 22)
    base = jax.random.randint(key_base, (ROWS,), CTX // 16, CTX + 1, dtype=jnp.int32)
    longest = jax.random.randint(key_index, (), 0, ROWS, dtype=jnp.int32)
    return base.at[longest].set(CTX).astype(jnp.int32)


def draw_hidden_in(key, part):
    key_columns = jax.random.fold_in(key, 31)
    key_base = jax.random.fold_in(key, 32)
    column_scale = jnp.exp(jax.random.uniform(key_columns, (D,), jnp.float32, 0.0, math.log(10.0)))
    column_scale = column_scale / jnp.sqrt(jnp.mean(column_scale * column_scale))
    base = jax.random.normal(key_base, (ROWS, STEPS, D), jnp.float32)
    return (0.5 * base * column_scale).astype(jnp.bfloat16)


def shard_levels(own_key, extent, shards, low, top_value):
    def one(axis_at, blocks):
        heights = jax.random.uniform(jax.random.fold_in(jax.random.fold_in(own_key, 6), axis_at), (blocks,), jnp.float32, low / len(shards), top_value / len(shards))
        return jnp.repeat(jnp.exp(heights), extent[axis_at] // blocks).reshape((-1,) + (1,) * (len(extent) - axis_at - 1))

    factor_of = one(*shards[0])
    for cut in shards[1:]:
        factor_of = factor_of * one(*cut)
    return factor_of


def assign_block(rng, own, number, rows, count, top, reach, lean):
    sequence = jax.random.permutation(rng, count)
    heavy_load, ordinary = shares(count, rows * top, reach, lean, True), shares(count, rows * top, reach, lean, False)
    places = jnp.arange(count)

    def named(sizes, offset_by):
        used = int((sizes > 0).sum())
        fixed = max(1, used // 4)
        shifted = fixed + (places - fixed + offset_by * (used - fixed)) % max(1, count - fixed)
        return jnp.zeros((count,), jnp.int32).at[sequence[jnp.where(places < fixed, places, shifted)]].set(jnp.asarray(sizes, jnp.int32))

    sizes = jnp.where(number % 4 == 0, named(heavy_load, number // 4), named(ordinary, number - number // 4 - 1))
    mixed = jax.random.permutation(jax.random.fold_in(own, 3), count)
    donor, taker = mixed[0:count // 2 * 2:2], mixed[1:count // 2 * 2:2]
    room = jnp.minimum(sizes[donor] - 1, reach - sizes[taker]) // 2
    room = jnp.where((donor == sequence[0]) | (taker == sequence[0]) | (sizes[taker] == 0), 0, jnp.maximum(room, 0))
    shifted = jax.random.randint(jax.random.fold_in(own, 4), (count // 2,), 0, 1 << 20) % (room + 1)
    sizes = sizes.at[donor].add(-shifted).at[taker].add(shifted)
    items = jnp.searchsorted(jnp.cumsum(sizes), jnp.arange(rows * top), side="right").astype(jnp.int32)
    table = items.reshape(top, rows).T
    table = table[jax.random.permutation(jax.random.fold_in(own, 1), rows)]
    offset_by = jax.random.randint(jax.random.fold_in(own, 2), (rows, 1), 0, top)
    return jnp.take_along_axis(table, (jnp.arange(top)[None, :] + offset_by) % top, axis=1)


def shares(amount, total, most, skew, full):
    portions = [(1 << 20) // math.isqrt(rank ** skew) + 1 for rank in range(1, amount + 1)]
    largest = most if full else min(most, max(-(-total // amount), total * portions[0] // sum(portions)))
    least = 1 if total - largest >= amount - 1 else 0
    holding, rest = [largest] + [least] * (amount - 1), total - largest - least * (amount - 1)
    while rest > 0:
        movable = [i for i in range(1, amount) if holding[i] < largest] or [i for i in range(1, amount) if holding[i] < most]
        mass, left = sum([portions[i] for i in movable]), rest
        for i in movable:
            extra = min(most - holding[i], max(1, left * portions[i] // mass), rest)
            holding[i] = holding[i] + extra
            rest = rest - extra
    return np.array(holding)


def gaussian(key, dims, spread, bound, split=(), kind=jnp.bfloat16):
    entries = jax.random.normal(key, dims, jnp.float32) * spread
    if len(split) > 0:
        entries = shard_levels(key, dims, split, -0.22, 0.18) * entries
    return jnp.clip(entries, min=-bound, max=bound).astype(kind)


def setup_inputs(seed: int = 0, part: int = 0) -> dict:
    streams_of = jax.random.split(jax.random.key(seed), 15)
    part_keys = jax.random.split(jax.random.fold_in(streams_of[14], part), 15)
    hidden_in = draw_hidden_in(jax.random.fold_in(jax.random.fold_in(streams_of[14], part), 71), part)
    queries = draw_queries(jax.random.fold_in(jax.random.fold_in(streams_of[14], part), 71), part)
    kv_cache = gaussian(part_keys[2], (ROWS, CTX, KV), 1.0, 6.0, ((0, 16),))
    new_kv = draw_new_kv(jax.random.fold_in(jax.random.fold_in(streams_of[14], part), 71), part)
    lengths = draw_lengths(jax.random.fold_in(jax.random.fold_in(streams_of[14], part), 71), part)
    expert_ids_keys = jax.random.split(jax.random.fold_in(part_keys[5], 1), ROWS * STEPS // (ROWS_EP * STEPS))
    expert_ids_turns = jax.random.permutation(jax.random.fold_in(part_keys[5], 3), ROWS * STEPS // (ROWS_EP * STEPS))
    expert_ids = jax.vmap(lambda own, number: assign_block(jax.random.fold_in(part_keys[5], 2), own, number, ROWS_EP * STEPS, EXPERTS, TOP, CAP, 3))(expert_ids_keys, expert_ids_turns).reshape((ROWS, STEPS, TOP))
    value_up = gaussian(streams_of[6], (HEADS, LAT, VHEAD), (max(LAT // 128, 1)) ** -0.5, 3.0, ((0, 16),))
    out_proj = gaussian(streams_of[7], (HEADS, VHEAD, D), (HEADS * VHEAD) ** -0.5, 0.046875, ((0, 16),))
    norm_gain = jnp.clip(1.0 + 0.18 * jax.random.normal(streams_of[8], (D,), jnp.float32), 0.099609375, 1.8984375).astype(jnp.bfloat16)
    router = gaussian(streams_of[9], (D, EXPERTS), D ** -0.5, 0.09375)
    expert_in = gaussian(streams_of[10], (EXPERTS, 2, D, MOE_FF), D ** -0.5, 0.09375, ((0, 4), (3, 4)))
    expert_out = gaussian(streams_of[11], (EXPERTS, MOE_FF, D), MOE_FF ** -0.5, 0.125, ((0, 4), (1, 4)))
    shared_in = gaussian(streams_of[12], (2, D, SH_FF), D ** -0.5, 0.09375, ((2, 4),))
    shared_out = gaussian(streams_of[13], (SH_FF, D), SH_FF ** -0.5, 0.1875, ((0, 4),))
    return {"hidden_in": hidden_in, "queries": queries, "kv_cache": kv_cache, "new_kv": new_kv, "lengths": lengths, "expert_ids": expert_ids, "value_up": value_up, "out_proj": out_proj, "norm_gain": norm_gain, "router": router, "expert_in": expert_in, "expert_out": expert_out, "shared_in": shared_in, "shared_out": shared_out}


score_scale = 192.0 ** (-0.5)
route_scale = 2.5
norm_eps = 1e-06

def attend_row(operands):
    query_row, cache_row, recent_row, length_row = operands
    steps_here, heads_here, kv_width = query_row.shape
    positions = cache_row.shape[0]
    flattened = query_row.reshape(steps_here * heads_here, kv_width)
    cached = jnp.dot(flattened, cache_row.T, preferred_element_type=jnp.float32).reshape(steps_here, heads_here, positions) * score_scale
    recent = jnp.dot(flattened, recent_row.T, preferred_element_type=jnp.float32).reshape(steps_here, heads_here, steps_here) * score_scale
    cache_live = jnp.arange(positions, dtype=jnp.int32) < length_row
    causal = jnp.arange(steps_here, dtype=jnp.int32)[None, :] <= jnp.arange(steps_here, dtype=jnp.int32)[:, None]
    cached = jnp.where(cache_live[None, None, :], cached, -1e+30)
    recent = jnp.where(causal[:, None, :], recent, -1e+30)
    highest = jnp.maximum(cached.max(-1), recent.max(-1))[..., None]
    cached_exp = jnp.exp(cached - highest)
    recent_exp = jnp.exp(recent - highest)
    denominator = cached_exp.sum(-1, keepdims=True) + recent_exp.sum(-1, keepdims=True)
    cached_prob = (cached_exp / denominator).astype(jnp.bfloat16)
    recent_prob = (recent_exp / denominator).astype(jnp.bfloat16)
    combined = jnp.dot(cached_prob.reshape(steps_here * heads_here, positions), cache_row, preferred_element_type=jnp.float32)
    combined = combined + jnp.dot(recent_prob.reshape(steps_here * heads_here, steps_here), recent_row, preferred_element_type=jnp.float32)
    return combined.reshape(steps_here, heads_here, kv_width)[:, :, :LAT].astype(jnp.bfloat16)

def head_values(operands):
    head_latent, head_weight = operands
    return jnp.dot(head_latent, head_weight, preferred_element_type=jnp.float32).astype(jnp.bfloat16)

def reference(hidden_in, queries, kv_cache, new_kv, lengths, expert_ids, value_up, out_proj, norm_gain, router, expert_in, expert_out, shared_in, shared_out):
    latent_out = lax.map(attend_row, (queries, kv_cache, new_kv, lengths))
    latent_heads = jnp.transpose(latent_out, (2, 0, 1, 3)).reshape(HEADS, ROWS * STEPS, LAT)
    values = lax.map(head_values, (latent_heads, value_up))
    flat_values = jnp.transpose(values, (1, 0, 2)).reshape(ROWS * STEPS, HEADS * VHEAD)
    attention = jnp.dot(flat_values, out_proj.reshape(HEADS * VHEAD, D), preferred_element_type=jnp.float32)
    residual = hidden_in.astype(jnp.float32).reshape(ROWS * STEPS, D) + attention
    mean_square = lax.optimization_barrier(jnp.mean(residual * residual, axis=-1, keepdims=True))
    item_rows = (residual * lax.rsqrt(mean_square + norm_eps) * norm_gain.astype(jnp.float32)).astype(jnp.bfloat16)
    affinity = jax.nn.sigmoid(jnp.dot(item_rows, router, preferred_element_type=jnp.float32))
    picked = expert_ids.reshape(ROWS * STEPS, TOP)
    chosen = lax.optimization_barrier(jnp.sum((picked[:, :, None] == jnp.arange(EXPERTS, dtype=jnp.int32)[None, None, :]).astype(jnp.float32), axis=1))
    scored = chosen * affinity
    gate_weight = route_scale * scored / lax.optimization_barrier(jnp.sum(scored, axis=-1, keepdims=True))

    def add_expert(running, operands):
        weight_in, weight_out, item_share = operands
        gate_part = jnp.dot(item_rows, weight_in[0], preferred_element_type=jnp.float32)
        up_part = jnp.dot(item_rows, weight_in[1], preferred_element_type=jnp.float32)
        activated = (jax.nn.silu(gate_part) * up_part).astype(jnp.bfloat16)
        produced = jnp.dot(activated, weight_out, preferred_element_type=jnp.float32)
        return (running + item_share[:, None] * produced, None)
    routed, unused = lax.scan(add_expert, jnp.zeros((ROWS * STEPS, D), jnp.float32), (expert_in, expert_out, gate_weight.T))
    shared_gate = jnp.dot(item_rows, shared_in[0], preferred_element_type=jnp.float32)
    shared_up = jnp.dot(item_rows, shared_in[1], preferred_element_type=jnp.float32)
    shared_act = (jax.nn.silu(shared_gate) * shared_up).astype(jnp.bfloat16)
    shared = jnp.dot(shared_act, shared_out, preferred_element_type=jnp.float32)
    layer_out = (residual + routed + shared).astype(jnp.bfloat16)
    return layer_out.reshape(ROWS, STEPS, D)
```

```python
import jax
import jax.numpy as jnp
from jax import lax
from jax.sharding import Mesh
from jax.sharding import PartitionSpec as P

LAT = 512


score_scale = 192.0 ** (-0.5)
route_scale = 2.5
norm_eps = 1e-06

CHIPS = ("epx", "tp")
ALL = ("epx", "core", "tp")


def attend_block(queries, kv_cache, new_kv, lengths):
    rows_here, steps_here, heads_here, kv_width = queries.shape
    positions = kv_cache.shape[1]
    cached = (
        jnp.einsum("rshk,rck->rshc", queries, kv_cache, preferred_element_type=jnp.float32)
        * score_scale
    )
    recent = (
        jnp.einsum("rshk,rjk->rshj", queries, new_kv, preferred_element_type=jnp.float32)
        * score_scale
    )
    cache_live = lax.broadcasted_iota(jnp.int32, (rows_here, positions), 1) < lengths[:, None]
    causal = lax.broadcasted_iota(jnp.int32, (steps_here, steps_here), 1) <= lax.broadcasted_iota(
        jnp.int32, (steps_here, steps_here), 0
    )
    cached = jnp.where(cache_live[:, None, None, :], cached, -1e30)
    recent = jnp.where(causal[None, :, None, :], recent, -1e30)
    highest = jnp.maximum(cached.max(-1), recent.max(-1))[..., None]
    cached_exp = jnp.exp(cached - highest)
    recent_exp = jnp.exp(recent - highest)
    denominator = cached_exp.sum(-1, keepdims=True) + recent_exp.sum(-1, keepdims=True)
    cached_prob = (cached_exp / denominator).astype(jnp.bfloat16)
    recent_prob = (recent_exp / denominator).astype(jnp.bfloat16)
    combined = jnp.einsum(
        "rshc,rck->rshk", cached_prob, kv_cache, preferred_element_type=jnp.float32
    )
    combined = combined + jnp.einsum(
        "rshj,rjk->rshk", recent_prob, new_kv, preferred_element_type=jnp.float32
    )
    return combined[..., :LAT].astype(jnp.bfloat16)


def swap_cores(x):
    return lax.ppermute(x, "core", [(0, 1), (1, 0)])


def chip_exchange(x):
    return lax.all_to_all(x, CHIPS, split_axis=0, concat_axis=0, tiled=True)


def sum_at_rows(kept, sent, chips):
    half = kept + swap_cores(sent.astype(jnp.bfloat16)).astype(jnp.float32)
    width = half.shape[1]
    parts = chip_exchange(half.astype(jnp.bfloat16).reshape(chips, -1, width))
    return jnp.sum(parts.astype(jnp.float32), axis=0)


def on_device(
    hidden_in,
    queries,
    kv_cache,
    new_kv,
    lengths,
    expert_ids,
    value_up,
    out_proj,
    norm_gain,
    router,
    expert_in,
    expert_out,
    shared_in,
    shared_out,
):
    rows_here, steps_here, model_width = hidden_in.shape
    items = rows_here * steps_here
    columns = lax.axis_size("epx")
    depth = lax.axis_size("tp")
    chips = columns * depth
    core = lax.axis_index("core")
    column = lax.axis_index("epx")
    place = lax.axis_index("tp")
    expert_count = router.shape[1]

    latent_out = attend_block(queries, kv_cache, new_kv, lengths)
    by_head = lax.all_to_all(latent_out, ALL, split_axis=2, concat_axis=0, tiled=True)
    head_vals = jnp.einsum(
        "rshl,hlv->rshv", by_head, value_up, preferred_element_type=jnp.float32
    ).astype(jnp.bfloat16)
    partial = jnp.einsum(
        "rshv,hvd->rsd", head_vals, out_proj, preferred_element_type=jnp.float32
    ).reshape(columns, 2, depth * items, model_width)
    kept = lax.dynamic_index_in_dim(partial, core, 1, keepdims=False)
    sent = lax.dynamic_index_in_dim(partial, 1 - core, 1, keepdims=False)
    attention = sum_at_rows(
        kept.reshape(-1, model_width), sent.reshape(-1, model_width), chips
    )
    residual = hidden_in.reshape(items, model_width).astype(jnp.float32) + attention
    mean_square = jnp.mean(residual * residual, axis=-1, keepdims=True)
    normed = (residual * lax.rsqrt(mean_square + norm_eps) * norm_gain.astype(jnp.float32)).astype(
        jnp.bfloat16
    )
    affinity = jax.nn.sigmoid(jnp.dot(normed, router, preferred_element_type=jnp.float32))
    picked = lax.dynamic_slice_in_dim(expert_ids, place * rows_here, rows_here, 0).reshape(
        items, expert_ids.shape[2]
    )
    expert_iota = lax.broadcasted_iota(jnp.int32, (1, 1, expert_count), 2)
    chosen = jnp.sum((picked[:, :, None] == expert_iota).astype(jnp.float32), axis=1)
    scored = chosen * affinity
    gate_weight = route_scale * scored / jnp.sum(scored, axis=-1, keepdims=True)
    gate_high = gate_weight.astype(jnp.bfloat16)
    gate_low = (gate_weight - gate_high.astype(jnp.float32)).astype(jnp.bfloat16)
    spare = -(2 * expert_count) % 128
    payload = jnp.concatenate(
        [normed, gate_high, gate_low, jnp.zeros((items, spare), jnp.bfloat16)], axis=1
    )
    mine = chip_exchange(jnp.broadcast_to(payload[None], (chips,) + payload.shape)).reshape(
        chips * items, -1
    )
    tokens = jnp.concatenate([mine, swap_cores(mine)], axis=0)
    block_items = tokens[:, :model_width]
    expert_here = column * 2 + core
    gate_pairs = tokens[:, model_width : model_width + 2 * expert_count].astype(jnp.float32)
    gates = gate_pairs[:, :expert_count] + gate_pairs[:, expert_count:]
    gate_here = lax.dynamic_slice_in_dim(gates, expert_here, 1, 1)

    gate_part = jnp.dot(block_items, expert_in[0, 0], preferred_element_type=jnp.float32)
    up_part = jnp.dot(block_items, expert_in[0, 1], preferred_element_type=jnp.float32)
    activated = (jax.nn.silu(gate_part) * up_part).astype(jnp.bfloat16)
    routed = gate_here * jnp.dot(activated, expert_out[0], preferred_element_type=jnp.float32)

    own = lax.dynamic_slice_in_dim(mine, column * depth * items, depth * items, 0)[
        :, :model_width
    ]
    shared_gate = jnp.dot(own, shared_in[0], preferred_element_type=jnp.float32)
    shared_up = jnp.dot(own, shared_in[1], preferred_element_type=jnp.float32)
    shared_act = (jax.nn.silu(shared_gate) * shared_up).astype(jnp.bfloat16)
    shared_part = jnp.dot(shared_act, shared_out, preferred_element_type=jnp.float32)

    kept = routed[: chips * items].reshape(columns, depth * items, model_width)
    at_column = lax.broadcasted_iota(jnp.int32, (columns, 1, 1), 0) == column
    kept = kept + jnp.where(at_column, shared_part[None], 0.0)
    expert_sum = sum_at_rows(
        kept.reshape(-1, model_width), routed[chips * items :], chips
    )
    layer_out = (residual + expert_sum).astype(jnp.bfloat16)
    return layer_out.reshape(rows_here, steps_here, model_width)


def solution(mesh):
    sizes = mesh.shape
    fine = Mesh(
        mesh.devices.reshape(sizes["groups"], sizes["ep"] // 2, 2, sizes["tp"]),
        ("groups", "epx", "core", "tp"),
    )
    ep = ("epx", "core")
    rows = ("groups", "epx", "core", "tp")
    in_specs = (
        P(rows, None, None),
        P(rows, None, None, None),
        P(rows, None, None),
        P(rows, None, None),
        P(rows),
        P(("groups",) + ep, None, None),
        P(ALL, None, None),
        P(ALL, None, None),
        P(),
        P(),
        P(ep, None, None, "tp"),
        P(ep, "tp", None),
        P(None, None, "tp"),
        P("tp", None),
    )
    out_specs = P(rows, None, None)
    return jax.shard_map(
        on_device, mesh=fine, in_specs=in_specs, out_specs=out_specs, check_vma=False
    )
```

```python
import functools

import jax
import jax.numpy as jnp
from jax import lax
from jax.experimental import pallas as pl
from jax.experimental.pallas import tpu as pltpu
from jax.sharding import Mesh
from jax.sharding import PartitionSpec as P

LAT = 512


score_scale = 192.0 ** (-0.5)
log2_e = 1.4426950408889634
route_scale = 2.5
norm_eps = 1e-06

CHIPS = ("epx", "tp")
ALL = ("epx", "core", "tp")
VMEM = pl.BlockSpec(memory_space=pltpu.VMEM)
SMEM = pl.BlockSpec(memory_space=pltpu.SMEM)
ANY = pl.BlockSpec(memory_space=pl.ANY)


def params(mib):
    return pltpu.CompilerParams(vmem_limit_bytes=mib << 20)


def attend_kernel(
    length_ref, q_hbm, kv_hbm, new_ref, out_ref,
    q_t, q_rows, kv_t, new_rows, scores, recent, weights, row_max, sems, *, chunk, block,
):
    steps, width, heads = q_t.shape
    positions = kv_t.shape[1]
    rows = steps * heads
    q_copy = pltpu.make_async_copy(q_hbm, q_t, sems.at[0])
    q_copy.start()
    copies = []
    for c in range(positions // chunk):
        span = pl.ds(c * chunk, chunk)
        copies.append(
            pltpu.make_async_copy(kv_hbm.at[:, span], kv_t.at[:, span], sems.at[1 + c])
        )
        copies[-1].start()
    new_rows[...] = jnp.zeros_like(new_rows)
    new_rows[0:steps, :] = new_ref[...]
    q_copy.wait()
    for s in range(steps):
        q_rows[s * heads : (s + 1) * heads, :] = q_t[s].T
    length = length_ref[0]
    lanes = new_rows.shape[0]
    fresh = lax.dot_general(
        q_rows[...], new_rows[...], (((1,), (1,)), ((), ())),
        preferred_element_type=jnp.float32,
    )
    step_of = lax.broadcasted_iota(jnp.int32, (rows, lanes), 0) // heads
    fresh = jnp.where(
        lax.broadcasted_iota(jnp.int32, (rows, lanes), 1) <= step_of, fresh, -1e30
    )
    recent[...] = fresh
    row_max[...] = fresh
    for c in range(positions // chunk):
        copies[c].wait()
        live = (lax.broadcasted_iota(jnp.int32, (1, chunk), 1) + c * chunk) < length
        for b in range(rows // block):
            span = slice(b * block, (b + 1) * block)
            s = jnp.dot(
                q_rows[span, :], kv_t[:, c * chunk : (c + 1) * chunk],
                preferred_element_type=jnp.float32,
            )
            s = jnp.where(live, s, -1e30)
            scores[span, c * chunk : (c + 1) * chunk] = s
            best = row_max[span, :]
            for j in range(chunk // lanes):
                best = jnp.maximum(best, s[:, j * lanes : (j + 1) * lanes])
            row_max[span, :] = best
    rate = score_scale * log2_e
    per_owner = out_ref.shape[1] // steps
    for b in range(rows // block):
        span = slice(b * block, (b + 1) * block)
        top = jnp.max(row_max[span, :], axis=1, keepdims=True) * rate
        fresh = jnp.exp2(recent[span, :] * rate - top)
        total = fresh
        fresh = fresh.astype(jnp.bfloat16)
        for c in range(positions // chunk):
            e = jnp.exp2(scores[span, c * chunk : (c + 1) * chunk] * rate - top)
            for j in range(chunk // lanes):
                total = total + e[:, j * lanes : (j + 1) * lanes]
            weights[span, c * chunk : (c + 1) * chunk] = e.astype(jnp.bfloat16)
        mixed = lax.dot_general(
            weights[span, :], kv_t[0:LAT, :], (((1,), (1,)), ((), ())),
            preferred_element_type=jnp.float32,
        ) + jnp.dot(fresh, new_rows[:, 0:LAT], preferred_element_type=jnp.float32)
        mixed = mixed / jnp.sum(total, axis=1, keepdims=True)
        for i in range(block // heads):
            s = b * (block // heads) + i
            part = mixed[i * heads : (i + 1) * heads, :]
            out_ref[:, s * per_owner : (s + 1) * per_owner, :] = part.reshape(
                heads // per_owner, per_owner, LAT
            ).astype(jnp.bfloat16)


def attend(queries, kv_cache, new_kv, lengths, owners):
    _, steps, heads, width = queries.shape
    positions = kv_cache.shape[1]
    rows = steps * heads
    chunk = 512
    lanes = 128
    block = 2 * heads
    return pl.pallas_call(
        functools.partial(attend_kernel, chunk=chunk, block=block),
        out_shape=jax.ShapeDtypeStruct((owners, rows // owners, LAT), jnp.bfloat16),
        in_specs=[SMEM, ANY, ANY, VMEM],
        out_specs=VMEM,
        scratch_shapes=[
            pltpu.VMEM((steps, width, heads), jnp.bfloat16),
            pltpu.VMEM((rows, width), jnp.bfloat16),
            pltpu.VMEM((width, positions), jnp.bfloat16),
            pltpu.VMEM((lanes, width), jnp.bfloat16),
            pltpu.VMEM((rows, positions), jnp.float32),
            pltpu.VMEM((rows, lanes), jnp.float32),
            pltpu.VMEM((rows, positions), jnp.bfloat16),
            pltpu.VMEM((rows, lanes), jnp.float32),
            pltpu.SemaphoreType.DMA((1 + positions // chunk,)),
        ],
        compiler_params=params(24),
        name="attend",
    )(
        lengths,
        jnp.swapaxes(queries[0], 1, 2),
        jnp.swapaxes(kv_cache[0], 0, 1),
        new_kv[0],
    )


def project_kernel(
    core_ref, latent_ref, up_ref, down_ref, kept_ref, sent_ref, latents, *, depth, strip
):
    sources, owned, _ = latent_ref.shape
    heads = up_ref.shape[0]
    steps = owned // heads
    items = sources * steps
    core = core_ref[0]
    place = 0
    for side in (core, 1 - core):
        for column in range(sources // (2 * depth)):
            for t in range(depth):
                source = (column * 2 + side) * depth + t
                block = latent_ref[source].astype(jnp.float32)
                for j in range(LAT // 128):
                    latents[j, place * owned : (place + 1) * owned, :] = block[
                        :, j * 128 : (j + 1) * 128
                    ]
                place += 1
    vals = []
    for h in range(heads):
        x = jnp.concatenate(
            [latents[j, pl.ds(h, items, stride=heads), :] for j in range(LAT // 128)], axis=1
        ).astype(jnp.bfloat16)
        vals.append(
            jnp.dot(x, up_ref[h], preferred_element_type=jnp.float32).astype(jnp.bfloat16)
        )
    vals = jnp.concatenate(vals, axis=1)
    width = down_ref.shape[1]
    half = items // 2
    for n in range(width // strip):
        cols = slice(n * strip, (n + 1) * strip)
        part = jnp.dot(vals, down_ref[:, cols], preferred_element_type=jnp.float32)
        kept_ref[:, cols] = part[:half]
        sent_ref[:, cols] = part[half:].astype(jnp.bfloat16)


def project(by_head, value_up, out_proj, core, depth):
    sources, owned, _ = by_head.shape
    heads, _, value_width = value_up.shape
    width = out_proj.shape[2]
    half = sources * owned // heads // 2
    return pl.pallas_call(
        functools.partial(project_kernel, depth=depth, strip=512),
        out_shape=(
            jax.ShapeDtypeStruct((half, width), jnp.float32),
            jax.ShapeDtypeStruct((half, width), jnp.bfloat16),
        ),
        in_specs=[SMEM, VMEM, VMEM, VMEM],
        out_specs=(VMEM, VMEM),
        scratch_shapes=[pltpu.VMEM((LAT // 128, sources * owned, 128), jnp.float32)],
        compiler_params=params(24),
        name="project",
    )(core, by_head, value_up, out_proj.reshape(heads * value_width, width))


def merge_kernel(kept_ref, got_ref, out_ref):
    chips, items, _ = out_ref.shape
    total = kept_ref[...] + got_ref[...].astype(jnp.float32)
    for j in range(chips):
        out_ref[j] = total[j * items : (j + 1) * items, :].astype(jnp.bfloat16)


def merge(kept, got, chips):
    rows, width = kept.shape
    return pl.pallas_call(
        merge_kernel,
        out_shape=jax.ShapeDtypeStruct((chips, rows // chips, width), jnp.bfloat16),
        in_specs=[VMEM, VMEM],
        out_specs=VMEM,
        compiler_params=params(8),
        name="merge",
    )(kept, got)


def norm_kernel(ids_ref, parts_ref, hidden_ref, gain_ref, router_ref, residual_ref, out_ref):
    chips, items, _ = parts_ref.shape
    width = hidden_ref.shape[1]
    experts = router_ref.shape[0]
    spare = out_ref.shape[2] - width
    total = hidden_ref[...].astype(jnp.float32)
    attention = parts_ref[0].astype(jnp.float32)
    for j in range(1, chips):
        attention = attention + parts_ref[j].astype(jnp.float32)
    residual = total + attention
    residual_ref[...] = residual
    square = jnp.mean(residual * residual, axis=1, keepdims=True)
    normed = (residual * lax.rsqrt(square + norm_eps) * gain_ref[...].astype(jnp.float32)).astype(
        jnp.bfloat16
    )
    logits = lax.dot_general(
        normed, router_ref[...], (((1,), (1,)), ((), ())), preferred_element_type=jnp.float32
    )
    affinity = 1.0 / (1.0 + jnp.exp(-logits))
    item = lax.broadcasted_iota(jnp.int32, (items, experts), 0)
    lane = lax.broadcasted_iota(jnp.int32, (items, experts), 1)
    chosen = jnp.zeros((items, experts), jnp.float32)
    for i in range(items):
        for k in range(ids_ref.shape[1]):
            chosen = chosen + jnp.where((item == i) & (lane == ids_ref[i, k]), 1.0, 0.0)
    scored = chosen * affinity
    gates = route_scale * scored / jnp.sum(scored, axis=1, keepdims=True)
    high = gates.astype(jnp.bfloat16)
    low = (gates - high.astype(jnp.float32)).astype(jnp.bfloat16)
    tail = jnp.concatenate(
        [high.astype(jnp.float32), low.astype(jnp.float32),
         jnp.zeros((items, spare - 2 * experts), jnp.float32)], axis=1
    ).astype(jnp.bfloat16)
    for j in range(chips):
        out_ref[j, :, 0:width] = normed
        out_ref[j, :, width:] = tail


def norm_rows(ids, parts, hidden, gain, router):
    chips, items, width = parts.shape
    experts = router.shape[1]
    spare = -(-2 * experts // 128) * 128
    return pl.pallas_call(
        norm_kernel,
        out_shape=(
            jax.ShapeDtypeStruct((items, width), jnp.float32),
            jax.ShapeDtypeStruct((chips, items, width + spare), jnp.bfloat16),
        ),
        in_specs=[SMEM, VMEM, VMEM, VMEM, VMEM],
        out_specs=(VMEM, VMEM),
        compiler_params=params(8),
        name="norm_rows",
    )(ids, parts, hidden, gain.reshape(1, width), router.T)


def experts_kernel(
    place_ref, mine_ref, other_ref, in_ref, out_w_ref, s_in_ref, s_out_ref,
    kept_ref, sent_ref, tokens, tails, own, *, depth, experts, strip,
):
    chips, items, padded = mine_ref.shape
    width = out_w_ref.shape[1]
    half = chips * items
    core, column = place_ref[0], place_ref[1]
    for side, ref in enumerate((mine_ref, other_ref)):
        for j in range(chips):
            rows = slice(side * half + j * items, side * half + (j + 1) * items)
            block = ref[j].astype(jnp.float32)
            tokens[rows, :] = block[:, :width]
            tails[rows, :] = block[:, width:]
    x = tokens[...].astype(jnp.bfloat16)
    here = column * 2 + core
    lane = lax.broadcasted_iota(jnp.int32, tails.shape, 1)
    gate = jnp.sum(
        jnp.where((lane == here) | (lane == here + experts), tails[...], 0.0),
        axis=1, keepdims=True,
    )
    g = jnp.dot(x, in_ref[0], preferred_element_type=jnp.float32)
    u = jnp.dot(x, in_ref[1], preferred_element_type=jnp.float32)
    act = (g / (1.0 + jnp.exp(-g)) * u).astype(jnp.bfloat16)
    start = pl.multiple_of(column * (depth * items), depth * items)
    xs = tokens[pl.ds(start, depth * items), :].astype(jnp.bfloat16)
    sg = jnp.dot(xs, s_in_ref[0], preferred_element_type=jnp.float32)
    su = jnp.dot(xs, s_in_ref[1], preferred_element_type=jnp.float32)
    s_act = (sg / (1.0 + jnp.exp(-sg)) * su).astype(jnp.bfloat16)
    for n in range(width // strip):
        cols = slice(n * strip, (n + 1) * strip)
        y = gate * jnp.dot(act, out_w_ref[:, cols], preferred_element_type=jnp.float32)
        ys = jnp.dot(s_act, s_out_ref[:, cols], preferred_element_type=jnp.float32)
        sent_ref[:, cols] = y[half:].astype(jnp.bfloat16)
        kept_ref[:, cols] = y[:half]
        kept_ref[pl.ds(start, depth * items), cols] = (
            kept_ref[pl.ds(start, depth * items), cols] + ys
        )


def run_experts(mine, other, expert_in, expert_out, shared_in, shared_out, place, depth, experts):
    chips, items, padded = mine.shape
    width = expert_out.shape[2]
    half = chips * items
    return pl.pallas_call(
        functools.partial(experts_kernel, depth=depth, experts=experts, strip=512),
        out_shape=(
            jax.ShapeDtypeStruct((half, width), jnp.float32),
            jax.ShapeDtypeStruct((half, width), jnp.bfloat16),
        ),
        in_specs=[SMEM] + [VMEM] * 6,
        out_specs=(VMEM, VMEM),
        scratch_shapes=[
            pltpu.VMEM((2 * half, width), jnp.float32),
            pltpu.VMEM((2 * half, padded - width), jnp.float32),
            pltpu.VMEM((depth * items, width), jnp.bfloat16),
        ],
        compiler_params=params(32),
        name="experts",
    )(place, mine, other, expert_in[0], expert_out[0], shared_in, shared_out)


def finish_kernel(parts_ref, residual_ref, out_ref):
    total = residual_ref[...]
    for j in range(parts_ref.shape[0]):
        total = total + parts_ref[j].astype(jnp.float32)
    out_ref[...] = total.astype(jnp.bfloat16)


def finish(parts, residual):
    return pl.pallas_call(
        finish_kernel,
        out_shape=jax.ShapeDtypeStruct(residual.shape, jnp.bfloat16),
        in_specs=[VMEM, VMEM],
        out_specs=VMEM,
        compiler_params=params(8),
        name="finish",
    )(parts, residual)


def swap_cores(x):
    return lax.ppermute(x, "core", [(0, 1), (1, 0)])


def chip_exchange(x):
    return lax.all_to_all(x, CHIPS, split_axis=0, concat_axis=0, tiled=True)


def attend_block(queries, kv_cache, new_kv, lengths):
    rows_here, steps_here, heads_here, kv_width = queries.shape
    positions = kv_cache.shape[1]
    cached = (
        jnp.einsum("rshk,rck->rshc", queries, kv_cache, preferred_element_type=jnp.float32)
        * score_scale
    )
    recent = (
        jnp.einsum("rshk,rjk->rshj", queries, new_kv, preferred_element_type=jnp.float32)
        * score_scale
    )
    cache_live = lax.broadcasted_iota(jnp.int32, (rows_here, positions), 1) < lengths[:, None]
    causal = lax.broadcasted_iota(jnp.int32, (steps_here, steps_here), 1) <= lax.broadcasted_iota(
        jnp.int32, (steps_here, steps_here), 0
    )
    cached = jnp.where(cache_live[:, None, None, :], cached, -1e30)
    recent = jnp.where(causal[None, :, None, :], recent, -1e30)
    highest = jnp.maximum(cached.max(-1), recent.max(-1))[..., None]
    cached_exp = jnp.exp(cached - highest)
    recent_exp = jnp.exp(recent - highest)
    denominator = cached_exp.sum(-1, keepdims=True) + recent_exp.sum(-1, keepdims=True)
    cached_prob = (cached_exp / denominator).astype(jnp.bfloat16)
    recent_prob = (recent_exp / denominator).astype(jnp.bfloat16)
    combined = jnp.einsum(
        "rshc,rck->rshk", cached_prob, kv_cache, preferred_element_type=jnp.float32
    )
    combined = combined + jnp.einsum(
        "rshj,rjk->rshk", recent_prob, new_kv, preferred_element_type=jnp.float32
    )
    return combined[..., :LAT].astype(jnp.bfloat16)


def sum_at_rows(kept, sent, chips):
    half = kept + swap_cores(sent.astype(jnp.bfloat16)).astype(jnp.float32)
    width = half.shape[1]
    parts = chip_exchange(half.astype(jnp.bfloat16).reshape(chips, -1, width))
    return jnp.sum(parts.astype(jnp.float32), axis=0)


def plain_device(
    hidden_in,
    queries,
    kv_cache,
    new_kv,
    lengths,
    expert_ids,
    value_up,
    out_proj,
    norm_gain,
    router,
    expert_in,
    expert_out,
    shared_in,
    shared_out,
):
    rows_here, steps_here, model_width = hidden_in.shape
    items = rows_here * steps_here
    columns = lax.axis_size("epx")
    depth = lax.axis_size("tp")
    chips = columns * depth
    core = lax.axis_index("core")
    column = lax.axis_index("epx")
    place = lax.axis_index("tp")
    expert_count = router.shape[1]

    latent_out = attend_block(queries, kv_cache, new_kv, lengths)
    by_head = lax.all_to_all(latent_out, ALL, split_axis=2, concat_axis=0, tiled=True)
    head_vals = jnp.einsum(
        "rshl,hlv->rshv", by_head, value_up, preferred_element_type=jnp.float32
    ).astype(jnp.bfloat16)
    partial = jnp.einsum(
        "rshv,hvd->rsd", head_vals, out_proj, preferred_element_type=jnp.float32
    ).reshape(columns, 2, depth * items, model_width)
    kept = lax.dynamic_index_in_dim(partial, core, 1, keepdims=False)
    sent = lax.dynamic_index_in_dim(partial, 1 - core, 1, keepdims=False)
    attention = sum_at_rows(
        kept.reshape(-1, model_width), sent.reshape(-1, model_width), chips
    )
    residual = hidden_in.reshape(items, model_width).astype(jnp.float32) + attention
    mean_square = jnp.mean(residual * residual, axis=-1, keepdims=True)
    normed = (residual * lax.rsqrt(mean_square + norm_eps) * norm_gain.astype(jnp.float32)).astype(
        jnp.bfloat16
    )
    affinity = jax.nn.sigmoid(jnp.dot(normed, router, preferred_element_type=jnp.float32))
    picked = lax.dynamic_slice_in_dim(expert_ids, place * rows_here, rows_here, 0).reshape(
        items, expert_ids.shape[2]
    )
    expert_iota = lax.broadcasted_iota(jnp.int32, (1, 1, expert_count), 2)
    chosen = jnp.sum((picked[:, :, None] == expert_iota).astype(jnp.float32), axis=1)
    scored = chosen * affinity
    gate_weight = route_scale * scored / jnp.sum(scored, axis=-1, keepdims=True)
    gate_high = gate_weight.astype(jnp.bfloat16)
    gate_low = (gate_weight - gate_high.astype(jnp.float32)).astype(jnp.bfloat16)
    spare = -(2 * expert_count) % 128
    payload = jnp.concatenate(
        [normed, gate_high, gate_low, jnp.zeros((items, spare), jnp.bfloat16)], axis=1
    )
    mine = chip_exchange(jnp.broadcast_to(payload[None], (chips,) + payload.shape)).reshape(
        chips * items, -1
    )
    tokens = jnp.concatenate([mine, swap_cores(mine)], axis=0)
    block_items = tokens[:, :model_width]
    expert_here = column * 2 + core
    gate_pairs = tokens[:, model_width : model_width + 2 * expert_count].astype(jnp.float32)
    gates = gate_pairs[:, :expert_count] + gate_pairs[:, expert_count:]
    gate_here = lax.dynamic_slice_in_dim(gates, expert_here, 1, 1)

    gate_part = jnp.dot(block_items, expert_in[0, 0], preferred_element_type=jnp.float32)
    up_part = jnp.dot(block_items, expert_in[0, 1], preferred_element_type=jnp.float32)
    activated = (jax.nn.silu(gate_part) * up_part).astype(jnp.bfloat16)
    routed = gate_here * jnp.dot(activated, expert_out[0], preferred_element_type=jnp.float32)

    own = lax.dynamic_slice_in_dim(mine, column * depth * items, depth * items, 0)[
        :, :model_width
    ]
    shared_gate = jnp.dot(own, shared_in[0], preferred_element_type=jnp.float32)
    shared_up = jnp.dot(own, shared_in[1], preferred_element_type=jnp.float32)
    shared_act = (jax.nn.silu(shared_gate) * shared_up).astype(jnp.bfloat16)
    shared_part = jnp.dot(shared_act, shared_out, preferred_element_type=jnp.float32)

    kept = routed[: chips * items].reshape(columns, depth * items, model_width)
    at_column = lax.broadcasted_iota(jnp.int32, (columns, 1, 1), 0) == column
    kept = kept + jnp.where(at_column, shared_part[None], 0.0)
    expert_sum = sum_at_rows(
        kept.reshape(-1, model_width), routed[chips * items :], chips
    )
    layer_out = (residual + expert_sum).astype(jnp.bfloat16)
    return layer_out.reshape(rows_here, steps_here, model_width)


def on_device(
    hidden_in,
    queries,
    kv_cache,
    new_kv,
    lengths,
    expert_ids,
    value_up,
    out_proj,
    norm_gain,
    router,
    expert_in,
    expert_out,
    shared_in,
    shared_out,
):
    rows_here, steps_here, model_width = hidden_in.shape
    items = rows_here * steps_here
    columns = lax.axis_size("epx")
    depth = lax.axis_size("tp")
    chips = columns * depth
    owners = 2 * chips
    core = lax.axis_index("core").astype(jnp.int32)
    column = lax.axis_index("epx").astype(jnp.int32)
    place = lax.axis_index("tp")
    experts = router.shape[1]

    latent_out = attend(queries, kv_cache, new_kv, lengths, owners)
    by_head = lax.all_to_all(latent_out, ALL, split_axis=0, concat_axis=0, tiled=True)
    kept, sent = project(by_head, value_up, out_proj, core.reshape(1), depth)
    parts = chip_exchange(merge(kept, swap_cores(sent), chips))
    ids = lax.dynamic_slice_in_dim(expert_ids, place * rows_here, rows_here, 0).reshape(
        items, expert_ids.shape[2]
    )
    residual, handed = norm_rows(
        ids, parts, hidden_in.reshape(items, model_width), norm_gain, router
    )
    mine = chip_exchange(handed)
    kept, sent = run_experts(
        mine, swap_cores(mine), expert_in, expert_out, shared_in, shared_out,
        jnp.stack([core, column]), depth, experts,
    )
    parts = chip_exchange(merge(kept, swap_cores(sent), chips))
    return finish(parts, residual).reshape(rows_here, steps_here, model_width)


def choose(*args):
    owners = 2 * lax.axis_size("epx") * lax.axis_size("tp")
    queries = args[1]
    whole_tiles = queries.shape[0] == 1 and queries.shape[2] % (8 * owners) == 0
    return on_device(*args) if whole_tiles else plain_device(*args)


def solution(mesh):
    sizes = mesh.shape
    fine = Mesh(
        mesh.devices.reshape(sizes["groups"], sizes["ep"] // 2, 2, sizes["tp"]),
        ("groups", "epx", "core", "tp"),
    )
    ep = ("epx", "core")
    rows = ("groups", "epx", "core", "tp")
    in_specs = (
        P(rows, None, None),
        P(rows, None, None, None),
        P(rows, None, None),
        P(rows, None, None),
        P(rows),
        P(("groups",) + ep, None, None),
        P(ALL, None, None),
        P(ALL, None, None),
        P(),
        P(),
        P(ep, None, None, "tp"),
        P(ep, "tp", None),
        P(None, None, "tp"),
        P("tp", None),
    )
    out_specs = P(rows, None, None)
    return jax.shard_map(
        choose, mesh=fine, in_specs=in_specs, out_specs=out_specs, check_vma=False
    )
```

```python
import functools

import jax
import jax.numpy as jnp
from jax import lax
from jax.experimental import pallas as pl
from jax.experimental.pallas import tpu as pltpu
from jax.sharding import Mesh
from jax.sharding import PartitionSpec as P

LAT = 512


score_scale = 192.0 ** (-0.5)
log2_e = 1.4426950408889634
route_scale = 2.5
norm_eps = 1e-06

CHIPS = ("epx", "tp")
ALL = ("epx", "core", "tp")
VMEM = pl.BlockSpec(memory_space=pltpu.VMEM)
SMEM = pl.BlockSpec(memory_space=pltpu.SMEM)
HBM = pl.BlockSpec(memory_space=pltpu.HBM)


def params(mib):
    return pltpu.CompilerParams(vmem_limit_bytes=mib << 20)


def fetch(stored, held, sems, first):
    copies = [
        pltpu.make_async_copy(a, b, sems.at[first + i])
        for i, (a, b) in enumerate(zip(stored, held))
    ]
    for copy in copies:
        copy.start()
    return copies


def in_hbm(x):
    return pltpu.with_memory_space_constraint(x, pltpu.HBM)


def like(x):
    return jax.ShapeDtypeStruct(x.shape, x.dtype)


def attend_kernel(length_ref, q_hbm, kv_hbm, new_hbm, *refs, chunk, block, ahead):
    stored, out_ref, held = refs[:ahead], refs[ahead], refs[ahead + 1 : 2 * ahead + 1]
    new_ref, q_t, q_rows, kv_t, new_rows, scores, recent, weights, row_max, sems = (
        refs[2 * ahead + 1 :]
    )
    steps, width, heads = q_t.shape
    positions = kv_t.shape[1]
    rows = steps * heads
    q_copy = pltpu.make_async_copy(q_hbm, q_t, sems.at[0])
    q_copy.start()
    new_copy = pltpu.make_async_copy(new_hbm, new_ref, sems.at[sems.shape[0] - 1])
    new_copy.start()
    copies = []
    for c in range(positions // chunk):
        span = pl.ds(c * chunk, chunk)
        copies.append(
            pltpu.make_async_copy(kv_hbm.at[:, span], kv_t.at[:, span], sems.at[1 + c])
        )
        copies[-1].start()
    new_rows[...] = jnp.zeros_like(new_rows)
    new_copy.wait()
    new_rows[0:steps, :] = new_ref[...]
    q_copy.wait()
    for s in range(steps):
        q_rows[s * heads : (s + 1) * heads, :] = q_t[s].T
    length = length_ref[0]
    lanes = new_rows.shape[0]
    fresh = lax.dot_general(
        q_rows[...], new_rows[...], (((1,), (1,)), ((), ())),
        preferred_element_type=jnp.float32,
    )
    step_of = lax.broadcasted_iota(jnp.int32, (rows, lanes), 0) // heads
    fresh = jnp.where(
        lax.broadcasted_iota(jnp.int32, (rows, lanes), 1) <= step_of, fresh, -1e30
    )
    recent[...] = fresh
    row_max[...] = fresh
    fetches = []
    for c in range(positions // chunk):
        copies[c].wait()
        if c + 1 == positions // chunk:
            fetches = fetch(stored, held, sems, 1 + positions // chunk)
        live = (lax.broadcasted_iota(jnp.int32, (1, chunk), 1) + c * chunk) < length
        for b in range(rows // block):
            span = slice(b * block, (b + 1) * block)
            s = jnp.dot(
                q_rows[span, :], kv_t[:, c * chunk : (c + 1) * chunk],
                preferred_element_type=jnp.float32,
            )
            s = jnp.where(live, s, -1e30)
            scores[span, c * chunk : (c + 1) * chunk] = s
            best = row_max[span, :]
            for j in range(chunk // lanes):
                best = jnp.maximum(best, s[:, j * lanes : (j + 1) * lanes])
            row_max[span, :] = best
    rate = score_scale * log2_e
    per_owner = out_ref.shape[1] // steps
    for b in range(rows // block):
        span = slice(b * block, (b + 1) * block)
        top = jnp.max(row_max[span, :], axis=1, keepdims=True) * rate
        fresh = jnp.exp2(recent[span, :] * rate - top)
        total = fresh
        fresh = fresh.astype(jnp.bfloat16)
        for c in range(positions // chunk):
            e = jnp.exp2(scores[span, c * chunk : (c + 1) * chunk] * rate - top)
            for j in range(chunk // lanes):
                total = total + e[:, j * lanes : (j + 1) * lanes]
            weights[span, c * chunk : (c + 1) * chunk] = e.astype(jnp.bfloat16)
        mixed = lax.dot_general(
            weights[span, :], kv_t[0:LAT, :], (((1,), (1,)), ((), ())),
            preferred_element_type=jnp.float32,
        ) + jnp.dot(fresh, new_rows[:, 0:LAT], preferred_element_type=jnp.float32)
        mixed = mixed / jnp.sum(total, axis=1, keepdims=True)
        for i in range(block // heads):
            s = b * (block // heads) + i
            part = mixed[i * heads : (i + 1) * heads, :]
            out_ref[:, s * per_owner : (s + 1) * per_owner, :] = part.reshape(
                heads // per_owner, per_owner, LAT
            ).astype(jnp.bfloat16)
    for copy in fetches:
        copy.wait()


def attend(queries, kv_cache, new_kv, lengths, owners, ahead):
    _, steps, heads, width = queries.shape
    positions = kv_cache.shape[1]
    rows = steps * heads
    chunk = 512
    lanes = 128
    block = 2 * heads
    return pl.pallas_call(
        functools.partial(attend_kernel, chunk=chunk, block=block, ahead=len(ahead)),
        out_shape=[jax.ShapeDtypeStruct((owners, rows // owners, LAT), jnp.bfloat16)]
        + [like(x) for x in ahead],
        in_specs=[SMEM] + [HBM] * (3 + len(ahead)),
        out_specs=[VMEM] * (1 + len(ahead)),
        scratch_shapes=[
            pltpu.VMEM((steps, width), jnp.bfloat16),
            pltpu.VMEM((steps, width, heads), jnp.bfloat16),
            pltpu.VMEM((rows, width), jnp.bfloat16),
            pltpu.VMEM((width, positions), jnp.bfloat16),
            pltpu.VMEM((lanes, width), jnp.bfloat16),
            pltpu.VMEM((rows, positions), jnp.float32),
            pltpu.VMEM((rows, lanes), jnp.float32),
            pltpu.VMEM((rows, positions), jnp.bfloat16),
            pltpu.VMEM((rows, lanes), jnp.float32),
            pltpu.SemaphoreType.DMA((2 + positions // chunk + len(ahead),)),
        ],
        compiler_params=params(16),
        name="attend",
    )(
        lengths,
        in_hbm(jnp.swapaxes(queries[0], 1, 2)),
        in_hbm(jnp.swapaxes(kv_cache[0], 0, 1)),
        in_hbm(new_kv[0]),
        *[in_hbm(x) for x in ahead],
    )


def project_kernel(
    latent_ref, up_ref, down_ref, *refs, depth, strip, ahead
):
    stored, kept_ref, sent_ref = refs[:ahead], refs[ahead], refs[ahead + 1]
    held, latents, sems = refs[ahead + 2 : 2 * ahead + 2], refs[2 * ahead + 2], refs[2 * ahead + 3]
    fetches = fetch(stored, held, sems, 0)
    sources, owned, _ = latent_ref.shape
    heads = up_ref.shape[0]
    steps = owned // heads
    items = sources * steps
    core = lax.axis_index("core")
    place = 0
    for side in (core, 1 - core):
        for column in range(sources // (2 * depth)):
            for t in range(depth):
                source = (column * 2 + side) * depth + t
                block = latent_ref[source].astype(jnp.float32)
                for j in range(LAT // 128):
                    latents[j, place * owned : (place + 1) * owned, :] = block[
                        :, j * 128 : (j + 1) * 128
                    ]
                place += 1
    vals = []
    for h in range(heads):
        x = jnp.concatenate(
            [latents[j, pl.ds(h, items, stride=heads), :] for j in range(LAT // 128)], axis=1
        ).astype(jnp.bfloat16)
        vals.append(
            jnp.dot(x, up_ref[h], preferred_element_type=jnp.float32).astype(jnp.bfloat16)
        )
    vals = jnp.concatenate(vals, axis=1)
    width = down_ref.shape[1]
    half = items // 2
    for n in range(width // strip):
        cols = slice(n * strip, (n + 1) * strip)
        part = jnp.dot(vals, down_ref[:, cols], preferred_element_type=jnp.float32)
        kept_ref[:, cols] = part[:half]
        sent_ref[:, cols] = part[half:].astype(jnp.bfloat16)
    for copy in fetches:
        copy.wait()


def project(by_head, value_up, out_proj, depth, ahead):
    sources, owned, _ = by_head.shape
    heads, _, value_width = value_up.shape
    width = out_proj.shape[2]
    half = sources * owned // heads // 2
    return pl.pallas_call(
        functools.partial(project_kernel, depth=depth, strip=512, ahead=len(ahead)),
        out_shape=[
            jax.ShapeDtypeStruct((half, width), jnp.float32),
            jax.ShapeDtypeStruct((half, width), jnp.bfloat16),
        ]
        + [like(x) for x in ahead],
        in_specs=[VMEM, VMEM, VMEM] + [HBM] * len(ahead),
        out_specs=[VMEM] * (2 + len(ahead)),
        scratch_shapes=[
            pltpu.VMEM((LAT // 128, sources * owned, 128), jnp.float32),
            pltpu.SemaphoreType.DMA((max(1, len(ahead)),)),
        ],
        compiler_params=params(8),
        name="project",
    )(
        by_head, value_up, out_proj.reshape(heads * value_width, width),
        *[in_hbm(x) for x in ahead],
    )


def merge_kernel(kept_ref, got_ref, out_ref):
    chips, items, _ = out_ref.shape
    total = kept_ref[...] + got_ref[...].astype(jnp.float32)
    for j in range(chips):
        out_ref[j] = total[j * items : (j + 1) * items, :].astype(jnp.bfloat16)


def merge(kept, got, chips):
    rows, width = kept.shape
    return pl.pallas_call(
        merge_kernel,
        out_shape=jax.ShapeDtypeStruct((chips, rows // chips, width), jnp.bfloat16),
        in_specs=[VMEM, VMEM],
        out_specs=VMEM,
        compiler_params=params(4),
        name="merge",
    )(kept, got)


def norm_kernel(ids_ref, parts_ref, hidden_ref, gain_ref, router_ref, residual_ref, out_ref):
    chips, items, _ = parts_ref.shape
    width = hidden_ref.shape[1]
    experts = router_ref.shape[0]
    spare = out_ref.shape[2] - width
    place = lax.axis_index("tp")
    total = hidden_ref[...].astype(jnp.float32)
    attention = parts_ref[0].astype(jnp.float32)
    for j in range(1, chips):
        attention = attention + parts_ref[j].astype(jnp.float32)
    residual = total + attention
    residual_ref[...] = residual
    square = jnp.mean(residual * residual, axis=1, keepdims=True)
    normed = (residual * lax.rsqrt(square + norm_eps) * gain_ref[...].astype(jnp.float32).reshape(1, width)).astype(
        jnp.bfloat16
    )
    logits = lax.dot_general(
        normed, router_ref[...], (((1,), (1,)), ((), ())), preferred_element_type=jnp.float32
    )
    affinity = 1.0 / (1.0 + jnp.exp(-logits))
    item = lax.broadcasted_iota(jnp.int32, (items, experts), 0)
    lane = lax.broadcasted_iota(jnp.int32, (items, experts), 1)
    chosen = jnp.zeros((items, experts), jnp.float32)
    for i in range(items):
        for k in range(ids_ref.shape[1]):
            named = ids_ref[place, k, i]
            chosen = chosen + jnp.where((item == i) & (lane == named), 1.0, 0.0)
    scored = chosen * affinity
    gates = route_scale * scored / jnp.sum(scored, axis=1, keepdims=True)
    high = gates.astype(jnp.bfloat16)
    low = (gates - high.astype(jnp.float32)).astype(jnp.bfloat16)
    tail = jnp.concatenate(
        [high.astype(jnp.float32), low.astype(jnp.float32),
         jnp.zeros((items, spare - 2 * experts), jnp.float32)], axis=1
    ).astype(jnp.bfloat16)
    for j in range(chips):
        out_ref[j, :, 0:width] = normed
        out_ref[j, :, width:] = tail


def norm_rows(ids, parts, hidden, gain, router):
    chips, items, width = parts.shape
    experts = router.shape[1]
    spare = -(-2 * experts // 128) * 128
    return pl.pallas_call(
        norm_kernel,
        out_shape=(
            jax.ShapeDtypeStruct((items, width), jnp.float32),
            jax.ShapeDtypeStruct((chips, items, width + spare), jnp.bfloat16),
        ),
        in_specs=[SMEM, VMEM, VMEM, VMEM, VMEM],
        out_specs=(VMEM, VMEM),
        compiler_params=params(8),
        name="norm_rows",
    )(ids, parts, hidden, gain, router.T)


def experts_kernel(
    mine_ref, other_ref, in_ref, out_w_ref, s_in_ref, s_out_ref,
    kept_ref, sent_ref, tokens, tails, own, *, depth, experts, strip,
):
    chips, items, padded = mine_ref.shape
    width = out_w_ref.shape[1]
    half = chips * items
    core, column = lax.axis_index("core"), lax.axis_index("epx")
    for side, ref in enumerate((mine_ref, other_ref)):
        for j in range(chips):
            rows = slice(side * half + j * items, side * half + (j + 1) * items)
            block = ref[j].astype(jnp.float32)
            tokens[rows, :] = block[:, :width]
            tails[rows, :] = block[:, width:]
    x = tokens[...].astype(jnp.bfloat16)
    here = column * 2 + core
    lane = lax.broadcasted_iota(jnp.int32, tails.shape, 1)
    gate = jnp.sum(
        jnp.where((lane == here) | (lane == here + experts), tails[...], 0.0),
        axis=1, keepdims=True,
    )
    g = jnp.dot(x, in_ref[0], preferred_element_type=jnp.float32)
    u = jnp.dot(x, in_ref[1], preferred_element_type=jnp.float32)
    act = (g / (1.0 + jnp.exp(-g)) * u).astype(jnp.bfloat16)
    start = pl.multiple_of(column * (depth * items), depth * items)
    xs = tokens[pl.ds(start, depth * items), :].astype(jnp.bfloat16)
    sg = jnp.dot(xs, s_in_ref[0], preferred_element_type=jnp.float32)
    su = jnp.dot(xs, s_in_ref[1], preferred_element_type=jnp.float32)
    s_act = (sg / (1.0 + jnp.exp(-sg)) * su).astype(jnp.bfloat16)
    for n in range(width // strip):
        cols = slice(n * strip, (n + 1) * strip)
        y = gate * jnp.dot(act, out_w_ref[:, cols], preferred_element_type=jnp.float32)
        ys = jnp.dot(s_act, s_out_ref[:, cols], preferred_element_type=jnp.float32)
        sent_ref[:, cols] = y[half:].astype(jnp.bfloat16)
        kept_ref[:, cols] = y[:half]
        kept_ref[pl.ds(start, depth * items), cols] = (
            kept_ref[pl.ds(start, depth * items), cols] + ys
        )


def run_experts(mine, other, expert_in, expert_out, shared_in, shared_out, depth, experts):
    chips, items, padded = mine.shape
    width = expert_out.shape[1]
    half = chips * items
    return pl.pallas_call(
        functools.partial(experts_kernel, depth=depth, experts=experts, strip=512),
        out_shape=(
            jax.ShapeDtypeStruct((half, width), jnp.float32),
            jax.ShapeDtypeStruct((half, width), jnp.bfloat16),
        ),
        in_specs=[VMEM] * 6,
        out_specs=(VMEM, VMEM),
        scratch_shapes=[
            pltpu.VMEM((2 * half, width), jnp.float32),
            pltpu.VMEM((2 * half, padded - width), jnp.float32),
            pltpu.VMEM((depth * items, width), jnp.bfloat16),
        ],
        compiler_params=params(8),
        name="experts",
    )(mine, other, expert_in, expert_out, shared_in, shared_out)


def finish_kernel(parts_ref, residual_ref, out_ref):
    total = residual_ref[...]
    for j in range(parts_ref.shape[0]):
        total = total + parts_ref[j].astype(jnp.float32)
    out_ref[...] = total.astype(jnp.bfloat16)


def finish(parts, residual):
    return pl.pallas_call(
        finish_kernel,
        out_shape=jax.ShapeDtypeStruct(residual.shape, jnp.bfloat16),
        in_specs=[VMEM, VMEM],
        out_specs=VMEM,
        compiler_params=params(8),
        name="finish",
    )(parts, residual)


def swap_cores(x):
    return lax.ppermute(x, "core", [(0, 1), (1, 0)])


def chip_exchange(x):
    return lax.all_to_all(x, CHIPS, split_axis=0, concat_axis=0, tiled=True)


def attend_block(queries, kv_cache, new_kv, lengths):
    rows_here, steps_here, heads_here, kv_width = queries.shape
    positions = kv_cache.shape[1]
    cached = (
        jnp.einsum("rshk,rck->rshc", queries, kv_cache, preferred_element_type=jnp.float32)
        * score_scale
    )
    recent = (
        jnp.einsum("rshk,rjk->rshj", queries, new_kv, preferred_element_type=jnp.float32)
        * score_scale
    )
    cache_live = lax.broadcasted_iota(jnp.int32, (rows_here, positions), 1) < lengths[:, None]
    causal = lax.broadcasted_iota(jnp.int32, (steps_here, steps_here), 1) <= lax.broadcasted_iota(
        jnp.int32, (steps_here, steps_here), 0
    )
    cached = jnp.where(cache_live[:, None, None, :], cached, -1e30)
    recent = jnp.where(causal[None, :, None, :], recent, -1e30)
    highest = jnp.maximum(cached.max(-1), recent.max(-1))[..., None]
    cached_exp = jnp.exp(cached - highest)
    recent_exp = jnp.exp(recent - highest)
    denominator = cached_exp.sum(-1, keepdims=True) + recent_exp.sum(-1, keepdims=True)
    cached_prob = (cached_exp / denominator).astype(jnp.bfloat16)
    recent_prob = (recent_exp / denominator).astype(jnp.bfloat16)
    combined = jnp.einsum(
        "rshc,rck->rshk", cached_prob, kv_cache, preferred_element_type=jnp.float32
    )
    combined = combined + jnp.einsum(
        "rshj,rjk->rshk", recent_prob, new_kv, preferred_element_type=jnp.float32
    )
    return combined[..., :LAT].astype(jnp.bfloat16)


def sum_at_rows(kept, sent, chips):
    half = kept + swap_cores(sent.astype(jnp.bfloat16)).astype(jnp.float32)
    width = half.shape[1]
    parts = chip_exchange(half.astype(jnp.bfloat16).reshape(chips, -1, width))
    return jnp.sum(parts.astype(jnp.float32), axis=0)


def plain_device(
    hidden_in,
    queries,
    kv_cache,
    new_kv,
    lengths,
    expert_ids,
    value_up,
    out_proj,
    norm_gain,
    router,
    expert_in,
    expert_out,
    shared_in,
    shared_out,
):
    rows_here, steps_here, model_width = hidden_in.shape
    items = rows_here * steps_here
    columns = lax.axis_size("epx")
    depth = lax.axis_size("tp")
    chips = columns * depth
    core = lax.axis_index("core")
    column = lax.axis_index("epx")
    place = lax.axis_index("tp")
    expert_count = router.shape[1]

    latent_out = attend_block(queries, kv_cache, new_kv, lengths)
    by_head = lax.all_to_all(latent_out, ALL, split_axis=2, concat_axis=0, tiled=True)
    head_vals = jnp.einsum(
        "rshl,hlv->rshv", by_head, value_up, preferred_element_type=jnp.float32
    ).astype(jnp.bfloat16)
    partial = jnp.einsum(
        "rshv,hvd->rsd", head_vals, out_proj, preferred_element_type=jnp.float32
    ).reshape(columns, 2, depth * items, model_width)
    kept = lax.dynamic_index_in_dim(partial, core, 1, keepdims=False)
    sent = lax.dynamic_index_in_dim(partial, 1 - core, 1, keepdims=False)
    attention = sum_at_rows(
        kept.reshape(-1, model_width), sent.reshape(-1, model_width), chips
    )
    residual = hidden_in.reshape(items, model_width).astype(jnp.float32) + attention
    mean_square = jnp.mean(residual * residual, axis=-1, keepdims=True)
    normed = (residual * lax.rsqrt(mean_square + norm_eps) * norm_gain.astype(jnp.float32)).astype(
        jnp.bfloat16
    )
    affinity = jax.nn.sigmoid(jnp.dot(normed, router, preferred_element_type=jnp.float32))
    picked = lax.dynamic_slice_in_dim(expert_ids, place * rows_here, rows_here, 0).reshape(
        items, expert_ids.shape[2]
    )
    expert_iota = lax.broadcasted_iota(jnp.int32, (1, 1, expert_count), 2)
    chosen = jnp.sum((picked[:, :, None] == expert_iota).astype(jnp.float32), axis=1)
    scored = chosen * affinity
    gate_weight = route_scale * scored / jnp.sum(scored, axis=-1, keepdims=True)
    gate_high = gate_weight.astype(jnp.bfloat16)
    gate_low = (gate_weight - gate_high.astype(jnp.float32)).astype(jnp.bfloat16)
    spare = -(2 * expert_count) % 128
    payload = jnp.concatenate(
        [normed, gate_high, gate_low, jnp.zeros((items, spare), jnp.bfloat16)], axis=1
    )
    mine = chip_exchange(jnp.broadcast_to(payload[None], (chips,) + payload.shape)).reshape(
        chips * items, -1
    )
    tokens = jnp.concatenate([mine, swap_cores(mine)], axis=0)
    block_items = tokens[:, :model_width]
    expert_here = column * 2 + core
    gate_pairs = tokens[:, model_width : model_width + 2 * expert_count].astype(jnp.float32)
    gates = gate_pairs[:, :expert_count] + gate_pairs[:, expert_count:]
    gate_here = lax.dynamic_slice_in_dim(gates, expert_here, 1, 1)

    gate_part = jnp.dot(block_items, expert_in[0, 0], preferred_element_type=jnp.float32)
    up_part = jnp.dot(block_items, expert_in[0, 1], preferred_element_type=jnp.float32)
    activated = (jax.nn.silu(gate_part) * up_part).astype(jnp.bfloat16)
    routed = gate_here * jnp.dot(activated, expert_out[0], preferred_element_type=jnp.float32)

    own = lax.dynamic_slice_in_dim(mine, column * depth * items, depth * items, 0)[
        :, :model_width
    ]
    shared_gate = jnp.dot(own, shared_in[0], preferred_element_type=jnp.float32)
    shared_up = jnp.dot(own, shared_in[1], preferred_element_type=jnp.float32)
    shared_act = (jax.nn.silu(shared_gate) * shared_up).astype(jnp.bfloat16)
    shared_part = jnp.dot(shared_act, shared_out, preferred_element_type=jnp.float32)

    kept = routed[: chips * items].reshape(columns, depth * items, model_width)
    at_column = lax.broadcasted_iota(jnp.int32, (columns, 1, 1), 0) == column
    kept = kept + jnp.where(at_column, shared_part[None], 0.0)
    expert_sum = sum_at_rows(
        kept.reshape(-1, model_width), routed[chips * items :], chips
    )
    layer_out = (residual + expert_sum).astype(jnp.bfloat16)
    return layer_out.reshape(rows_here, steps_here, model_width)


def on_device(
    hidden_in,
    queries,
    kv_cache,
    new_kv,
    lengths,
    expert_ids,
    value_up,
    out_proj,
    norm_gain,
    router,
    expert_in,
    expert_out,
    shared_in,
    shared_out,
):
    rows_here, steps_here, model_width = hidden_in.shape
    items = rows_here * steps_here
    columns = lax.axis_size("epx")
    depth = lax.axis_size("tp")
    chips = columns * depth
    owners = 2 * chips
    experts = router.shape[1]

    latent_out, out_proj, value_up, expert_in = attend(
        queries, kv_cache, new_kv, lengths, owners, [out_proj, value_up, expert_in[0]]
    )
    by_head = lax.all_to_all(latent_out, ALL, split_axis=0, concat_axis=0, tiled=True)
    kept, sent, expert_out, shared_in, shared_out = project(
        by_head, value_up, out_proj, depth, [expert_out[0], shared_in, shared_out]
    )
    parts = chip_exchange(merge(kept, swap_cores(sent), chips))
    ids = jnp.swapaxes(expert_ids, 1, 2)
    residual, handed = norm_rows(
        ids, parts, hidden_in.reshape(items, model_width), norm_gain, router
    )
    mine = chip_exchange(handed)
    kept, sent = run_experts(
        mine, swap_cores(mine), expert_in, expert_out, shared_in, shared_out, depth, experts,
    )
    parts = chip_exchange(merge(kept, swap_cores(sent), chips))
    return finish(parts, residual).reshape(rows_here, steps_here, model_width)


def choose(*args):
    owners = 2 * lax.axis_size("epx") * lax.axis_size("tp")
    queries = args[1]
    whole_tiles = queries.shape[0] == 1 and queries.shape[2] % (8 * owners) == 0
    return on_device(*args) if whole_tiles else plain_device(*args)


def solution(mesh):
    sizes = mesh.shape
    fine = Mesh(
        mesh.devices.reshape(sizes["groups"], sizes["ep"] // 2, 2, sizes["tp"]),
        ("groups", "epx", "core", "tp"),
    )
    ep = ("epx", "core")
    rows = ("groups", "epx", "core", "tp")
    in_specs = (
        P(rows, None, None),
        P(rows, None, None, None),
        P(rows, None, None),
        P(rows, None, None),
        P(rows),
        P(("groups",) + ep, None, None),
        P(ALL, None, None),
        P(ALL, None, None),
        P(),
        P(),
        P(ep, None, None, "tp"),
        P(ep, "tp", None),
        P(None, None, "tp"),
        P("tp", None),
    )
    out_specs = P(rows, None, None)
    return jax.shard_map(
        choose, mesh=fine, in_specs=in_specs, out_specs=out_specs, check_vma=False
    )
```

```python
import functools

import jax
import jax.numpy as jnp
from jax import lax
from jax.experimental import pallas as pl
from jax.experimental.pallas import tpu as pltpu
from jax.sharding import Mesh
from jax.sharding import PartitionSpec as P

LAT = 512


score_scale = 192.0 ** (-0.5)
log2_e = 1.4426950408889634
route_scale = 2.5
norm_eps = 1e-06

CHIPS = ("epx", "tp")
ALL = ("epx", "core", "tp")
VMEM = pl.BlockSpec(memory_space=pltpu.VMEM)
SMEM = pl.BlockSpec(memory_space=pltpu.SMEM)
HBM = pl.BlockSpec(memory_space=pltpu.HBM)


def params(mib):
    return pltpu.CompilerParams(vmem_limit_bytes=mib << 20)


def fetch(stored, held, sems, first):
    copies = [
        pltpu.make_async_copy(a, b, sems.at[first + i])
        for i, (a, b) in enumerate(zip(stored, held))
    ]
    for copy in copies:
        copy.start()
    return copies


def in_hbm(x):
    return pltpu.with_memory_space_constraint(x, pltpu.HBM)


def like(x):
    return jax.ShapeDtypeStruct(x.shape, x.dtype)


def attend_kernel(length_ref, q_hbm, kv_hbm, new_hbm, *refs, chunk, block, ahead):
    stored, out_ref, held = refs[:ahead], refs[ahead], refs[ahead + 1 : 2 * ahead + 1]
    new_ref, q_t, q_rows, kv_t, new_rows, scores, recent, weights, row_max, sems = (
        refs[2 * ahead + 1 :]
    )
    steps, width, heads = q_t.shape
    positions = kv_t.shape[1]
    rows = steps * heads
    q_copy = pltpu.make_async_copy(q_hbm, q_t, sems.at[0])
    q_copy.start()
    new_copy = pltpu.make_async_copy(new_hbm, new_ref, sems.at[sems.shape[0] - 1])
    new_copy.start()
    copies = []
    for c in range(positions // chunk):
        span = pl.ds(c * chunk, chunk)
        copies.append(
            pltpu.make_async_copy(kv_hbm.at[:, span], kv_t.at[:, span], sems.at[1 + c])
        )
        copies[-1].start()
    new_rows[...] = jnp.zeros_like(new_rows)
    new_copy.wait()
    new_rows[0:steps, :] = new_ref[...]
    q_copy.wait()
    for s in range(steps):
        q_rows[s * heads : (s + 1) * heads, :] = q_t[s].T
    length = length_ref[0]
    lanes = new_rows.shape[0]
    fresh = lax.dot_general(
        q_rows[...], new_rows[...], (((1,), (1,)), ((), ())),
        preferred_element_type=jnp.float32,
    )
    step_of = lax.broadcasted_iota(jnp.int32, (rows, lanes), 0) // heads
    fresh = jnp.where(
        lax.broadcasted_iota(jnp.int32, (rows, lanes), 1) <= step_of, fresh, -1e30
    )
    recent[...] = fresh
    row_max[...] = fresh
    fetches = []
    for c in range(positions // chunk):
        copies[c].wait()
        if c == 0:
            fetches = fetch(stored, held, sems, 1 + positions // chunk)
        live = (lax.broadcasted_iota(jnp.int32, (1, chunk), 1) + c * chunk) < length
        for b in range(rows // block):
            span = slice(b * block, (b + 1) * block)
            s = jnp.dot(
                q_rows[span, :], kv_t[:, c * chunk : (c + 1) * chunk],
                preferred_element_type=jnp.float32,
            )
            s = jnp.where(live, s, -1e30)
            scores[span, c * chunk : (c + 1) * chunk] = s
            best = row_max[span, :]
            for j in range(chunk // lanes):
                best = jnp.maximum(best, s[:, j * lanes : (j + 1) * lanes])
            row_max[span, :] = best
    rate = score_scale * log2_e
    per_owner = out_ref.shape[1] // steps
    for b in range(rows // block):
        span = slice(b * block, (b + 1) * block)
        top = jnp.max(row_max[span, :], axis=1, keepdims=True) * rate
        fresh = jnp.exp2(recent[span, :] * rate - top)
        total = fresh
        fresh = fresh.astype(jnp.bfloat16)
        for c in range(positions // chunk):
            e = jnp.exp2(scores[span, c * chunk : (c + 1) * chunk] * rate - top)
            for j in range(chunk // lanes):
                total = total + e[:, j * lanes : (j + 1) * lanes]
            weights[span, c * chunk : (c + 1) * chunk] = e.astype(jnp.bfloat16)
        mixed = lax.dot_general(
            weights[span, :], kv_t[0:LAT, :], (((1,), (1,)), ((), ())),
            preferred_element_type=jnp.float32,
        ) + jnp.dot(fresh, new_rows[:, 0:LAT], preferred_element_type=jnp.float32)
        mixed = mixed / jnp.sum(total, axis=1, keepdims=True)
        for i in range(block // heads):
            s = b * (block // heads) + i
            part = mixed[i * heads : (i + 1) * heads, :]
            out_ref[:, s * per_owner : (s + 1) * per_owner, :] = part.reshape(
                heads // per_owner, per_owner, LAT
            ).astype(jnp.bfloat16)
    for copy in fetches:
        copy.wait()


def attend(queries, kv_cache, new_kv, lengths, owners, ahead):
    _, steps, heads, width = queries.shape
    positions = kv_cache.shape[1]
    rows = steps * heads
    chunk = 512
    lanes = 128
    block = 2 * heads
    return pl.pallas_call(
        functools.partial(attend_kernel, chunk=chunk, block=block, ahead=len(ahead)),
        out_shape=[jax.ShapeDtypeStruct((owners, rows // owners, LAT), jnp.bfloat16)]
        + [like(x) for x in ahead],
        in_specs=[SMEM] + [HBM] * (3 + len(ahead)),
        out_specs=[VMEM] * (1 + len(ahead)),
        scratch_shapes=[
            pltpu.VMEM((steps, width), jnp.bfloat16),
            pltpu.VMEM((steps, width, heads), jnp.bfloat16),
            pltpu.VMEM((rows, width), jnp.bfloat16),
            pltpu.VMEM((width, positions), jnp.bfloat16),
            pltpu.VMEM((lanes, width), jnp.bfloat16),
            pltpu.VMEM((rows, positions), jnp.float32),
            pltpu.VMEM((rows, lanes), jnp.float32),
            pltpu.VMEM((rows, positions), jnp.bfloat16),
            pltpu.VMEM((rows, lanes), jnp.float32),
            pltpu.SemaphoreType.DMA((2 + positions // chunk + len(ahead),)),
        ],
        compiler_params=params(16),
        name="attend",
    )(
        lengths,
        in_hbm(jnp.swapaxes(queries[0], 1, 2)),
        in_hbm(jnp.swapaxes(kv_cache[0], 0, 1)),
        in_hbm(new_kv[0]),
        *[in_hbm(x) for x in ahead],
    )


def project_kernel(
    latent_ref, up_ref, down_ref, *refs, depth, strip, ahead
):
    stored, kept_ref, sent_ref = refs[:ahead], refs[ahead], refs[ahead + 1]
    held, latents, sems = refs[ahead + 2 : 2 * ahead + 2], refs[2 * ahead + 2], refs[2 * ahead + 3]
    fetches = fetch(stored, held, sems, 0)
    sources, owned, _ = latent_ref.shape
    heads = up_ref.shape[0]
    steps = owned // heads
    items = sources * steps
    core = lax.axis_index("core")
    place = 0
    for side in (core, 1 - core):
        for column in range(sources // (2 * depth)):
            for t in range(depth):
                source = (column * 2 + side) * depth + t
                block = latent_ref[source].astype(jnp.float32)
                for j in range(LAT // 128):
                    latents[j, place * owned : (place + 1) * owned, :] = block[
                        :, j * 128 : (j + 1) * 128
                    ]
                place += 1
    vals = []
    for h in range(heads):
        x = jnp.concatenate(
            [latents[j, pl.ds(h, items, stride=heads), :] for j in range(LAT // 128)], axis=1
        ).astype(jnp.bfloat16)
        vals.append(
            jnp.dot(x, up_ref[h], preferred_element_type=jnp.float32).astype(jnp.bfloat16)
        )
    vals = jnp.concatenate(vals, axis=1)
    width = down_ref.shape[1]
    half = items // 2
    for n in range(width // strip):
        cols = slice(n * strip, (n + 1) * strip)
        part = jnp.dot(vals, down_ref[:, cols], preferred_element_type=jnp.float32)
        kept_ref[:, cols] = part[:half]
        sent_ref[:, cols] = part[half:].astype(jnp.bfloat16)
    for copy in fetches:
        copy.wait()


def project(by_head, value_up, out_proj, depth, ahead):
    sources, owned, _ = by_head.shape
    heads, _, value_width = value_up.shape
    width = out_proj.shape[2]
    half = sources * owned // heads // 2
    return pl.pallas_call(
        functools.partial(project_kernel, depth=depth, strip=512, ahead=len(ahead)),
        out_shape=[
            jax.ShapeDtypeStruct((half, width), jnp.float32),
            jax.ShapeDtypeStruct((half, width), jnp.bfloat16),
        ]
        + [like(x) for x in ahead],
        in_specs=[VMEM, VMEM, VMEM] + [HBM] * len(ahead),
        out_specs=[VMEM] * (2 + len(ahead)),
        scratch_shapes=[
            pltpu.VMEM((LAT // 128, sources * owned, 128), jnp.float32),
            pltpu.SemaphoreType.DMA((max(1, len(ahead)),)),
        ],
        compiler_params=params(8),
        name="project",
    )(
        by_head, value_up, out_proj.reshape(heads * value_width, width),
        *[in_hbm(x) for x in ahead],
    )


def merge_kernel(kept_ref, got_ref, out_ref):
    chips, items, _ = out_ref.shape
    total = kept_ref[...] + got_ref[...].astype(jnp.float32)
    for j in range(chips):
        out_ref[j] = total[j * items : (j + 1) * items, :].astype(jnp.bfloat16)


def merge(kept, got, chips):
    rows, width = kept.shape
    return pl.pallas_call(
        merge_kernel,
        out_shape=jax.ShapeDtypeStruct((chips, rows // chips, width), jnp.bfloat16),
        in_specs=[VMEM, VMEM],
        out_specs=VMEM,
        compiler_params=params(4),
        name="merge",
    )(kept, got)


def norm_kernel(ids_ref, parts_ref, hidden_ref, gain_ref, router_ref, residual_ref, out_ref):
    chips, items, _ = parts_ref.shape
    width = hidden_ref.shape[1]
    experts = router_ref.shape[0]
    spare = out_ref.shape[2] - width
    place = lax.axis_index("tp")
    total = hidden_ref[...].astype(jnp.float32)
    attention = parts_ref[0].astype(jnp.float32)
    for j in range(1, chips):
        attention = attention + parts_ref[j].astype(jnp.float32)
    residual = total + attention
    residual_ref[...] = residual
    square = jnp.mean(residual * residual, axis=1, keepdims=True)
    normed = (residual * lax.rsqrt(square + norm_eps) * gain_ref[...].astype(jnp.float32).reshape(1, width)).astype(
        jnp.bfloat16
    )
    lane = lax.broadcasted_iota(jnp.int32, (items, experts), 1)
    exact = normed.astype(jnp.float32)
    logits = jnp.zeros((items, experts), jnp.float32)
    for e in range(experts):
        column = router_ref[e : e + 1, :].astype(jnp.float32)
        logits = jnp.where(lane == e, jnp.sum(exact * column, axis=1, keepdims=True), logits)
    affinity = 1.0 / (1.0 + jnp.exp(-logits))
    ids = ids_ref[place]
    own = lax.broadcasted_iota(jnp.int32, (items, items), 0) == lax.broadcasted_iota(
        jnp.int32, (items, items), 1
    )
    chosen = jnp.zeros((items, experts), jnp.float32)
    for k in range(ids.shape[0]):
        named = jnp.sum(jnp.where(own, ids[k : k + 1, :], 0), axis=1, keepdims=True)
        chosen = chosen + (lane == named).astype(jnp.float32)
    scored = chosen * affinity
    gates = route_scale * scored / jnp.sum(scored, axis=1, keepdims=True)
    high = gates.astype(jnp.bfloat16)
    low = (gates - high.astype(jnp.float32)).astype(jnp.bfloat16)
    tail = jnp.concatenate(
        [high.astype(jnp.float32), low.astype(jnp.float32),
         jnp.zeros((items, spare - 2 * experts), jnp.float32)], axis=1
    ).astype(jnp.bfloat16)
    for j in range(chips):
        out_ref[j, :, 0:width] = normed
        out_ref[j, :, width:] = tail


def norm_rows(ids, parts, hidden, gain, router):
    chips, items, width = parts.shape
    experts = router.shape[1]
    spare = -(-2 * experts // 128) * 128
    return pl.pallas_call(
        norm_kernel,
        out_shape=(
            jax.ShapeDtypeStruct((items, width), jnp.float32),
            jax.ShapeDtypeStruct((chips, items, width + spare), jnp.bfloat16),
        ),
        in_specs=[VMEM] * 5,
        out_specs=(VMEM, VMEM),
        compiler_params=params(8),
        name="norm_rows",
    )(ids, parts, hidden, gain, router.T)


def experts_kernel(
    mine_ref, other_ref, in_ref, out_w_ref, s_in_ref, s_out_ref,
    kept_ref, sent_ref, tokens, tails, own, *, depth, experts, strip,
):
    chips, items, padded = mine_ref.shape
    width = out_w_ref.shape[1]
    half = chips * items
    core, column = lax.axis_index("core"), lax.axis_index("epx")
    for side, ref in enumerate((mine_ref, other_ref)):
        for j in range(chips):
            rows = slice(side * half + j * items, side * half + (j + 1) * items)
            block = ref[j].astype(jnp.float32)
            tokens[rows, :] = block[:, :width]
            tails[rows, :] = block[:, width:]
    x = tokens[...].astype(jnp.bfloat16)
    here = column * 2 + core
    lane = lax.broadcasted_iota(jnp.int32, tails.shape, 1)
    gate = jnp.sum(
        jnp.where((lane == here) | (lane == here + experts), tails[...], 0.0),
        axis=1, keepdims=True,
    )
    g = jnp.dot(x, in_ref[0], preferred_element_type=jnp.float32)
    u = jnp.dot(x, in_ref[1], preferred_element_type=jnp.float32)
    act = (g / (1.0 + jnp.exp(-g)) * u).astype(jnp.bfloat16)
    start = pl.multiple_of(column * (depth * items), depth * items)
    xs = tokens[pl.ds(start, depth * items), :].astype(jnp.bfloat16)
    sg = jnp.dot(xs, s_in_ref[0], preferred_element_type=jnp.float32)
    su = jnp.dot(xs, s_in_ref[1], preferred_element_type=jnp.float32)
    s_act = (sg / (1.0 + jnp.exp(-sg)) * su).astype(jnp.bfloat16)
    for n in range(width // strip):
        cols = slice(n * strip, (n + 1) * strip)
        y = gate * jnp.dot(act, out_w_ref[:, cols], preferred_element_type=jnp.float32)
        ys = jnp.dot(s_act, s_out_ref[:, cols], preferred_element_type=jnp.float32)
        sent_ref[:, cols] = y[half:].astype(jnp.bfloat16)
        kept_ref[:, cols] = y[:half]
        kept_ref[pl.ds(start, depth * items), cols] = (
            kept_ref[pl.ds(start, depth * items), cols] + ys
        )


def run_experts(mine, other, expert_in, expert_out, shared_in, shared_out, depth, experts):
    chips, items, padded = mine.shape
    width = expert_out.shape[1]
    half = chips * items
    return pl.pallas_call(
        functools.partial(experts_kernel, depth=depth, experts=experts, strip=512),
        out_shape=(
            jax.ShapeDtypeStruct((half, width), jnp.float32),
            jax.ShapeDtypeStruct((half, width), jnp.bfloat16),
        ),
        in_specs=[VMEM] * 6,
        out_specs=(VMEM, VMEM),
        scratch_shapes=[
            pltpu.VMEM((2 * half, width), jnp.float32),
            pltpu.VMEM((2 * half, padded - width), jnp.float32),
            pltpu.VMEM((depth * items, width), jnp.bfloat16),
        ],
        compiler_params=params(8),
        name="experts",
    )(mine, other, expert_in, expert_out, shared_in, shared_out)


def finish_kernel(parts_ref, residual_ref, out_ref):
    total = residual_ref[...]
    for j in range(parts_ref.shape[0]):
        total = total + parts_ref[j].astype(jnp.float32)
    out_ref[...] = total.astype(jnp.bfloat16)


def finish(parts, residual):
    return pl.pallas_call(
        finish_kernel,
        out_shape=jax.ShapeDtypeStruct(residual.shape, jnp.bfloat16),
        in_specs=[VMEM, VMEM],
        out_specs=VMEM,
        compiler_params=params(8),
        name="finish",
    )(parts, residual)


def swap_cores(x):
    return lax.ppermute(x, "core", [(0, 1), (1, 0)])


def chip_exchange(x):
    return lax.all_to_all(x, CHIPS, split_axis=0, concat_axis=0, tiled=True)


def attend_block(queries, kv_cache, new_kv, lengths):
    rows_here, steps_here, heads_here, kv_width = queries.shape
    positions = kv_cache.shape[1]
    cached = (
        jnp.einsum("rshk,rck->rshc", queries, kv_cache, preferred_element_type=jnp.float32)
        * score_scale
    )
    recent = (
        jnp.einsum("rshk,rjk->rshj", queries, new_kv, preferred_element_type=jnp.float32)
        * score_scale
    )
    cache_live = lax.broadcasted_iota(jnp.int32, (rows_here, positions), 1) < lengths[:, None]
    causal = lax.broadcasted_iota(jnp.int32, (steps_here, steps_here), 1) <= lax.broadcasted_iota(
        jnp.int32, (steps_here, steps_here), 0
    )
    cached = jnp.where(cache_live[:, None, None, :], cached, -1e30)
    recent = jnp.where(causal[None, :, None, :], recent, -1e30)
    highest = jnp.maximum(cached.max(-1), recent.max(-1))[..., None]
    cached_exp = jnp.exp(cached - highest)
    recent_exp = jnp.exp(recent - highest)
    denominator = cached_exp.sum(-1, keepdims=True) + recent_exp.sum(-1, keepdims=True)
    cached_prob = (cached_exp / denominator).astype(jnp.bfloat16)
    recent_prob = (recent_exp / denominator).astype(jnp.bfloat16)
    combined = jnp.einsum(
        "rshc,rck->rshk", cached_prob, kv_cache, preferred_element_type=jnp.float32
    )
    combined = combined + jnp.einsum(
        "rshj,rjk->rshk", recent_prob, new_kv, preferred_element_type=jnp.float32
    )
    return combined[..., :LAT].astype(jnp.bfloat16)


def sum_at_rows(kept, sent, chips):
    half = kept + swap_cores(sent.astype(jnp.bfloat16)).astype(jnp.float32)
    width = half.shape[1]
    parts = chip_exchange(half.astype(jnp.bfloat16).reshape(chips, -1, width))
    return jnp.sum(parts.astype(jnp.float32), axis=0)


def plain_device(
    hidden_in,
    queries,
    kv_cache,
    new_kv,
    lengths,
    expert_ids,
    value_up,
    out_proj,
    norm_gain,
    router,
    expert_in,
    expert_out,
    shared_in,
    shared_out,
):
    rows_here, steps_here, model_width = hidden_in.shape
    items = rows_here * steps_here
    columns = lax.axis_size("epx")
    depth = lax.axis_size("tp")
    chips = columns * depth
    core = lax.axis_index("core")
    column = lax.axis_index("epx")
    place = lax.axis_index("tp")
    expert_count = router.shape[1]

    latent_out = attend_block(queries, kv_cache, new_kv, lengths)
    by_head = lax.all_to_all(latent_out, ALL, split_axis=2, concat_axis=0, tiled=True)
    head_vals = jnp.einsum(
        "rshl,hlv->rshv", by_head, value_up, preferred_element_type=jnp.float32
    ).astype(jnp.bfloat16)
    partial = jnp.einsum(
        "rshv,hvd->rsd", head_vals, out_proj, preferred_element_type=jnp.float32
    ).reshape(columns, 2, depth * items, model_width)
    kept = lax.dynamic_index_in_dim(partial, core, 1, keepdims=False)
    sent = lax.dynamic_index_in_dim(partial, 1 - core, 1, keepdims=False)
    attention = sum_at_rows(
        kept.reshape(-1, model_width), sent.reshape(-1, model_width), chips
    )
    residual = hidden_in.reshape(items, model_width).astype(jnp.float32) + attention
    mean_square = jnp.mean(residual * residual, axis=-1, keepdims=True)
    normed = (residual * lax.rsqrt(mean_square + norm_eps) * norm_gain.astype(jnp.float32)).astype(
        jnp.bfloat16
    )
    affinity = jax.nn.sigmoid(jnp.dot(normed, router, preferred_element_type=jnp.float32))
    picked = lax.dynamic_slice_in_dim(expert_ids, place * rows_here, rows_here, 0).reshape(
        items, expert_ids.shape[2]
    )
    expert_iota = lax.broadcasted_iota(jnp.int32, (1, 1, expert_count), 2)
    chosen = jnp.sum((picked[:, :, None] == expert_iota).astype(jnp.float32), axis=1)
    scored = chosen * affinity
    gate_weight = route_scale * scored / jnp.sum(scored, axis=-1, keepdims=True)
    gate_high = gate_weight.astype(jnp.bfloat16)
    gate_low = (gate_weight - gate_high.astype(jnp.float32)).astype(jnp.bfloat16)
    spare = -(2 * expert_count) % 128
    payload = jnp.concatenate(
        [normed, gate_high, gate_low, jnp.zeros((items, spare), jnp.bfloat16)], axis=1
    )
    mine = chip_exchange(jnp.broadcast_to(payload[None], (chips,) + payload.shape)).reshape(
        chips * items, -1
    )
    tokens = jnp.concatenate([mine, swap_cores(mine)], axis=0)
    block_items = tokens[:, :model_width]
    expert_here = column * 2 + core
    gate_pairs = tokens[:, model_width : model_width + 2 * expert_count].astype(jnp.float32)
    gates = gate_pairs[:, :expert_count] + gate_pairs[:, expert_count:]
    gate_here = lax.dynamic_slice_in_dim(gates, expert_here, 1, 1)

    gate_part = jnp.dot(block_items, expert_in[0, 0], preferred_element_type=jnp.float32)
    up_part = jnp.dot(block_items, expert_in[0, 1], preferred_element_type=jnp.float32)
    activated = (jax.nn.silu(gate_part) * up_part).astype(jnp.bfloat16)
    routed = gate_here * jnp.dot(activated, expert_out[0], preferred_element_type=jnp.float32)

    own = lax.dynamic_slice_in_dim(mine, column * depth * items, depth * items, 0)[
        :, :model_width
    ]
    shared_gate = jnp.dot(own, shared_in[0], preferred_element_type=jnp.float32)
    shared_up = jnp.dot(own, shared_in[1], preferred_element_type=jnp.float32)
    shared_act = (jax.nn.silu(shared_gate) * shared_up).astype(jnp.bfloat16)
    shared_part = jnp.dot(shared_act, shared_out, preferred_element_type=jnp.float32)

    kept = routed[: chips * items].reshape(columns, depth * items, model_width)
    at_column = lax.broadcasted_iota(jnp.int32, (columns, 1, 1), 0) == column
    kept = kept + jnp.where(at_column, shared_part[None], 0.0)
    expert_sum = sum_at_rows(
        kept.reshape(-1, model_width), routed[chips * items :], chips
    )
    layer_out = (residual + expert_sum).astype(jnp.bfloat16)
    return layer_out.reshape(rows_here, steps_here, model_width)


def on_device(
    hidden_in,
    queries,
    kv_cache,
    new_kv,
    lengths,
    expert_ids,
    value_up,
    out_proj,
    norm_gain,
    router,
    expert_in,
    expert_out,
    shared_in,
    shared_out,
):
    rows_here, steps_here, model_width = hidden_in.shape
    items = rows_here * steps_here
    columns = lax.axis_size("epx")
    depth = lax.axis_size("tp")
    chips = columns * depth
    owners = 2 * chips
    experts = router.shape[1]

    latent_out, out_proj, value_up = attend(
        queries, kv_cache, new_kv, lengths, owners, [out_proj, value_up]
    )
    expert_in, expert_out = expert_in[0], expert_out[0]
    by_head = lax.all_to_all(latent_out, ALL, split_axis=0, concat_axis=0, tiled=True)
    kept, sent = project(
        by_head, value_up, out_proj, depth, []
    )
    parts = chip_exchange(merge(kept, swap_cores(sent), chips))
    ids = jnp.swapaxes(expert_ids, 1, 2)
    residual, handed = norm_rows(
        ids, parts, hidden_in.reshape(items, model_width), norm_gain, router
    )
    mine = chip_exchange(handed)
    kept, sent = run_experts(
        mine, swap_cores(mine), expert_in, expert_out, shared_in, shared_out, depth, experts,
    )
    parts = chip_exchange(merge(kept, swap_cores(sent), chips))
    return finish(parts, residual).reshape(rows_here, steps_here, model_width)


def choose(*args):
    owners = 2 * lax.axis_size("epx") * lax.axis_size("tp")
    queries = args[1]
    whole_tiles = queries.shape[0] == 1 and queries.shape[2] % (8 * owners) == 0
    return on_device(*args) if whole_tiles else plain_device(*args)


def solution(mesh):
    sizes = mesh.shape
    fine = Mesh(
        mesh.devices.reshape(sizes["groups"], sizes["ep"] // 2, 2, sizes["tp"]),
        ("groups", "epx", "core", "tp"),
    )
    ep = ("epx", "core")
    rows = ("groups", "epx", "core", "tp")
    in_specs = (
        P(rows, None, None),
        P(rows, None, None, None),
        P(rows, None, None),
        P(rows, None, None),
        P(rows),
        P(("groups",) + ep, None, None),
        P(ALL, None, None),
        P(ALL, None, None),
        P(),
        P(),
        P(ep, None, None, "tp"),
        P(ep, "tp", None),
        P(None, None, "tp"),
        P("tp", None),
    )
    out_specs = P(rows, None, None)
    return jax.shard_map(
        choose, mesh=fine, in_specs=in_specs, out_specs=out_specs, check_vma=False
    )
```

```python
import functools

import jax
import jax.numpy as jnp
from jax import lax
from jax.experimental import pallas as pl
from jax.experimental.pallas import tpu as pltpu
from jax.sharding import Mesh
from jax.sharding import PartitionSpec as P

LAT = 512


score_scale = 192.0 ** (-0.5)
log2_e = 1.4426950408889634
route_scale = 2.5
norm_eps = 1e-06

CHIPS = ("epx", "tp")
ALL = ("epx", "core", "tp")
VMEM = pl.BlockSpec(memory_space=pltpu.VMEM)
SMEM = pl.BlockSpec(memory_space=pltpu.SMEM)
HBM = pl.BlockSpec(memory_space=pltpu.HBM)


def params(mib):
    return pltpu.CompilerParams(vmem_limit_bytes=mib << 20)


def fetch(stored, held, sems, first):
    copies = [
        pltpu.make_async_copy(a, b, sems.at[first + i])
        for i, (a, b) in enumerate(zip(stored, held))
    ]
    for copy in copies:
        copy.start()
    return copies


def in_hbm(x):
    return pltpu.with_memory_space_constraint(x, pltpu.HBM)


def like(x):
    return jax.ShapeDtypeStruct(x.shape, x.dtype)


def attend_kernel(length_ref, q_hbm, kv_hbm, new_hbm, *refs, chunk, block, depth, ahead):
    stored, out_ref, held = refs[:ahead], refs[ahead], refs[ahead + 1 : 2 * ahead + 1]
    new_ref, q_t, q_rows, kv_t, new_rows, scores, weights, row_max, mixed, sems = refs[
        2 * ahead + 1 :
    ]
    steps, width, heads = q_t.shape
    positions = kv_t.shape[1]
    rows = steps * heads
    blocks = rows // block
    per_block = block // heads
    chunks = positions // chunk
    lanes = new_rows.shape[0]
    q_copies = [
        pltpu.make_async_copy(
            q_hbm.at[pl.ds(b * per_block, per_block)],
            q_t.at[pl.ds(b * per_block, per_block)],
            sems.at[b],
        )
        for b in range(blocks)
    ]
    kv_copies = [
        pltpu.make_async_copy(
            kv_hbm.at[:, pl.ds(c * chunk, chunk)],
            kv_t.at[:, pl.ds(c * chunk, chunk)],
            sems.at[blocks + c],
        )
        for c in range(chunks)
    ]
    new_copy = pltpu.make_async_copy(new_hbm, new_ref, sems.at[blocks + chunks])
    q_copies[0].start()
    kv_copies[0].start()
    new_copy.start()
    for copy in q_copies[1:] + kv_copies[1:]:
        copy.start()
    new_rows[...] = jnp.zeros_like(new_rows)
    new_copy.wait()
    new_rows[0:steps, :] = new_ref[...]
    length = length_ref[0]
    rate = score_scale * log2_e
    per_owner = out_ref.shape[1] // (2 * steps)

    def turn(b):
        q_copies[b].wait()
        for i in range(per_block):
            s = b * per_block + i
            q_rows[s * heads : (s + 1) * heads, :] = q_t[s].T

    def score(b, c):
        span = slice(b * block, (b + 1) * block)
        s = jnp.dot(
            q_rows[span, :], kv_t[:, c * chunk : (c + 1) * chunk],
            preferred_element_type=jnp.float32,
        )
        live = (lax.broadcasted_iota(jnp.int32, (1, chunk), 1) + c * chunk) < length
        s = jnp.where(live, s, -1e30)
        scores[span, c * chunk : (c + 1) * chunk] = s
        best = s[:, 0:lanes] if c == 0 else jnp.maximum(row_max[span, :], s[:, 0:lanes])
        for j in range(1, chunk // lanes):
            best = jnp.maximum(best, s[:, j * lanes : (j + 1) * lanes])
        row_max[span, :] = best

    def peak(b):
        span = slice(b * block, (b + 1) * block)
        fresh = lax.dot_general(
            q_rows[span, :], new_rows[...], (((1,), (1,)), ((), ())),
            preferred_element_type=jnp.float32,
        )
        step_of = b * per_block + lax.broadcasted_iota(jnp.int32, (block, lanes), 0) // heads
        fresh = jnp.where(
            lax.broadcasted_iota(jnp.int32, (block, lanes), 1) <= step_of, fresh, -1e30
        )
        top = jnp.max(jnp.maximum(row_max[span, :], fresh), axis=1, keepdims=True) * rate
        fresh = jnp.exp2(fresh * rate - top)
        return [top, fresh, fresh.astype(jnp.bfloat16)]

    def soften(b, c, state):
        span = slice(b * block, (b + 1) * block)
        e = jnp.exp2(scores[span, c * chunk : (c + 1) * chunk] * rate - state[0])
        for j in range(chunk // lanes):
            state[1] = state[1] + e[:, j * lanes : (j + 1) * lanes]
        weights[span, c * chunk : (c + 1) * chunk] = e.astype(jnp.bfloat16)

    def mix(b, first, last, state):
        span = slice(b * block, (b + 1) * block)
        part = lax.dot_general(
            weights[span, first * chunk : last * chunk],
            kv_t[0:LAT, first * chunk : last * chunk],
            (((1,), (1,)), ((), ())),
            preferred_element_type=jnp.float32,
        )
        if first == 0:
            part = part + jnp.dot(
                state[2], new_rows[:, 0:LAT], preferred_element_type=jnp.float32
            )
        else:
            part = part + mixed[...]
        if last < chunks:
            mixed[...] = part
            return
        part = part * (1.0 / jnp.sum(state[1], axis=1, keepdims=True))
        for i in range(per_block):
            s = b * per_block + i
            for d in range(heads // per_owner):
                column, side, t = d // (2 * depth), d // depth % 2, d % depth
                row = (side * steps + s) * per_owner
                first_row = i * heads + d * per_owner
                out_ref[column * depth + t, row : row + per_owner, :] = part[
                    first_row : first_row + per_owner, :
                ].astype(jnp.bfloat16)

    states = {}
    fetches = []
    turn(0)
    for stage in range(blocks + 2):
        mixing = stage - 2
        if mixing >= 0 and stage - 1 >= blocks:
            mix(mixing, 0, chunks, states[mixing])
            continue
        for c in range(chunks):
            if stage < blocks:
                if stage == 0:
                    kv_copies[c].wait()
                    if c == 0:
                        fetches = fetch(stored, held, sems, blocks + chunks + 1)
                score(stage, c)
                if c == 0 and stage + 1 < blocks:
                    turn(stage + 1)
            if 0 <= stage - 1 < blocks:
                soften(stage - 1, c, states[stage - 1])
            if mixing >= 0 and c % 2 == 1:
                mix(mixing, c - 1, c + 1, states[mixing])
        if stage < blocks:
            states[stage] = peak(stage)
    for copy in fetches:
        copy.wait()


def attend(queries, kv_cache, new_kv, lengths, chips, depth, ahead, chunk=512):
    _, steps, heads, width = queries.shape
    positions = kv_cache.shape[1]
    rows = steps * heads
    lanes = 128
    block = 2 * heads
    return pl.pallas_call(
        functools.partial(
            attend_kernel, chunk=chunk, block=block, depth=depth, ahead=len(ahead)
        ),
        out_shape=[jax.ShapeDtypeStruct((chips, rows // chips, LAT), jnp.bfloat16)]
        + [like(x) for x in ahead],
        in_specs=[SMEM] + [HBM] * (3 + len(ahead)),
        out_specs=[VMEM] * (1 + len(ahead)),
        scratch_shapes=[
            pltpu.VMEM((steps, width), jnp.bfloat16),
            pltpu.VMEM((steps, width, heads), jnp.bfloat16),
            pltpu.VMEM((rows, width), jnp.bfloat16),
            pltpu.VMEM((width, positions), jnp.bfloat16),
            pltpu.VMEM((lanes, width), jnp.bfloat16),
            pltpu.VMEM((rows, positions), jnp.float32),
            pltpu.VMEM((rows, positions), jnp.bfloat16),
            pltpu.VMEM((rows, lanes), jnp.float32),
            pltpu.VMEM((block, LAT), jnp.float32),
            pltpu.SemaphoreType.DMA((rows // block + positions // chunk + 1 + len(ahead),)),
        ],
        compiler_params=params(20),
        name="attend",
    )(
        lengths,
        in_hbm(jnp.swapaxes(queries[0], 1, 2)),
        in_hbm(jnp.swapaxes(kv_cache[0], 0, 1)),
        in_hbm(new_kv[0]),
        *[in_hbm(x) for x in ahead],
    )


def project_kernel(latent_ref, up_ref, up2_ref, down_ref, down2_ref, out_ref, latents, *, strip):
    sources, owned, _ = latent_ref.shape
    heads = up_ref.shape[0]
    owned = owned // 2
    steps = owned // heads
    items = sources * steps
    core = lax.axis_index("core")
    blocks = LAT // 128
    vals = []
    for side, w_ref in enumerate((up_ref, up2_ref)):
        start = pl.multiple_of((core if side == 0 else 1 - core) * owned, owned)
        for source in range(sources):
            block = latent_ref[source, pl.ds(start, owned), :].astype(jnp.float32)
            for j in range(blocks):
                latents[side * blocks + j, source * owned : (source + 1) * owned, :] = block[
                    :, j * 128 : (j + 1) * 128
                ]
        for h in range(heads):
            x = jnp.concatenate(
                [
                    latents[side * blocks + j, pl.ds(h, items, stride=heads), :]
                    for j in range(blocks)
                ],
                axis=1,
            ).astype(jnp.bfloat16)
            vals.append(
                jnp.dot(x, w_ref[h], preferred_element_type=jnp.float32).astype(jnp.bfloat16)
            )
    own = jnp.concatenate(vals[:heads], axis=1)
    partner = jnp.concatenate(vals[heads:], axis=1)
    width = down_ref.shape[1]
    for n in range(width // strip):
        cols = slice(n * strip, (n + 1) * strip)
        part = jnp.dot(own, down_ref[:, cols], preferred_element_type=jnp.float32)
        part = part + jnp.dot(partner, down2_ref[:, cols], preferred_element_type=jnp.float32)
        for j in range(sources):
            out_ref[j, :, cols] = part[j * steps : (j + 1) * steps].astype(jnp.bfloat16)


def project(by_head, value_up, value_up2, out_proj, out_proj2):
    sources, owned, _ = by_head.shape
    heads, _, value_width = value_up.shape
    width = out_proj.shape[2]
    flat = (heads * value_width, width)
    return pl.pallas_call(
        functools.partial(project_kernel, strip=512),
        out_shape=jax.ShapeDtypeStruct((sources, owned // (2 * heads), width), jnp.bfloat16),
        in_specs=[VMEM] * 5,
        out_specs=VMEM,
        scratch_shapes=[
            pltpu.VMEM((2 * LAT // 128, sources * owned // 2, 128), jnp.float32),
        ],
        compiler_params=params(8),
        name="project",
    )(by_head, value_up, value_up2, out_proj.reshape(flat), out_proj2.reshape(flat))


def norm_kernel(ids_ref, parts_ref, hidden_ref, gain_ref, router_ref, residual_ref, out_ref):
    chips, items, _ = parts_ref.shape
    width = hidden_ref.shape[1]
    experts = router_ref.shape[0]
    spare = out_ref.shape[2] - width
    place = lax.axis_index("tp")
    total = hidden_ref[...].astype(jnp.float32)
    attention = parts_ref[0].astype(jnp.float32)
    for j in range(1, chips):
        attention = attention + parts_ref[j].astype(jnp.float32)
    residual = total + attention
    residual_ref[...] = residual
    square = jnp.mean(residual * residual, axis=1, keepdims=True)
    normed = (residual * lax.rsqrt(square + norm_eps) * gain_ref[...].astype(jnp.float32).reshape(1, width)).astype(
        jnp.bfloat16
    )
    lane = lax.broadcasted_iota(jnp.int32, (items, experts), 1)
    exact = normed.astype(jnp.float32)
    logits = jnp.zeros((items, experts), jnp.float32)
    for e in range(experts):
        column = router_ref[e : e + 1, :].astype(jnp.float32)
        logits = jnp.where(lane == e, jnp.sum(exact * column, axis=1, keepdims=True), logits)
    affinity = 1.0 / (1.0 + jnp.exp(-logits))
    ids = ids_ref[place]
    own = lax.broadcasted_iota(jnp.int32, (items, items), 0) == lax.broadcasted_iota(
        jnp.int32, (items, items), 1
    )
    chosen = jnp.zeros((items, experts), jnp.float32)
    for k in range(ids.shape[0]):
        named = jnp.sum(jnp.where(own, ids[k : k + 1, :], 0), axis=1, keepdims=True)
        chosen = chosen + (lane == named).astype(jnp.float32)
    scored = chosen * affinity
    gates = route_scale * scored / jnp.sum(scored, axis=1, keepdims=True)
    high = gates.astype(jnp.bfloat16)
    low = (gates - high.astype(jnp.float32)).astype(jnp.bfloat16)
    tail = jnp.concatenate(
        [high.astype(jnp.float32), low.astype(jnp.float32),
         jnp.zeros((items, spare - 2 * experts), jnp.float32)], axis=1
    ).astype(jnp.bfloat16)
    for j in range(chips):
        out_ref[j, :, 0:width] = normed
        out_ref[j, :, width:] = tail


def norm_rows(ids, parts, hidden, gain, router):
    chips, items, width = parts.shape
    experts = router.shape[1]
    spare = -(-2 * experts // 128) * 128
    return pl.pallas_call(
        norm_kernel,
        out_shape=(
            jax.ShapeDtypeStruct((items, width), jnp.float32),
            jax.ShapeDtypeStruct((chips, items, width + spare), jnp.bfloat16),
        ),
        in_specs=[VMEM] * 5,
        out_specs=(VMEM, VMEM),
        compiler_params=params(8),
        name="norm_rows",
    )(ids, parts, hidden, gain, router.T)


def merge_kernel(kept_ref, got_ref, out_ref):
    chips, items, _ = out_ref.shape
    total = kept_ref[...] + got_ref[...].astype(jnp.float32)
    for j in range(chips):
        out_ref[j] = total[j * items : (j + 1) * items, :].astype(jnp.bfloat16)


def merge(kept, got, chips):
    rows, width = kept.shape
    return pl.pallas_call(
        merge_kernel,
        out_shape=jax.ShapeDtypeStruct((chips, rows // chips, width), jnp.bfloat16),
        in_specs=[VMEM, VMEM],
        out_specs=VMEM,
        compiler_params=params(4),
        name="merge",
    )(kept, got)


def silu_gate(g, u):
    return (g / (1.0 + jnp.exp(-g)) * u).astype(jnp.bfloat16)


def gather_rows(ref, first, tokens, tails):
    items = ref.shape[1]
    width = tokens.shape[1]
    for j in range(ref.shape[0]):
        rows = slice(first + j * items, first + (j + 1) * items)
        block = ref[j].astype(jnp.float32)
        tokens[rows, :] = block[:, :width]
        if tails is not None:
            tails[rows, :] = block[:, width:]


def shared_kernel(mine_ref, in_ref, out_w_ref, out_ref, tokens, *, strip):
    rows, width = out_ref.shape
    depth = rows // mine_ref.shape[1]
    column = lax.axis_index("epx")
    for t in range(depth):
        items = mine_ref.shape[1]
        tokens[t * items : (t + 1) * items, :] = mine_ref[column * depth + t].astype(
            jnp.float32
        )[:, :width]
    x = tokens[...].astype(jnp.bfloat16)
    g = jnp.dot(x, in_ref[0], preferred_element_type=jnp.float32)
    u = jnp.dot(x, in_ref[1], preferred_element_type=jnp.float32)
    act = silu_gate(g, u)
    for n in range(width // strip):
        cols = slice(n * strip, (n + 1) * strip)
        out_ref[:, cols] = jnp.dot(act, out_w_ref[:, cols], preferred_element_type=jnp.float32)


def run_shared(mine, shared_in, shared_out, depth):
    rows, width = depth * mine.shape[1], shared_out.shape[1]
    return pl.pallas_call(
        functools.partial(shared_kernel, strip=512),
        out_shape=jax.ShapeDtypeStruct((rows, width), jnp.float32),
        in_specs=[VMEM] * 3,
        out_specs=VMEM,
        scratch_shapes=[pltpu.VMEM((rows, width), jnp.float32)],
        compiler_params=params(6),
        name="shared",
    )(mine, shared_in, shared_out)


def routed_kernel(
    mine_ref, other_ref, in_ref, out_w_ref, sent_ref, act_ref, gate_ref, tokens, tails,
    *, experts, strip,
):
    half, width = sent_ref.shape
    core, column = lax.axis_index("core"), lax.axis_index("epx")
    gather_rows(mine_ref, 0, tokens, tails)
    gather_rows(other_ref, half, tokens, tails)
    x = tokens[...].astype(jnp.bfloat16)
    here = column * 2 + core
    lane = lax.broadcasted_iota(jnp.int32, tails.shape, 1)
    gate = jnp.sum(
        jnp.where((lane == here) | (lane == here + experts), tails[...], 0.0),
        axis=1, keepdims=True,
    )
    g = jnp.dot(x, in_ref[0], preferred_element_type=jnp.float32)
    u = jnp.dot(x, in_ref[1], preferred_element_type=jnp.float32)
    act = silu_gate(g, u)
    act_ref[...] = act[:half]
    gate_ref[...] = jnp.broadcast_to(gate[:half], gate_ref.shape)
    for n in range(width // strip):
        cols = slice(n * strip, (n + 1) * strip)
        y = gate[half:] * jnp.dot(
            act[half:], out_w_ref[:, cols], preferred_element_type=jnp.float32
        )
        sent_ref[:, cols] = y.astype(jnp.bfloat16)


def run_routed(mine, other, expert_in, expert_out, experts):
    chips, items, padded = mine.shape
    hidden, width = expert_out.shape
    half = chips * items
    return pl.pallas_call(
        functools.partial(routed_kernel, experts=experts, strip=512),
        out_shape=(
            jax.ShapeDtypeStruct((half, width), jnp.bfloat16),
            jax.ShapeDtypeStruct((half, hidden), jnp.bfloat16),
            jax.ShapeDtypeStruct((half, 128), jnp.float32),
        ),
        in_specs=[VMEM] * 4,
        out_specs=(VMEM, VMEM, VMEM),
        scratch_shapes=[
            pltpu.VMEM((2 * half, width), jnp.float32),
            pltpu.VMEM((2 * half, padded - width), jnp.float32),
        ],
        compiler_params=params(8),
        name="routed",
    )(mine, other, expert_in, expert_out)


def keep_kernel(act_ref, gate_ref, out_w_ref, shared_ref, kept_ref, *, strip):
    width = kept_ref.shape[1]
    rows = shared_ref.shape[0]
    start = pl.multiple_of(lax.axis_index("epx") * rows, rows)
    gate = gate_ref[:, 0:1]
    for n in range(width // strip):
        cols = slice(n * strip, (n + 1) * strip)
        kept_ref[:, cols] = gate * jnp.dot(
            act_ref[...], out_w_ref[:, cols], preferred_element_type=jnp.float32
        )
    kept_ref[pl.ds(start, rows), :] = kept_ref[pl.ds(start, rows), :] + shared_ref[...]


def run_keep(act, gate, expert_out, shared):
    return pl.pallas_call(
        functools.partial(keep_kernel, strip=512),
        out_shape=jax.ShapeDtypeStruct((act.shape[0], expert_out.shape[1]), jnp.float32),
        in_specs=[VMEM] * 4,
        out_specs=VMEM,
        compiler_params=params(6),
        name="keep",
    )(act, gate, expert_out, shared)


def finish_kernel(parts_ref, residual_ref, out_ref):
    total = residual_ref[...]
    for j in range(parts_ref.shape[0]):
        total = total + parts_ref[j].astype(jnp.float32)
    out_ref[...] = total.astype(jnp.bfloat16)


def finish(parts, residual):
    return pl.pallas_call(
        finish_kernel,
        out_shape=jax.ShapeDtypeStruct(residual.shape, jnp.bfloat16),
        in_specs=[VMEM, VMEM],
        out_specs=VMEM,
        compiler_params=params(8),
        name="finish",
    )(parts, residual)


def swap_cores(x):
    return lax.ppermute(x, "core", [(0, 1), (1, 0)])


def chip_exchange(x):
    return lax.all_to_all(x, CHIPS, split_axis=0, concat_axis=0, tiled=True)


def attend_block(queries, kv_cache, new_kv, lengths):
    rows_here, steps_here, heads_here, kv_width = queries.shape
    positions = kv_cache.shape[1]
    cached = (
        jnp.einsum("rshk,rck->rshc", queries, kv_cache, preferred_element_type=jnp.float32)
        * score_scale
    )
    recent = (
        jnp.einsum("rshk,rjk->rshj", queries, new_kv, preferred_element_type=jnp.float32)
        * score_scale
    )
    cache_live = lax.broadcasted_iota(jnp.int32, (rows_here, positions), 1) < lengths[:, None]
    causal = lax.broadcasted_iota(jnp.int32, (steps_here, steps_here), 1) <= lax.broadcasted_iota(
        jnp.int32, (steps_here, steps_here), 0
    )
    cached = jnp.where(cache_live[:, None, None, :], cached, -1e30)
    recent = jnp.where(causal[None, :, None, :], recent, -1e30)
    highest = jnp.maximum(cached.max(-1), recent.max(-1))[..., None]
    cached_exp = jnp.exp(cached - highest)
    recent_exp = jnp.exp(recent - highest)
    denominator = cached_exp.sum(-1, keepdims=True) + recent_exp.sum(-1, keepdims=True)
    cached_prob = (cached_exp / denominator).astype(jnp.bfloat16)
    recent_prob = (recent_exp / denominator).astype(jnp.bfloat16)
    combined = jnp.einsum(
        "rshc,rck->rshk", cached_prob, kv_cache, preferred_element_type=jnp.float32
    )
    combined = combined + jnp.einsum(
        "rshj,rjk->rshk", recent_prob, new_kv, preferred_element_type=jnp.float32
    )
    return combined[..., :LAT].astype(jnp.bfloat16)


def sum_at_rows(kept, sent, chips):
    half = kept + swap_cores(sent.astype(jnp.bfloat16)).astype(jnp.float32)
    width = half.shape[1]
    parts = chip_exchange(half.astype(jnp.bfloat16).reshape(chips, -1, width))
    return jnp.sum(parts.astype(jnp.float32), axis=0)


def plain_device(
    hidden_in,
    queries,
    kv_cache,
    new_kv,
    lengths,
    expert_ids,
    value_up,
    out_proj,
    norm_gain,
    router,
    expert_in,
    expert_out,
    shared_in,
    shared_out,
):
    rows_here, steps_here, model_width = hidden_in.shape
    items = rows_here * steps_here
    columns = lax.axis_size("epx")
    depth = lax.axis_size("tp")
    chips = columns * depth
    core = lax.axis_index("core")
    column = lax.axis_index("epx")
    place = lax.axis_index("tp")
    expert_count = router.shape[1]

    latent_out = attend_block(queries, kv_cache, new_kv, lengths)
    by_head = lax.all_to_all(latent_out, ALL, split_axis=2, concat_axis=0, tiled=True)
    head_vals = jnp.einsum(
        "rshl,hlv->rshv", by_head, value_up, preferred_element_type=jnp.float32
    ).astype(jnp.bfloat16)
    partial = jnp.einsum(
        "rshv,hvd->rsd", head_vals, out_proj, preferred_element_type=jnp.float32
    ).reshape(columns, 2, depth * items, model_width)
    kept = lax.dynamic_index_in_dim(partial, core, 1, keepdims=False)
    sent = lax.dynamic_index_in_dim(partial, 1 - core, 1, keepdims=False)
    attention = sum_at_rows(
        kept.reshape(-1, model_width), sent.reshape(-1, model_width), chips
    )
    residual = hidden_in.reshape(items, model_width).astype(jnp.float32) + attention
    mean_square = jnp.mean(residual * residual, axis=-1, keepdims=True)
    normed = (residual * lax.rsqrt(mean_square + norm_eps) * norm_gain.astype(jnp.float32)).astype(
        jnp.bfloat16
    )
    affinity = jax.nn.sigmoid(jnp.dot(normed, router, preferred_element_type=jnp.float32))
    picked = lax.dynamic_slice_in_dim(expert_ids, place * rows_here, rows_here, 0).reshape(
        items, expert_ids.shape[2]
    )
    expert_iota = lax.broadcasted_iota(jnp.int32, (1, 1, expert_count), 2)
    chosen = jnp.sum((picked[:, :, None] == expert_iota).astype(jnp.float32), axis=1)
    scored = chosen * affinity
    gate_weight = route_scale * scored / jnp.sum(scored, axis=-1, keepdims=True)
    gate_high = gate_weight.astype(jnp.bfloat16)
    gate_low = (gate_weight - gate_high.astype(jnp.float32)).astype(jnp.bfloat16)
    spare = -(2 * expert_count) % 128
    payload = jnp.concatenate(
        [normed, gate_high, gate_low, jnp.zeros((items, spare), jnp.bfloat16)], axis=1
    )
    mine = chip_exchange(jnp.broadcast_to(payload[None], (chips,) + payload.shape)).reshape(
        chips * items, -1
    )
    tokens = jnp.concatenate([mine, swap_cores(mine)], axis=0)
    block_items = tokens[:, :model_width]
    expert_here = column * 2 + core
    gate_pairs = tokens[:, model_width : model_width + 2 * expert_count].astype(jnp.float32)
    gates = gate_pairs[:, :expert_count] + gate_pairs[:, expert_count:]
    gate_here = lax.dynamic_slice_in_dim(gates, expert_here, 1, 1)

    gate_part = jnp.dot(block_items, expert_in[0, 0], preferred_element_type=jnp.float32)
    up_part = jnp.dot(block_items, expert_in[0, 1], preferred_element_type=jnp.float32)
    activated = (jax.nn.silu(gate_part) * up_part).astype(jnp.bfloat16)
    routed = gate_here * jnp.dot(activated, expert_out[0], preferred_element_type=jnp.float32)

    own = lax.dynamic_slice_in_dim(mine, column * depth * items, depth * items, 0)[
        :, :model_width
    ]
    shared_gate = jnp.dot(own, shared_in[0], preferred_element_type=jnp.float32)
    shared_up = jnp.dot(own, shared_in[1], preferred_element_type=jnp.float32)
    shared_act = (jax.nn.silu(shared_gate) * shared_up).astype(jnp.bfloat16)
    shared_part = jnp.dot(shared_act, shared_out, preferred_element_type=jnp.float32)

    kept = routed[: chips * items].reshape(columns, depth * items, model_width)
    at_column = lax.broadcasted_iota(jnp.int32, (columns, 1, 1), 0) == column
    kept = kept + jnp.where(at_column, shared_part[None], 0.0)
    expert_sum = sum_at_rows(
        kept.reshape(-1, model_width), routed[chips * items :], chips
    )
    layer_out = (residual + expert_sum).astype(jnp.bfloat16)
    return layer_out.reshape(rows_here, steps_here, model_width)


def on_device(
    hidden_in,
    queries,
    kv_cache,
    new_kv,
    lengths,
    expert_ids,
    value_up,
    out_proj,
    norm_gain,
    router,
    expert_in,
    expert_out,
    shared_in,
    shared_out,
):
    rows_here, steps_here, model_width = hidden_in.shape
    items = rows_here * steps_here
    columns = lax.axis_size("epx")
    depth = lax.axis_size("tp")
    chips = columns * depth
    experts = router.shape[1]

    value_up2 = swap_cores(value_up)
    out_proj2 = swap_cores(out_proj)
    expert_in, expert_out = expert_in[0], expert_out[0]
    latent_out, out_proj, value_up = attend(
        queries, kv_cache, new_kv, lengths, chips, depth, [out_proj, value_up]
    )
    by_head = chip_exchange(latent_out)
    parts = chip_exchange(project(by_head, value_up, value_up2, out_proj, out_proj2))
    ids = jnp.swapaxes(expert_ids, 1, 2)
    residual, handed = norm_rows(
        ids, parts, hidden_in.reshape(items, model_width), norm_gain, router
    )
    mine = chip_exchange(handed)
    other = swap_cores(mine)
    shared = run_shared(mine, shared_in, shared_out, depth)
    other, shared = lax.optimization_barrier((other, shared))
    sent, act, gate = run_routed(mine, other, expert_in, expert_out, experts)
    got = swap_cores(sent)
    kept = run_keep(act, gate, expert_out, shared)
    parts = chip_exchange(merge(kept, got, chips))
    return finish(parts, residual).reshape(rows_here, steps_here, model_width)


def choose(*args):
    owners = 2 * lax.axis_size("epx") * lax.axis_size("tp")
    queries = args[1]
    whole_tiles = queries.shape[0] == 1 and queries.shape[2] % (8 * owners) == 0
    return on_device(*args) if whole_tiles else plain_device(*args)


def solution(mesh):
    sizes = mesh.shape
    fine = Mesh(
        mesh.devices.reshape(sizes["groups"], sizes["ep"] // 2, 2, sizes["tp"]),
        ("groups", "epx", "core", "tp"),
    )
    ep = ("epx", "core")
    rows = ("groups", "epx", "core", "tp")
    in_specs = (
        P(rows, None, None),
        P(rows, None, None, None),
        P(rows, None, None),
        P(rows, None, None),
        P(rows),
        P(("groups",) + ep, None, None),
        P(ALL, None, None),
        P(ALL, None, None),
        P(),
        P(),
        P(ep, None, None, "tp"),
        P(ep, "tp", None),
        P(None, None, "tp"),
        P("tp", None),
    )
    out_specs = P(rows, None, None)
    return jax.shard_map(
        choose, mesh=fine, in_specs=in_specs, out_specs=out_specs, check_vma=False
    )
```

```python
import functools

import jax
import jax.numpy as jnp
from jax import lax
from jax.experimental import pallas as pl
from jax.experimental.pallas import tpu as pltpu
from jax.sharding import Mesh
from jax.sharding import PartitionSpec as P

LAT = 512


score_scale = 192.0 ** (-0.5)
log2_e = 1.4426950408889634
route_scale = 2.5
norm_eps = 1e-06

CHIPS = ("epx", "tp")
ALL = ("epx", "core", "tp")
VMEM = pl.BlockSpec(memory_space=pltpu.VMEM)
SMEM = pl.BlockSpec(memory_space=pltpu.SMEM)
HBM = pl.BlockSpec(memory_space=pltpu.HBM)


def params(mib):
    return pltpu.CompilerParams(vmem_limit_bytes=mib << 20)


def fetch(stored, held, sems, first):
    copies = [
        pltpu.make_async_copy(a, b, sems.at[first + i])
        for i, (a, b) in enumerate(zip(stored, held))
    ]
    for copy in copies:
        copy.start()
    return copies


def in_hbm(x):
    return pltpu.with_memory_space_constraint(x, pltpu.HBM)


def like(x):
    return jax.ShapeDtypeStruct(x.shape, x.dtype)


def attend_kernel(length_ref, q_hbm, kv_hbm, new_hbm, *refs, chunk, block, depth, ahead):
    stored, out_ref, held = refs[:ahead], refs[ahead], refs[ahead + 1 : 2 * ahead + 1]
    new_ref, q_t, q_rows, kv_t, new_rows, scores, weights, row_max, mixed, sems = refs[
        2 * ahead + 1 :
    ]
    steps, width, heads = q_t.shape
    positions = kv_t.shape[1]
    rows = steps * heads
    blocks = rows // block
    per_block = block // heads
    chunks = positions // chunk
    lanes = new_rows.shape[0]
    q_copies = [
        pltpu.make_async_copy(
            q_hbm.at[pl.ds(b * per_block, per_block)],
            q_t.at[pl.ds(b * per_block, per_block)],
            sems.at[b],
        )
        for b in range(blocks)
    ]
    kv_copies = [
        pltpu.make_async_copy(
            kv_hbm.at[:, pl.ds(c * chunk, chunk)],
            kv_t.at[:, pl.ds(c * chunk, chunk)],
            sems.at[blocks + c],
        )
        for c in range(chunks)
    ]
    new_copy = pltpu.make_async_copy(new_hbm, new_ref, sems.at[blocks + chunks])
    q_copies[0].start()
    kv_copies[0].start()
    new_copy.start()
    for copy in q_copies[1:] + kv_copies[1:]:
        copy.start()
    new_rows[...] = jnp.zeros_like(new_rows)
    new_copy.wait()
    new_rows[0:steps, :] = new_ref[...]
    length = length_ref[0]
    rate = score_scale * log2_e
    per_owner = out_ref.shape[1] // (2 * steps)

    def turn(b):
        q_copies[b].wait()
        for i in range(per_block):
            s = b * per_block + i
            q_rows[s * heads : (s + 1) * heads, :] = q_t[s].T

    def score(b, c):
        span = slice(b * block, (b + 1) * block)
        s = jnp.dot(
            q_rows[span, :], kv_t[:, c * chunk : (c + 1) * chunk],
            preferred_element_type=jnp.float32,
        )
        live = (lax.broadcasted_iota(jnp.int32, (1, chunk), 1) + c * chunk) < length
        s = jnp.where(live, s, -1e30)
        scores[span, c * chunk : (c + 1) * chunk] = s
        best = s[:, 0:lanes] if c == 0 else jnp.maximum(row_max[span, :], s[:, 0:lanes])
        for j in range(1, chunk // lanes):
            best = jnp.maximum(best, s[:, j * lanes : (j + 1) * lanes])
        row_max[span, :] = best

    def peak(b):
        span = slice(b * block, (b + 1) * block)
        fresh = lax.dot_general(
            q_rows[span, :], new_rows[...], (((1,), (1,)), ((), ())),
            preferred_element_type=jnp.float32,
        )
        step_of = b * per_block + lax.broadcasted_iota(jnp.int32, (block, lanes), 0) // heads
        fresh = jnp.where(
            lax.broadcasted_iota(jnp.int32, (block, lanes), 1) <= step_of, fresh, -1e30
        )
        top = jnp.max(jnp.maximum(row_max[span, :], fresh), axis=1, keepdims=True) * rate
        fresh = jnp.exp2(fresh * rate - top)
        return [top, fresh, fresh.astype(jnp.bfloat16)]

    def soften(b, c, state):
        span = slice(b * block, (b + 1) * block)
        e = jnp.exp2(scores[span, c * chunk : (c + 1) * chunk] * rate - state[0])
        for j in range(chunk // lanes):
            state[1] = state[1] + e[:, j * lanes : (j + 1) * lanes]
        weights[span, c * chunk : (c + 1) * chunk] = e.astype(jnp.bfloat16)

    def mix(b, first, last, state):
        span = slice(b * block, (b + 1) * block)
        part = lax.dot_general(
            weights[span, first * chunk : last * chunk],
            kv_t[0:LAT, first * chunk : last * chunk],
            (((1,), (1,)), ((), ())),
            preferred_element_type=jnp.float32,
        )
        if first == 0:
            part = part + jnp.dot(
                state[2], new_rows[:, 0:LAT], preferred_element_type=jnp.float32
            )
        else:
            part = part + mixed[...]
        if last < chunks:
            mixed[...] = part
            return
        part = part * (1.0 / jnp.sum(state[1], axis=1, keepdims=True))
        for i in range(per_block):
            s = b * per_block + i
            for d in range(heads // per_owner):
                column, side, t = d // (2 * depth), d // depth % 2, d % depth
                row = (side * steps + s) * per_owner
                first_row = i * heads + d * per_owner
                out_ref[column * depth + t, row : row + per_owner, :] = part[
                    first_row : first_row + per_owner, :
                ].astype(jnp.bfloat16)

    states = {}
    fetches = []
    turn(0)
    for stage in range(blocks + 2):
        mixing = stage - 2
        if mixing >= 0 and stage - 1 >= blocks:
            mix(mixing, 0, chunks, states[mixing])
            continue
        for c in range(chunks):
            if stage < blocks:
                if stage == 0:
                    kv_copies[c].wait()
                    if c == 0:
                        fetches = fetch(stored, held, sems, blocks + chunks + 1)
                score(stage, c)
                if c == 0 and stage + 1 < blocks:
                    turn(stage + 1)
            if 0 <= stage - 1 < blocks:
                soften(stage - 1, c, states[stage - 1])
            if mixing >= 0:
                mix(mixing, c, c + 1, states[mixing])
        if stage < blocks:
            states[stage] = peak(stage)
    for copy in fetches:
        copy.wait()


def attend(queries, kv_cache, new_kv, lengths, chips, depth, ahead, chunk=1024):
    _, steps, heads, width = queries.shape
    positions = kv_cache.shape[1]
    rows = steps * heads
    lanes = 128
    block = 2 * heads
    return pl.pallas_call(
        functools.partial(
            attend_kernel, chunk=chunk, block=block, depth=depth, ahead=len(ahead)
        ),
        out_shape=[jax.ShapeDtypeStruct((chips, rows // chips, LAT), jnp.bfloat16)]
        + [like(x) for x in ahead],
        in_specs=[SMEM] + [HBM] * (3 + len(ahead)),
        out_specs=[VMEM] * (1 + len(ahead)),
        scratch_shapes=[
            pltpu.VMEM((steps, width), jnp.bfloat16),
            pltpu.VMEM((steps, width, heads), jnp.bfloat16),
            pltpu.VMEM((rows, width), jnp.bfloat16),
            pltpu.VMEM((width, positions), jnp.bfloat16),
            pltpu.VMEM((lanes, width), jnp.bfloat16),
            pltpu.VMEM((rows, positions), jnp.float32),
            pltpu.VMEM((rows, positions), jnp.bfloat16),
            pltpu.VMEM((rows, lanes), jnp.float32),
            pltpu.VMEM((block, LAT), jnp.float32),
            pltpu.SemaphoreType.DMA((rows // block + positions // chunk + 1 + len(ahead),)),
        ],
        compiler_params=params(20),
        name="attend",
    )(
        lengths,
        in_hbm(jnp.swapaxes(queries[0], 1, 2)),
        in_hbm(jnp.swapaxes(kv_cache[0], 0, 1)),
        in_hbm(new_kv[0]),
        *[in_hbm(x) for x in ahead],
    )


def project_kernel(latent_ref, up_ref, up2_ref, down_ref, down2_ref, out_ref, latents, *, strip):
    sources, owned, _ = latent_ref.shape
    heads = up_ref.shape[0]
    owned = owned // 2
    steps = owned // heads
    items = sources * steps
    core = lax.axis_index("core")
    blocks = LAT // 128
    vals = []
    for side, w_ref in enumerate((up_ref, up2_ref)):
        start = pl.multiple_of((core if side == 0 else 1 - core) * owned, owned)
        for source in range(sources):
            block = latent_ref[source, pl.ds(start, owned), :].astype(jnp.float32)
            for j in range(blocks):
                latents[side * blocks + j, source * owned : (source + 1) * owned, :] = block[
                    :, j * 128 : (j + 1) * 128
                ]
        for h in range(heads):
            x = jnp.concatenate(
                [
                    latents[side * blocks + j, pl.ds(h, items, stride=heads), :]
                    for j in range(blocks)
                ],
                axis=1,
            ).astype(jnp.bfloat16)
            vals.append(
                jnp.dot(x, w_ref[h], preferred_element_type=jnp.float32).astype(jnp.bfloat16)
            )
    own = jnp.concatenate(vals[:heads], axis=1)
    partner = jnp.concatenate(vals[heads:], axis=1)
    width = down_ref.shape[1]
    for n in range(width // strip):
        cols = slice(n * strip, (n + 1) * strip)
        part = jnp.dot(own, down_ref[:, cols], preferred_element_type=jnp.float32)
        part = part + jnp.dot(partner, down2_ref[:, cols], preferred_element_type=jnp.float32)
        for j in range(sources):
            out_ref[j, :, cols] = part[j * steps : (j + 1) * steps].astype(jnp.bfloat16)


def project(by_head, value_up, value_up2, out_proj, out_proj2):
    sources, owned, _ = by_head.shape
    heads, _, value_width = value_up.shape
    width = out_proj.shape[2]
    flat = (heads * value_width, width)
    return pl.pallas_call(
        functools.partial(project_kernel, strip=512),
        out_shape=jax.ShapeDtypeStruct((sources, owned // (2 * heads), width), jnp.bfloat16),
        in_specs=[VMEM] * 5,
        out_specs=VMEM,
        scratch_shapes=[
            pltpu.VMEM((2 * LAT // 128, sources * owned // 2, 128), jnp.float32),
        ],
        compiler_params=params(8),
        name="project",
    )(by_head, value_up, value_up2, out_proj.reshape(flat), out_proj2.reshape(flat))


def norm_kernel(ids_ref, parts_ref, hidden_ref, gain_ref, router_ref, residual_ref, out_ref):
    chips, items, _ = parts_ref.shape
    width = hidden_ref.shape[1]
    experts = router_ref.shape[0]
    spare = out_ref.shape[2] - width
    place = lax.axis_index("tp")
    total = hidden_ref[...].astype(jnp.float32)
    attention = parts_ref[0].astype(jnp.float32)
    for j in range(1, chips):
        attention = attention + parts_ref[j].astype(jnp.float32)
    residual = total + attention
    residual_ref[...] = residual
    square = jnp.mean(residual * residual, axis=1, keepdims=True)
    normed = (residual * lax.rsqrt(square + norm_eps) * gain_ref[...].astype(jnp.float32).reshape(1, width)).astype(
        jnp.bfloat16
    )
    lane = lax.broadcasted_iota(jnp.int32, (items, experts), 1)
    exact = normed.astype(jnp.float32)
    logits = jnp.zeros((items, experts), jnp.float32)
    for e in range(experts):
        column = router_ref[e : e + 1, :].astype(jnp.float32)
        logits = jnp.where(lane == e, jnp.sum(exact * column, axis=1, keepdims=True), logits)
    affinity = 1.0 / (1.0 + jnp.exp(-logits))
    ids = ids_ref[place]
    own = lax.broadcasted_iota(jnp.int32, (items, items), 0) == lax.broadcasted_iota(
        jnp.int32, (items, items), 1
    )
    chosen = jnp.zeros((items, experts), jnp.float32)
    for k in range(ids.shape[0]):
        named = jnp.sum(jnp.where(own, ids[k : k + 1, :], 0), axis=1, keepdims=True)
        chosen = chosen + (lane == named).astype(jnp.float32)
    scored = chosen * affinity
    gates = route_scale * scored / jnp.sum(scored, axis=1, keepdims=True)
    high = gates.astype(jnp.bfloat16)
    low = (gates - high.astype(jnp.float32)).astype(jnp.bfloat16)
    tail = jnp.concatenate(
        [high.astype(jnp.float32), low.astype(jnp.float32),
         jnp.zeros((items, spare - 2 * experts), jnp.float32)], axis=1
    ).astype(jnp.bfloat16)
    for j in range(chips):
        out_ref[j, :, 0:width] = normed
        out_ref[j, :, width:] = tail


def norm_rows(ids, parts, hidden, gain, router):
    chips, items, width = parts.shape
    experts = router.shape[1]
    spare = -(-2 * experts // 128) * 128
    return pl.pallas_call(
        norm_kernel,
        out_shape=(
            jax.ShapeDtypeStruct((items, width), jnp.float32),
            jax.ShapeDtypeStruct((chips, items, width + spare), jnp.bfloat16),
        ),
        in_specs=[VMEM] * 5,
        out_specs=(VMEM, VMEM),
        compiler_params=params(8),
        name="norm_rows",
    )(ids, parts, hidden, gain, router.T)


def merge_kernel(kept_ref, got_ref, out_ref):
    chips, items, _ = out_ref.shape
    total = kept_ref[...] + got_ref[...].astype(jnp.float32)
    for j in range(chips):
        out_ref[j] = total[j * items : (j + 1) * items, :].astype(jnp.bfloat16)


def merge(kept, got, chips):
    rows, width = kept.shape
    return pl.pallas_call(
        merge_kernel,
        out_shape=jax.ShapeDtypeStruct((chips, rows // chips, width), jnp.bfloat16),
        in_specs=[VMEM, VMEM],
        out_specs=VMEM,
        compiler_params=params(4),
        name="merge",
    )(kept, got)


def silu_gate(g, u):
    return (g / (1.0 + jnp.exp(-g)) * u).astype(jnp.bfloat16)


def gather_rows(ref, first, tokens, tails):
    items = ref.shape[1]
    width = tokens.shape[1]
    for j in range(ref.shape[0]):
        rows = slice(first + j * items, first + (j + 1) * items)
        block = ref[j].astype(jnp.float32)
        tokens[rows, :] = block[:, :width]
        if tails is not None:
            tails[rows, :] = block[:, width:]


def shared_kernel(mine_ref, in_ref, out_w_ref, out_ref, tokens, *, strip):
    rows, width = out_ref.shape
    depth = rows // mine_ref.shape[1]
    column = lax.axis_index("epx")
    for t in range(depth):
        items = mine_ref.shape[1]
        tokens[t * items : (t + 1) * items, :] = mine_ref[column * depth + t].astype(
            jnp.float32
        )[:, :width]
    x = tokens[...].astype(jnp.bfloat16)
    g = jnp.dot(x, in_ref[0], preferred_element_type=jnp.float32)
    u = jnp.dot(x, in_ref[1], preferred_element_type=jnp.float32)
    act = silu_gate(g, u)
    for n in range(width // strip):
        cols = slice(n * strip, (n + 1) * strip)
        out_ref[:, cols] = jnp.dot(act, out_w_ref[:, cols], preferred_element_type=jnp.float32)


def run_shared(mine, shared_in, shared_out, depth):
    rows, width = depth * mine.shape[1], shared_out.shape[1]
    return pl.pallas_call(
        functools.partial(shared_kernel, strip=512),
        out_shape=jax.ShapeDtypeStruct((rows, width), jnp.float32),
        in_specs=[VMEM] * 3,
        out_specs=VMEM,
        scratch_shapes=[pltpu.VMEM((rows, width), jnp.float32)],
        compiler_params=params(6),
        name="shared",
    )(mine, shared_in, shared_out)


def routed_kernel(
    mine_ref, other_ref, in_ref, out_w_ref, sent_ref, act_ref, gate_ref, tokens, tails,
    *, experts, strip,
):
    half, width = sent_ref.shape
    core, column = lax.axis_index("core"), lax.axis_index("epx")
    gather_rows(mine_ref, 0, tokens, tails)
    gather_rows(other_ref, half, tokens, tails)
    x = tokens[...].astype(jnp.bfloat16)
    here = column * 2 + core
    lane = lax.broadcasted_iota(jnp.int32, tails.shape, 1)
    gate = jnp.sum(
        jnp.where((lane == here) | (lane == here + experts), tails[...], 0.0),
        axis=1, keepdims=True,
    )
    g = jnp.dot(x, in_ref[0], preferred_element_type=jnp.float32)
    u = jnp.dot(x, in_ref[1], preferred_element_type=jnp.float32)
    act = silu_gate(g, u)
    act_ref[...] = act[:half]
    gate_ref[...] = jnp.broadcast_to(gate[:half], gate_ref.shape)
    for n in range(width // strip):
        cols = slice(n * strip, (n + 1) * strip)
        y = gate[half:] * jnp.dot(
            act[half:], out_w_ref[:, cols], preferred_element_type=jnp.float32
        )
        sent_ref[:, cols] = y.astype(jnp.bfloat16)


def run_routed(mine, other, expert_in, expert_out, experts):
    chips, items, padded = mine.shape
    hidden, width = expert_out.shape
    half = chips * items
    return pl.pallas_call(
        functools.partial(routed_kernel, experts=experts, strip=512),
        out_shape=(
            jax.ShapeDtypeStruct((half, width), jnp.bfloat16),
            jax.ShapeDtypeStruct((half, hidden), jnp.bfloat16),
            jax.ShapeDtypeStruct((half, 128), jnp.float32),
        ),
        in_specs=[VMEM] * 4,
        out_specs=(VMEM, VMEM, VMEM),
        scratch_shapes=[
            pltpu.VMEM((2 * half, width), jnp.float32),
            pltpu.VMEM((2 * half, padded - width), jnp.float32),
        ],
        compiler_params=params(8),
        name="routed",
    )(mine, other, expert_in, expert_out)


def keep_kernel(act_ref, gate_ref, out_w_ref, shared_ref, kept_ref, *, strip):
    width = kept_ref.shape[1]
    rows = shared_ref.shape[0]
    start = pl.multiple_of(lax.axis_index("epx") * rows, rows)
    gate = gate_ref[:, 0:1]
    for n in range(width // strip):
        cols = slice(n * strip, (n + 1) * strip)
        kept_ref[:, cols] = gate * jnp.dot(
            act_ref[...], out_w_ref[:, cols], preferred_element_type=jnp.float32
        )
    kept_ref[pl.ds(start, rows), :] = kept_ref[pl.ds(start, rows), :] + shared_ref[...]


def run_keep(act, gate, expert_out, shared):
    return pl.pallas_call(
        functools.partial(keep_kernel, strip=512),
        out_shape=jax.ShapeDtypeStruct((act.shape[0], expert_out.shape[1]), jnp.float32),
        in_specs=[VMEM] * 4,
        out_specs=VMEM,
        compiler_params=params(6),
        name="keep",
    )(act, gate, expert_out, shared)


def finish_kernel(parts_ref, residual_ref, out_ref):
    total = residual_ref[...]
    for j in range(parts_ref.shape[0]):
        total = total + parts_ref[j].astype(jnp.float32)
    out_ref[...] = total.astype(jnp.bfloat16)


def finish(parts, residual):
    return pl.pallas_call(
        finish_kernel,
        out_shape=jax.ShapeDtypeStruct(residual.shape, jnp.bfloat16),
        in_specs=[VMEM, VMEM],
        out_specs=VMEM,
        compiler_params=params(8),
        name="finish",
    )(parts, residual)


def swap_cores(x):
    return lax.ppermute(x, "core", [(0, 1), (1, 0)])


def chip_exchange(x):
    return lax.all_to_all(x, CHIPS, split_axis=0, concat_axis=0, tiled=True)


def attend_block(queries, kv_cache, new_kv, lengths):
    rows_here, steps_here, heads_here, kv_width = queries.shape
    positions = kv_cache.shape[1]
    cached = (
        jnp.einsum("rshk,rck->rshc", queries, kv_cache, preferred_element_type=jnp.float32)
        * score_scale
    )
    recent = (
        jnp.einsum("rshk,rjk->rshj", queries, new_kv, preferred_element_type=jnp.float32)
        * score_scale
    )
    cache_live = lax.broadcasted_iota(jnp.int32, (rows_here, positions), 1) < lengths[:, None]
    causal = lax.broadcasted_iota(jnp.int32, (steps_here, steps_here), 1) <= lax.broadcasted_iota(
        jnp.int32, (steps_here, steps_here), 0
    )
    cached = jnp.where(cache_live[:, None, None, :], cached, -1e30)
    recent = jnp.where(causal[None, :, None, :], recent, -1e30)
    highest = jnp.maximum(cached.max(-1), recent.max(-1))[..., None]
    cached_exp = jnp.exp(cached - highest)
    recent_exp = jnp.exp(recent - highest)
    denominator = cached_exp.sum(-1, keepdims=True) + recent_exp.sum(-1, keepdims=True)
    cached_prob = (cached_exp / denominator).astype(jnp.bfloat16)
    recent_prob = (recent_exp / denominator).astype(jnp.bfloat16)
    combined = jnp.einsum(
        "rshc,rck->rshk", cached_prob, kv_cache, preferred_element_type=jnp.float32
    )
    combined = combined + jnp.einsum(
        "rshj,rjk->rshk", recent_prob, new_kv, preferred_element_type=jnp.float32
    )
    return combined[..., :LAT].astype(jnp.bfloat16)


def sum_at_rows(kept, sent, chips):
    half = kept + swap_cores(sent.astype(jnp.bfloat16)).astype(jnp.float32)
    width = half.shape[1]
    parts = chip_exchange(half.astype(jnp.bfloat16).reshape(chips, -1, width))
    return jnp.sum(parts.astype(jnp.float32), axis=0)


def plain_device(
    hidden_in,
    queries,
    kv_cache,
    new_kv,
    lengths,
    expert_ids,
    value_up,
    out_proj,
    norm_gain,
    router,
    expert_in,
    expert_out,
    shared_in,
    shared_out,
):
    rows_here, steps_here, model_width = hidden_in.shape
    items = rows_here * steps_here
    columns = lax.axis_size("epx")
    depth = lax.axis_size("tp")
    chips = columns * depth
    core = lax.axis_index("core")
    column = lax.axis_index("epx")
    place = lax.axis_index("tp")
    expert_count = router.shape[1]

    latent_out = attend_block(queries, kv_cache, new_kv, lengths)
    by_head = lax.all_to_all(latent_out, ALL, split_axis=2, concat_axis=0, tiled=True)
    head_vals = jnp.einsum(
        "rshl,hlv->rshv", by_head, value_up, preferred_element_type=jnp.float32
    ).astype(jnp.bfloat16)
    partial = jnp.einsum(
        "rshv,hvd->rsd", head_vals, out_proj, preferred_element_type=jnp.float32
    ).reshape(columns, 2, depth * items, model_width)
    kept = lax.dynamic_index_in_dim(partial, core, 1, keepdims=False)
    sent = lax.dynamic_index_in_dim(partial, 1 - core, 1, keepdims=False)
    attention = sum_at_rows(
        kept.reshape(-1, model_width), sent.reshape(-1, model_width), chips
    )
    residual = hidden_in.reshape(items, model_width).astype(jnp.float32) + attention
    mean_square = jnp.mean(residual * residual, axis=-1, keepdims=True)
    normed = (residual * lax.rsqrt(mean_square + norm_eps) * norm_gain.astype(jnp.float32)).astype(
        jnp.bfloat16
    )
    affinity = jax.nn.sigmoid(jnp.dot(normed, router, preferred_element_type=jnp.float32))
    picked = lax.dynamic_slice_in_dim(expert_ids, place * rows_here, rows_here, 0).reshape(
        items, expert_ids.shape[2]
    )
    expert_iota = lax.broadcasted_iota(jnp.int32, (1, 1, expert_count), 2)
    chosen = jnp.sum((picked[:, :, None] == expert_iota).astype(jnp.float32), axis=1)
    scored = chosen * affinity
    gate_weight = route_scale * scored / jnp.sum(scored, axis=-1, keepdims=True)
    gate_high = gate_weight.astype(jnp.bfloat16)
    gate_low = (gate_weight - gate_high.astype(jnp.float32)).astype(jnp.bfloat16)
    spare = -(2 * expert_count) % 128
    payload = jnp.concatenate(
        [normed, gate_high, gate_low, jnp.zeros((items, spare), jnp.bfloat16)], axis=1
    )
    mine = chip_exchange(jnp.broadcast_to(payload[None], (chips,) + payload.shape)).reshape(
        chips * items, -1
    )
    tokens = jnp.concatenate([mine, swap_cores(mine)], axis=0)
    block_items = tokens[:, :model_width]
    expert_here = column * 2 + core
    gate_pairs = tokens[:, model_width : model_width + 2 * expert_count].astype(jnp.float32)
    gates = gate_pairs[:, :expert_count] + gate_pairs[:, expert_count:]
    gate_here = lax.dynamic_slice_in_dim(gates, expert_here, 1, 1)

    gate_part = jnp.dot(block_items, expert_in[0, 0], preferred_element_type=jnp.float32)
    up_part = jnp.dot(block_items, expert_in[0, 1], preferred_element_type=jnp.float32)
    activated = (jax.nn.silu(gate_part) * up_part).astype(jnp.bfloat16)
    routed = gate_here * jnp.dot(activated, expert_out[0], preferred_element_type=jnp.float32)

    own = lax.dynamic_slice_in_dim(mine, column * depth * items, depth * items, 0)[
        :, :model_width
    ]
    shared_gate = jnp.dot(own, shared_in[0], preferred_element_type=jnp.float32)
    shared_up = jnp.dot(own, shared_in[1], preferred_element_type=jnp.float32)
    shared_act = (jax.nn.silu(shared_gate) * shared_up).astype(jnp.bfloat16)
    shared_part = jnp.dot(shared_act, shared_out, preferred_element_type=jnp.float32)

    kept = routed[: chips * items].reshape(columns, depth * items, model_width)
    at_column = lax.broadcasted_iota(jnp.int32, (columns, 1, 1), 0) == column
    kept = kept + jnp.where(at_column, shared_part[None], 0.0)
    expert_sum = sum_at_rows(
        kept.reshape(-1, model_width), routed[chips * items :], chips
    )
    layer_out = (residual + expert_sum).astype(jnp.bfloat16)
    return layer_out.reshape(rows_here, steps_here, model_width)


def on_device(
    hidden_in,
    queries,
    kv_cache,
    new_kv,
    lengths,
    expert_ids,
    value_up,
    out_proj,
    norm_gain,
    router,
    expert_in,
    expert_out,
    shared_in,
    shared_out,
):
    rows_here, steps_here, model_width = hidden_in.shape
    items = rows_here * steps_here
    columns = lax.axis_size("epx")
    depth = lax.axis_size("tp")
    chips = columns * depth
    experts = router.shape[1]

    value_up2 = swap_cores(value_up)
    out_proj2 = swap_cores(out_proj)
    expert_in, expert_out = expert_in[0], expert_out[0]
    latent_out, out_proj, value_up = attend(
        queries, kv_cache, new_kv, lengths, chips, depth, [out_proj, value_up]
    )
    by_head = chip_exchange(latent_out)
    parts = chip_exchange(project(by_head, value_up, value_up2, out_proj, out_proj2))
    ids = jnp.swapaxes(expert_ids, 1, 2)
    residual, handed = norm_rows(
        ids, parts, hidden_in.reshape(items, model_width), norm_gain, router
    )
    mine = chip_exchange(handed)
    other = swap_cores(mine)
    shared = run_shared(mine, shared_in, shared_out, depth)
    other, shared = lax.optimization_barrier((other, shared))
    sent, act, gate = run_routed(mine, other, expert_in, expert_out, experts)
    got = swap_cores(sent)
    kept = run_keep(act, gate, expert_out, shared)
    parts = chip_exchange(merge(kept, got, chips))
    return finish(parts, residual).reshape(rows_here, steps_here, model_width)


def choose(*args):
    owners = 2 * lax.axis_size("epx") * lax.axis_size("tp")
    queries = args[1]
    whole_tiles = queries.shape[0] == 1 and queries.shape[2] % (8 * owners) == 0
    return on_device(*args) if whole_tiles else plain_device(*args)


def solution(mesh):
    sizes = mesh.shape
    fine = Mesh(
        mesh.devices.reshape(sizes["groups"], sizes["ep"] // 2, 2, sizes["tp"]),
        ("groups", "epx", "core", "tp"),
    )
    ep = ("epx", "core")
    rows = ("groups", "epx", "core", "tp")
    in_specs = (
        P(rows, None, None),
        P(rows, None, None, None),
        P(rows, None, None),
        P(rows, None, None),
        P(rows),
        P(("groups",) + ep, None, None),
        P(ALL, None, None),
        P(ALL, None, None),
        P(),
        P(),
        P(ep, None, None, "tp"),
        P(ep, "tp", None),
        P(None, None, "tp"),
        P("tp", None),
    )
    out_specs = P(rows, None, None)
    return jax.shard_map(
        choose, mesh=fine, in_specs=in_specs, out_specs=out_specs, check_vma=False
    )
```

```python
import functools

import jax
import jax.numpy as jnp
import numpy as np
from jax import lax
from jax.experimental import pallas as pl
from jax.experimental.pallas import tpu as pltpu
from jax.sharding import Mesh
from jax.sharding import PartitionSpec as P

LAT = 512


score_scale = 192.0 ** (-0.5)
log2_e = 1.4426950408889634
route_scale = 2.5
norm_eps = 1e-06

CHIPS = ("epx", "tp")
ALL = ("epx", "core", "tp")
VMEM = pl.BlockSpec(memory_space=pltpu.VMEM)
SMEM = pl.BlockSpec(memory_space=pltpu.SMEM)
HBM = pl.BlockSpec(memory_space=pltpu.HBM)


def params(mib):
    return pltpu.CompilerParams(vmem_limit_bytes=mib << 20)


def fetch(stored, held, sems, first):
    copies = [
        pltpu.make_async_copy(a, b, sems.at[first + i])
        for i, (a, b) in enumerate(zip(stored, held))
    ]
    for copy in copies:
        copy.start()
    return copies


def in_hbm(x):
    return pltpu.with_memory_space_constraint(x, pltpu.HBM)


def like(x):
    return jax.ShapeDtypeStruct(x.shape, x.dtype)


def attend_kernel(length_ref, q_hbm, kv_hbm, new_hbm, *refs, chunk, block, depth, places, ahead):
    stored, out_ref, held = refs[:ahead], refs[ahead], refs[ahead + 1 : 2 * ahead + 1]
    new_ref, q_t, q_rows, kv_t, new_rows, scores, weights, row_max, mixed, sems = refs[
        2 * ahead + 1 :
    ]
    steps, width, heads = q_t.shape
    positions = kv_t.shape[1]
    rows = steps * heads
    blocks = rows // block
    per_block = block // heads
    chunks = positions // chunk
    lanes = new_rows.shape[0]
    q_copies = [
        pltpu.make_async_copy(
            q_hbm.at[pl.ds(b * per_block, per_block)],
            q_t.at[pl.ds(b * per_block, per_block)],
            sems.at[b],
        )
        for b in range(blocks)
    ]
    kv_copies = [
        pltpu.make_async_copy(
            kv_hbm.at[:, pl.ds(c * chunk, chunk)],
            kv_t.at[:, pl.ds(c * chunk, chunk)],
            sems.at[blocks + c],
        )
        for c in range(chunks)
    ]
    new_copy = pltpu.make_async_copy(new_hbm, new_ref, sems.at[blocks + chunks])
    q_copies[0].start()
    kv_copies[0].start()
    new_copy.start()
    for copy in q_copies[1:] + kv_copies[1:]:
        copy.start()
    new_rows[...] = jnp.zeros_like(new_rows)
    new_copy.wait()
    new_rows[0:steps, :] = new_ref[...]
    length = length_ref[0]
    rate = score_scale * log2_e
    per_owner = out_ref.shape[1] // (2 * steps)

    def turn(b):
        q_copies[b].wait()
        for i in range(per_block):
            s = b * per_block + i
            q_rows[s * heads : (s + 1) * heads, :] = q_t[s].T

    def score(b, c):
        span = slice(b * block, (b + 1) * block)
        s = jnp.dot(
            q_rows[span, :], kv_t[:, c * chunk : (c + 1) * chunk],
            preferred_element_type=jnp.float32,
        )
        live = (lax.broadcasted_iota(jnp.int32, (1, chunk), 1) + c * chunk) < length
        s = jnp.where(live, s, -1e30)
        scores[span, c * chunk : (c + 1) * chunk] = s
        best = s[:, 0:lanes] if c == 0 else jnp.maximum(row_max[span, :], s[:, 0:lanes])
        for j in range(1, chunk // lanes):
            best = jnp.maximum(best, s[:, j * lanes : (j + 1) * lanes])
        row_max[span, :] = best

    def peak(b):
        span = slice(b * block, (b + 1) * block)
        fresh = lax.dot_general(
            q_rows[span, :], new_rows[...], (((1,), (1,)), ((), ())),
            preferred_element_type=jnp.float32,
        )
        step_of = b * per_block + lax.broadcasted_iota(jnp.int32, (block, lanes), 0) // heads
        fresh = jnp.where(
            lax.broadcasted_iota(jnp.int32, (block, lanes), 1) <= step_of, fresh, -1e30
        )
        top = jnp.max(jnp.maximum(row_max[span, :], fresh), axis=1, keepdims=True) * rate
        fresh = jnp.exp2(fresh * rate - top)
        return [top, fresh, fresh.astype(jnp.bfloat16)]

    def soften(b, c, state):
        span = slice(b * block, (b + 1) * block)
        e = jnp.exp2(scores[span, c * chunk : (c + 1) * chunk] * rate - state[0])
        for j in range(chunk // lanes):
            state[1] = state[1] + e[:, j * lanes : (j + 1) * lanes]
        weights[span, c * chunk : (c + 1) * chunk] = e.astype(jnp.bfloat16)

    def mix(b, first, last, state):
        span = slice(b * block, (b + 1) * block)
        part = lax.dot_general(
            weights[span, first * chunk : last * chunk],
            kv_t[0:LAT, first * chunk : last * chunk],
            (((1,), (1,)), ((), ())),
            preferred_element_type=jnp.float32,
        )
        if first == 0:
            part = part + jnp.dot(
                state[2], new_rows[:, 0:LAT], preferred_element_type=jnp.float32
            )
        else:
            part = part + mixed[...]
        if last < chunks:
            mixed[...] = part
            return
        part = part * (1.0 / jnp.sum(state[1], axis=1, keepdims=True))
        for i in range(per_block):
            s = b * per_block + i
            for d in range(heads // per_owner):
                column, side, t = d // (2 * depth), d // depth % 2, d % depth
                row = (side * steps + s) * per_owner
                first_row = i * heads + d * per_owner
                out_ref[places[column * depth + t], row : row + per_owner, :] = part[
                    first_row : first_row + per_owner, :
                ].astype(jnp.bfloat16)

    states = {}
    fetches = []
    turn(0)
    for stage in range(blocks + 2):
        mixing = stage - 2
        if mixing >= 0 and stage - 1 >= blocks:
            mix(mixing, 0, chunks, states[mixing])
            continue
        for c in range(chunks):
            if stage < blocks:
                if stage == 0:
                    kv_copies[c].wait()
                    if c == 0:
                        fetches = fetch(stored, held, sems, blocks + chunks + 1)
                score(stage, c)
                if c == 0 and stage + 1 < blocks:
                    turn(stage + 1)
            if 0 <= stage - 1 < blocks:
                soften(stage - 1, c, states[stage - 1])
            if mixing >= 0:
                mix(mixing, c, c + 1, states[mixing])
        if stage < blocks:
            states[stage] = peak(stage)
    for copy in fetches:
        copy.wait()


def attend(queries, kv_cache, new_kv, lengths, places, depth, ahead, chunk=1024):
    _, steps, heads, width = queries.shape
    positions = kv_cache.shape[1]
    rows = steps * heads
    lanes = 128
    block = 2 * heads
    chips = len(places)
    return pl.pallas_call(
        functools.partial(
            attend_kernel,
            chunk=chunk,
            block=block,
            depth=depth,
            places=places,
            ahead=len(ahead),
        ),
        out_shape=[jax.ShapeDtypeStruct((chips, rows // chips, LAT), jnp.bfloat16)]
        + [like(x) for x in ahead],
        in_specs=[SMEM] + [HBM] * (3 + len(ahead)),
        out_specs=[VMEM] * (1 + len(ahead)),
        scratch_shapes=[
            pltpu.VMEM((steps, width), jnp.bfloat16),
            pltpu.VMEM((steps, width, heads), jnp.bfloat16),
            pltpu.VMEM((rows, width), jnp.bfloat16),
            pltpu.VMEM((width, positions), jnp.bfloat16),
            pltpu.VMEM((lanes, width), jnp.bfloat16),
            pltpu.VMEM((rows, positions), jnp.float32),
            pltpu.VMEM((rows, positions), jnp.bfloat16),
            pltpu.VMEM((rows, lanes), jnp.float32),
            pltpu.VMEM((block, LAT), jnp.float32),
            pltpu.SemaphoreType.DMA((rows // block + positions // chunk + 1 + len(ahead),)),
        ],
        compiler_params=params(20),
        name="attend",
    )(
        lengths,
        in_hbm(jnp.swapaxes(queries[0], 1, 2)),
        in_hbm(jnp.swapaxes(kv_cache[0], 0, 1)),
        in_hbm(new_kv[0]),
        *[in_hbm(x) for x in ahead],
    )


def project_kernel(latent_ref, up_ref, up2_ref, down_ref, down2_ref, out_ref, latents, *, strip):
    sources, owned, _ = latent_ref.shape
    heads = up_ref.shape[0]
    owned = owned // 2
    steps = owned // heads
    items = sources * steps
    core = lax.axis_index("core")
    blocks = LAT // 128
    vals = []
    for side, w_ref in enumerate((up_ref, up2_ref)):
        start = pl.multiple_of((core if side == 0 else 1 - core) * owned, owned)
        for source in range(sources):
            block = latent_ref[source, pl.ds(start, owned), :].astype(jnp.float32)
            for j in range(blocks):
                latents[side * blocks + j, source * owned : (source + 1) * owned, :] = block[
                    :, j * 128 : (j + 1) * 128
                ]
        for h in range(heads):
            x = jnp.concatenate(
                [
                    latents[side * blocks + j, pl.ds(h, items, stride=heads), :]
                    for j in range(blocks)
                ],
                axis=1,
            ).astype(jnp.bfloat16)
            vals.append(
                jnp.dot(x, w_ref[h], preferred_element_type=jnp.float32).astype(jnp.bfloat16)
            )
    own = jnp.concatenate(vals[:heads], axis=1)
    partner = jnp.concatenate(vals[heads:], axis=1)
    width = down_ref.shape[1]
    for n in range(width // strip):
        cols = slice(n * strip, (n + 1) * strip)
        part = jnp.dot(own, down_ref[:, cols], preferred_element_type=jnp.float32)
        part = part + jnp.dot(partner, down2_ref[:, cols], preferred_element_type=jnp.float32)
        for j in range(sources):
            out_ref[j, :, cols] = part[j * steps : (j + 1) * steps].astype(jnp.bfloat16)


def project(by_head, value_up, value_up2, out_proj, out_proj2):
    sources, owned, _ = by_head.shape
    heads, _, value_width = value_up.shape
    width = out_proj.shape[2]
    flat = (heads * value_width, width)
    return pl.pallas_call(
        functools.partial(project_kernel, strip=512),
        out_shape=jax.ShapeDtypeStruct((sources, owned // (2 * heads), width), jnp.bfloat16),
        in_specs=[VMEM] * 5,
        out_specs=VMEM,
        scratch_shapes=[
            pltpu.VMEM((2 * LAT // 128, sources * owned // 2, 128), jnp.float32),
        ],
        compiler_params=params(8),
        name="project",
    )(by_head, value_up, value_up2, out_proj.reshape(flat), out_proj2.reshape(flat))


def norm_kernel(ids_ref, parts_ref, hidden_ref, gain_ref, router_ref, residual_ref, out_ref):
    chips, items, _ = parts_ref.shape
    width = hidden_ref.shape[1]
    experts = router_ref.shape[0]
    spare = out_ref.shape[2] - width
    place = lax.axis_index("tp")
    total = hidden_ref[...].astype(jnp.float32)
    attention = parts_ref[0].astype(jnp.float32)
    for j in range(1, chips):
        attention = attention + parts_ref[j].astype(jnp.float32)
    residual = total + attention
    residual_ref[...] = residual
    square = jnp.mean(residual * residual, axis=1, keepdims=True)
    normed = (residual * lax.rsqrt(square + norm_eps) * gain_ref[...].astype(jnp.float32).reshape(1, width)).astype(
        jnp.bfloat16
    )
    lane = lax.broadcasted_iota(jnp.int32, (items, experts), 1)
    exact = normed.astype(jnp.float32)
    logits = jnp.zeros((items, experts), jnp.float32)
    for e in range(experts):
        column = router_ref[e : e + 1, :].astype(jnp.float32)
        logits = jnp.where(lane == e, jnp.sum(exact * column, axis=1, keepdims=True), logits)
    affinity = 1.0 / (1.0 + jnp.exp(-logits))
    ids = ids_ref[place]
    own = lax.broadcasted_iota(jnp.int32, (items, items), 0) == lax.broadcasted_iota(
        jnp.int32, (items, items), 1
    )
    chosen = jnp.zeros((items, experts), jnp.float32)
    for k in range(ids.shape[0]):
        named = jnp.sum(jnp.where(own, ids[k : k + 1, :], 0), axis=1, keepdims=True)
        chosen = chosen + (lane == named).astype(jnp.float32)
    scored = chosen * affinity
    gates = route_scale * scored / jnp.sum(scored, axis=1, keepdims=True)
    high = gates.astype(jnp.bfloat16)
    low = (gates - high.astype(jnp.float32)).astype(jnp.bfloat16)
    tail = jnp.concatenate(
        [high.astype(jnp.float32), low.astype(jnp.float32),
         jnp.zeros((items, spare - 2 * experts), jnp.float32)], axis=1
    ).astype(jnp.bfloat16)
    for j in range(chips):
        out_ref[j, :, 0:width] = normed
        out_ref[j, :, width:] = tail


def norm_rows(ids, parts, hidden, gain, router):
    chips, items, width = parts.shape
    experts = router.shape[1]
    spare = -(-2 * experts // 128) * 128
    return pl.pallas_call(
        norm_kernel,
        out_shape=(
            jax.ShapeDtypeStruct((items, width), jnp.float32),
            jax.ShapeDtypeStruct((chips, items, width + spare), jnp.bfloat16),
        ),
        in_specs=[VMEM] * 5,
        out_specs=(VMEM, VMEM),
        compiler_params=params(8),
        name="norm_rows",
    )(ids, parts, hidden, gain, router.T)


def merge_kernel(kept_ref, got_ref, out_ref):
    chips, items, _ = out_ref.shape
    total = kept_ref[...] + got_ref[...].astype(jnp.float32)
    for j in range(chips):
        out_ref[j] = total[j * items : (j + 1) * items, :].astype(jnp.bfloat16)


def merge(kept, got, chips):
    rows, width = kept.shape
    return pl.pallas_call(
        merge_kernel,
        out_shape=jax.ShapeDtypeStruct((chips, rows // chips, width), jnp.bfloat16),
        in_specs=[VMEM, VMEM],
        out_specs=VMEM,
        compiler_params=params(4),
        name="merge",
    )(kept, got)


def silu_gate(g, u):
    return (g / (1.0 + jnp.exp(-g)) * u).astype(jnp.bfloat16)


def gather_rows(ref, first, tokens, tails):
    items = ref.shape[1]
    width = tokens.shape[1]
    for j in range(ref.shape[0]):
        rows = slice(first + j * items, first + (j + 1) * items)
        block = ref[j].astype(jnp.float32)
        tokens[rows, :] = block[:, :width]
        if tails is not None:
            tails[rows, :] = block[:, width:]


def shared_kernel(mine_ref, in_ref, out_w_ref, out_ref, tokens, *, strip, places):
    rows, width = out_ref.shape
    depth = rows // mine_ref.shape[1]
    column = lax.axis_index("epx")
    items = mine_ref.shape[1]
    for t in range(depth):
        place = sum(
            jnp.where(column == x, places[x * depth + t], 0)
            for x in range(len(places) // depth)
        )
        tokens[t * items : (t + 1) * items, :] = mine_ref[place].astype(jnp.float32)[:, :width]
    x = tokens[...].astype(jnp.bfloat16)
    g = jnp.dot(x, in_ref[0], preferred_element_type=jnp.float32)
    u = jnp.dot(x, in_ref[1], preferred_element_type=jnp.float32)
    act = silu_gate(g, u)
    for n in range(width // strip):
        cols = slice(n * strip, (n + 1) * strip)
        out_ref[:, cols] = jnp.dot(act, out_w_ref[:, cols], preferred_element_type=jnp.float32)


def run_shared(mine, shared_in, shared_out, places, depth):
    rows, width = depth * mine.shape[1], shared_out.shape[1]
    return pl.pallas_call(
        functools.partial(shared_kernel, strip=512, places=places),
        out_shape=jax.ShapeDtypeStruct((rows, width), jnp.float32),
        in_specs=[VMEM] * 3,
        out_specs=VMEM,
        scratch_shapes=[pltpu.VMEM((rows, width), jnp.float32)],
        compiler_params=params(6),
        name="shared",
    )(mine, shared_in, shared_out)


def routed_kernel(
    mine_ref, other_ref, in_ref, out_w_ref, sent_ref, act_ref, gate_ref, tokens, tails,
    *, experts, strip,
):
    half, width = sent_ref.shape
    core, column = lax.axis_index("core"), lax.axis_index("epx")
    gather_rows(mine_ref, 0, tokens, tails)
    gather_rows(other_ref, half, tokens, tails)
    x = tokens[...].astype(jnp.bfloat16)
    here = column * 2 + core
    lane = lax.broadcasted_iota(jnp.int32, tails.shape, 1)
    gate = jnp.sum(
        jnp.where((lane == here) | (lane == here + experts), tails[...], 0.0),
        axis=1, keepdims=True,
    )
    g = jnp.dot(x, in_ref[0], preferred_element_type=jnp.float32)
    u = jnp.dot(x, in_ref[1], preferred_element_type=jnp.float32)
    act = silu_gate(g, u)
    act_ref[...] = act[:half]
    gate_ref[...] = jnp.broadcast_to(gate[:half], gate_ref.shape)
    for n in range(width // strip):
        cols = slice(n * strip, (n + 1) * strip)
        y = gate[half:] * jnp.dot(
            act[half:], out_w_ref[:, cols], preferred_element_type=jnp.float32
        )
        sent_ref[:, cols] = y.astype(jnp.bfloat16)


def run_routed(mine, other, expert_in, expert_out, experts):
    chips, items, padded = mine.shape
    hidden, width = expert_out.shape
    half = chips * items
    return pl.pallas_call(
        functools.partial(routed_kernel, experts=experts, strip=512),
        out_shape=(
            jax.ShapeDtypeStruct((half, width), jnp.bfloat16),
            jax.ShapeDtypeStruct((half, hidden), jnp.bfloat16),
            jax.ShapeDtypeStruct((half, 128), jnp.float32),
        ),
        in_specs=[VMEM] * 4,
        out_specs=(VMEM, VMEM, VMEM),
        scratch_shapes=[
            pltpu.VMEM((2 * half, width), jnp.float32),
            pltpu.VMEM((2 * half, padded - width), jnp.float32),
        ],
        compiler_params=params(8),
        name="routed",
    )(mine, other, expert_in, expert_out)


def keep_kernel(act_ref, gate_ref, out_w_ref, shared_ref, kept_ref, *, strip, places):
    width = kept_ref.shape[1]
    rows = shared_ref.shape[0]
    items = kept_ref.shape[0] // len(places)
    depth = rows // items
    column = lax.axis_index("epx")
    gate = gate_ref[:, 0:1]
    for n in range(width // strip):
        cols = slice(n * strip, (n + 1) * strip)
        kept_ref[:, cols] = gate * jnp.dot(
            act_ref[...], out_w_ref[:, cols], preferred_element_type=jnp.float32
        )
    for x in range(len(places) // depth):
        for t in range(depth):
            first = places[x * depth + t] * items
            part = shared_ref[t * items : (t + 1) * items, :]
            kept_ref[first : first + items, :] = kept_ref[first : first + items, :] + jnp.where(
                column == x, part, 0.0
            )


def run_keep(act, gate, expert_out, shared, places):
    return pl.pallas_call(
        functools.partial(keep_kernel, strip=512, places=places),
        out_shape=jax.ShapeDtypeStruct((act.shape[0], expert_out.shape[1]), jnp.float32),
        in_specs=[VMEM] * 4,
        out_specs=VMEM,
        compiler_params=params(6),
        name="keep",
    )(act, gate, expert_out, shared)


def finish_kernel(parts_ref, residual_ref, out_ref):
    total = residual_ref[...]
    for j in range(parts_ref.shape[0]):
        total = total + parts_ref[j].astype(jnp.float32)
    out_ref[...] = total.astype(jnp.bfloat16)


def finish(parts, residual):
    return pl.pallas_call(
        finish_kernel,
        out_shape=jax.ShapeDtypeStruct(residual.shape, jnp.bfloat16),
        in_specs=[VMEM, VMEM],
        out_specs=VMEM,
        compiler_params=params(8),
        name="finish",
    )(parts, residual)


def swap_cores(x):
    return lax.ppermute(x, "core", [(0, 1), (1, 0)])


def chip_exchange(x):
    return lax.all_to_all(x, CHIPS, split_axis=0, concat_axis=0, tiled=True)


def order_of_chips(chips):
    return [int(chip) for chip in np.random.RandomState(28286).permutation(chips)]


def plane_exchange(x, order, depth):
    groups = [
        [(chip // depth * 2 + core) * depth + chip % depth for chip in order] for core in range(2)
    ]
    return lax.all_to_all(
        x, ALL, split_axis=0, concat_axis=0, axis_index_groups=groups, tiled=True
    )


def attend_block(queries, kv_cache, new_kv, lengths):
    rows_here, steps_here, heads_here, kv_width = queries.shape
    positions = kv_cache.shape[1]
    cached = (
        jnp.einsum("rshk,rck->rshc", queries, kv_cache, preferred_element_type=jnp.float32)
        * score_scale
    )
    recent = (
        jnp.einsum("rshk,rjk->rshj", queries, new_kv, preferred_element_type=jnp.float32)
        * score_scale
    )
    cache_live = lax.broadcasted_iota(jnp.int32, (rows_here, positions), 1) < lengths[:, None]
    causal = lax.broadcasted_iota(jnp.int32, (steps_here, steps_here), 1) <= lax.broadcasted_iota(
        jnp.int32, (steps_here, steps_here), 0
    )
    cached = jnp.where(cache_live[:, None, None, :], cached, -1e30)
    recent = jnp.where(causal[None, :, None, :], recent, -1e30)
    highest = jnp.maximum(cached.max(-1), recent.max(-1))[..., None]
    cached_exp = jnp.exp(cached - highest)
    recent_exp = jnp.exp(recent - highest)
    denominator = cached_exp.sum(-1, keepdims=True) + recent_exp.sum(-1, keepdims=True)
    cached_prob = (cached_exp / denominator).astype(jnp.bfloat16)
    recent_prob = (recent_exp / denominator).astype(jnp.bfloat16)
    combined = jnp.einsum(
        "rshc,rck->rshk", cached_prob, kv_cache, preferred_element_type=jnp.float32
    )
    combined = combined + jnp.einsum(
        "rshj,rjk->rshk", recent_prob, new_kv, preferred_element_type=jnp.float32
    )
    return combined[..., :LAT].astype(jnp.bfloat16)


def sum_at_rows(kept, sent, chips):
    half = kept + swap_cores(sent.astype(jnp.bfloat16)).astype(jnp.float32)
    width = half.shape[1]
    parts = chip_exchange(half.astype(jnp.bfloat16).reshape(chips, -1, width))
    return jnp.sum(parts.astype(jnp.float32), axis=0)


def plain_device(
    hidden_in,
    queries,
    kv_cache,
    new_kv,
    lengths,
    expert_ids,
    value_up,
    out_proj,
    norm_gain,
    router,
    expert_in,
    expert_out,
    shared_in,
    shared_out,
):
    rows_here, steps_here, model_width = hidden_in.shape
    items = rows_here * steps_here
    columns = lax.axis_size("epx")
    depth = lax.axis_size("tp")
    chips = columns * depth
    core = lax.axis_index("core")
    column = lax.axis_index("epx")
    place = lax.axis_index("tp")
    expert_count = router.shape[1]

    latent_out = attend_block(queries, kv_cache, new_kv, lengths)
    by_head = lax.all_to_all(latent_out, ALL, split_axis=2, concat_axis=0, tiled=True)
    head_vals = jnp.einsum(
        "rshl,hlv->rshv", by_head, value_up, preferred_element_type=jnp.float32
    ).astype(jnp.bfloat16)
    partial = jnp.einsum(
        "rshv,hvd->rsd", head_vals, out_proj, preferred_element_type=jnp.float32
    ).reshape(columns, 2, depth * items, model_width)
    kept = lax.dynamic_index_in_dim(partial, core, 1, keepdims=False)
    sent = lax.dynamic_index_in_dim(partial, 1 - core, 1, keepdims=False)
    attention = sum_at_rows(
        kept.reshape(-1, model_width), sent.reshape(-1, model_width), chips
    )
    residual = hidden_in.reshape(items, model_width).astype(jnp.float32) + attention
    mean_square = jnp.mean(residual * residual, axis=-1, keepdims=True)
    normed = (residual * lax.rsqrt(mean_square + norm_eps) * norm_gain.astype(jnp.float32)).astype(
        jnp.bfloat16
    )
    affinity = jax.nn.sigmoid(jnp.dot(normed, router, preferred_element_type=jnp.float32))
    picked = lax.dynamic_slice_in_dim(expert_ids, place * rows_here, rows_here, 0).reshape(
        items, expert_ids.shape[2]
    )
    expert_iota = lax.broadcasted_iota(jnp.int32, (1, 1, expert_count), 2)
    chosen = jnp.sum((picked[:, :, None] == expert_iota).astype(jnp.float32), axis=1)
    scored = chosen * affinity
    gate_weight = route_scale * scored / jnp.sum(scored, axis=-1, keepdims=True)
    gate_high = gate_weight.astype(jnp.bfloat16)
    gate_low = (gate_weight - gate_high.astype(jnp.float32)).astype(jnp.bfloat16)
    spare = -(2 * expert_count) % 128
    payload = jnp.concatenate(
        [normed, gate_high, gate_low, jnp.zeros((items, spare), jnp.bfloat16)], axis=1
    )
    mine = chip_exchange(jnp.broadcast_to(payload[None], (chips,) + payload.shape)).reshape(
        chips * items, -1
    )
    tokens = jnp.concatenate([mine, swap_cores(mine)], axis=0)
    block_items = tokens[:, :model_width]
    expert_here = column * 2 + core
    gate_pairs = tokens[:, model_width : model_width + 2 * expert_count].astype(jnp.float32)
    gates = gate_pairs[:, :expert_count] + gate_pairs[:, expert_count:]
    gate_here = lax.dynamic_slice_in_dim(gates, expert_here, 1, 1)

    gate_part = jnp.dot(block_items, expert_in[0, 0], preferred_element_type=jnp.float32)
    up_part = jnp.dot(block_items, expert_in[0, 1], preferred_element_type=jnp.float32)
    activated = (jax.nn.silu(gate_part) * up_part).astype(jnp.bfloat16)
    routed = gate_here * jnp.dot(activated, expert_out[0], preferred_element_type=jnp.float32)

    own = lax.dynamic_slice_in_dim(mine, column * depth * items, depth * items, 0)[
        :, :model_width
    ]
    shared_gate = jnp.dot(own, shared_in[0], preferred_element_type=jnp.float32)
    shared_up = jnp.dot(own, shared_in[1], preferred_element_type=jnp.float32)
    shared_act = (jax.nn.silu(shared_gate) * shared_up).astype(jnp.bfloat16)
    shared_part = jnp.dot(shared_act, shared_out, preferred_element_type=jnp.float32)

    kept = routed[: chips * items].reshape(columns, depth * items, model_width)
    at_column = lax.broadcasted_iota(jnp.int32, (columns, 1, 1), 0) == column
    kept = kept + jnp.where(at_column, shared_part[None], 0.0)
    expert_sum = sum_at_rows(
        kept.reshape(-1, model_width), routed[chips * items :], chips
    )
    layer_out = (residual + expert_sum).astype(jnp.bfloat16)
    return layer_out.reshape(rows_here, steps_here, model_width)


def on_device(
    hidden_in,
    queries,
    kv_cache,
    new_kv,
    lengths,
    expert_ids,
    value_up,
    out_proj,
    norm_gain,
    router,
    expert_in,
    expert_out,
    shared_in,
    shared_out,
):
    rows_here, steps_here, model_width = hidden_in.shape
    items = rows_here * steps_here
    columns = lax.axis_size("epx")
    depth = lax.axis_size("tp")
    chips = columns * depth
    order = order_of_chips(chips)
    places = [order.index(chip) for chip in range(chips)]
    experts = router.shape[1]

    value_up2 = swap_cores(value_up)
    out_proj2 = swap_cores(out_proj)
    expert_in, expert_out = expert_in[0], expert_out[0]
    latent_out, out_proj, value_up = attend(
        queries, kv_cache, new_kv, lengths, places, depth, [out_proj, value_up]
    )
    by_head = plane_exchange(latent_out, order, depth)
    parts = plane_exchange(
        project(by_head, value_up, value_up2, out_proj, out_proj2), order, depth
    )
    ids = jnp.swapaxes(expert_ids, 1, 2)
    residual, handed = norm_rows(
        ids, parts, hidden_in.reshape(items, model_width), norm_gain, router
    )
    mine = plane_exchange(handed, order, depth)
    other = swap_cores(mine)
    shared = run_shared(mine, shared_in, shared_out, places, depth)
    other, shared = lax.optimization_barrier((other, shared))
    sent, act, gate = run_routed(mine, other, expert_in, expert_out, experts)
    got = swap_cores(sent)
    kept = run_keep(act, gate, expert_out, shared, places)
    parts = plane_exchange(merge(kept, got, chips), order, depth)
    return finish(parts, residual).reshape(rows_here, steps_here, model_width)


def choose(*args):
    owners = 2 * lax.axis_size("epx") * lax.axis_size("tp")
    queries = args[1]
    whole_tiles = queries.shape[0] == 1 and queries.shape[2] % (8 * owners) == 0
    return on_device(*args) if whole_tiles else plain_device(*args)


def solution(mesh):
    sizes = mesh.shape
    fine = Mesh(
        mesh.devices.reshape(sizes["groups"], sizes["ep"] // 2, 2, sizes["tp"]),
        ("groups", "epx", "core", "tp"),
    )
    ep = ("epx", "core")
    rows = ("groups", "epx", "core", "tp")
    in_specs = (
        P(rows, None, None),
        P(rows, None, None, None),
        P(rows, None, None),
        P(rows, None, None),
        P(rows),
        P(("groups",) + ep, None, None),
        P(ALL, None, None),
        P(ALL, None, None),
        P(),
        P(),
        P(ep, None, None, "tp"),
        P(ep, "tp", None),
        P(None, None, "tp"),
        P("tp", None),
    )
    out_specs = P(rows, None, None)
    return jax.shard_map(
        choose, mesh=fine, in_specs=in_specs, out_specs=out_specs, check_vma=False
    )
```

```python
import functools

import jax
import jax.numpy as jnp
import numpy as np
from jax import lax
from jax.experimental import pallas as pl
from jax.experimental.pallas import tpu as pltpu
from jax.sharding import Mesh
from jax.sharding import PartitionSpec as P

LAT = 512


score_scale = 192.0 ** (-0.5)
log2_e = 1.4426950408889634
route_scale = 2.5
norm_eps = 1e-06

CHIPS = ("epx", "tp")
ALL = ("epx", "core", "tp")
VMEM = pl.BlockSpec(memory_space=pltpu.VMEM)
SMEM = pl.BlockSpec(memory_space=pltpu.SMEM)
HBM = pl.BlockSpec(memory_space=pltpu.HBM)


def params(mib):
    return pltpu.CompilerParams(vmem_limit_bytes=mib << 20)


def fetch(stored, held, sems, first):
    copies = [
        pltpu.make_async_copy(a, b, sems.at[first + i])
        for i, (a, b) in enumerate(zip(stored, held))
    ]
    for copy in copies:
        copy.start()
    return copies


def in_hbm(x):
    return pltpu.with_memory_space_constraint(x, pltpu.HBM)


def like(x):
    return jax.ShapeDtypeStruct(x.shape, x.dtype)


def attend_kernel(length_ref, q_hbm, kv_hbm, new_hbm, *refs, chunk, block, depth, places, ahead):
    stored, out_ref, held = refs[:ahead], refs[ahead], refs[ahead + 1 : 2 * ahead + 1]
    new_ref, q_t, q_rows, kv_t, new_rows, scores, weights, row_max, mixed, sems = refs[
        2 * ahead + 1 :
    ]
    steps, width, heads = q_t.shape
    positions = kv_t.shape[1]
    rows = steps * heads
    blocks = rows // block
    per_block = block // heads
    chunks = positions // chunk
    lanes = new_rows.shape[0]
    q_copies = [
        pltpu.make_async_copy(
            q_hbm.at[pl.ds(b * per_block, per_block)],
            q_t.at[pl.ds(b * per_block, per_block)],
            sems.at[b],
        )
        for b in range(blocks)
    ]
    kv_copies = [
        pltpu.make_async_copy(
            kv_hbm.at[:, pl.ds(c * chunk, chunk)],
            kv_t.at[:, pl.ds(c * chunk, chunk)],
            sems.at[blocks + c],
        )
        for c in range(chunks)
    ]
    new_copy = pltpu.make_async_copy(new_hbm, new_ref, sems.at[blocks + chunks])
    q_copies[0].start()
    kv_copies[0].start()
    new_copy.start()
    for copy in q_copies[1:] + kv_copies[1:]:
        copy.start()
    new_rows[...] = jnp.zeros_like(new_rows)
    new_copy.wait()
    new_rows[0:steps, :] = new_ref[...]
    length = length_ref[0]
    rate = score_scale * log2_e
    per_owner = out_ref.shape[1] // (2 * steps)

    def turn(b):
        q_copies[b].wait()
        for i in range(per_block):
            s = b * per_block + i
            q_rows[s * heads : (s + 1) * heads, :] = q_t[s].T

    def score(b, c):
        span = slice(b * block, (b + 1) * block)
        s = jnp.dot(
            q_rows[span, :], kv_t[:, c * chunk : (c + 1) * chunk],
            preferred_element_type=jnp.float32,
        )
        live = (lax.broadcasted_iota(jnp.int32, (1, chunk), 1) + c * chunk) < length
        s = jnp.where(live, s, -1e30)
        scores[span, c * chunk : (c + 1) * chunk] = s
        best = s[:, 0:lanes] if c == 0 else jnp.maximum(row_max[span, :], s[:, 0:lanes])
        for j in range(1, chunk // lanes):
            best = jnp.maximum(best, s[:, j * lanes : (j + 1) * lanes])
        row_max[span, :] = best

    def peak(b):
        span = slice(b * block, (b + 1) * block)
        fresh = lax.dot_general(
            q_rows[span, :], new_rows[...], (((1,), (1,)), ((), ())),
            preferred_element_type=jnp.float32,
        )
        step_of = b * per_block + lax.broadcasted_iota(jnp.int32, (block, lanes), 0) // heads
        fresh = jnp.where(
            lax.broadcasted_iota(jnp.int32, (block, lanes), 1) <= step_of, fresh, -1e30
        )
        top = jnp.max(jnp.maximum(row_max[span, :], fresh), axis=1, keepdims=True) * rate
        fresh = jnp.exp2(fresh * rate - top)
        return [top, fresh, fresh.astype(jnp.bfloat16)]

    def soften(b, c, state):
        span = slice(b * block, (b + 1) * block)
        e = jnp.exp2(scores[span, c * chunk : (c + 1) * chunk] * rate - state[0])
        for j in range(chunk // lanes):
            state[1] = state[1] + e[:, j * lanes : (j + 1) * lanes]
        weights[span, c * chunk : (c + 1) * chunk] = e.astype(jnp.bfloat16)

    def mix(b, first, last, state):
        span = slice(b * block, (b + 1) * block)
        part = lax.dot_general(
            weights[span, first * chunk : last * chunk],
            kv_t[0:LAT, first * chunk : last * chunk],
            (((1,), (1,)), ((), ())),
            preferred_element_type=jnp.float32,
        )
        if first == 0:
            part = part + jnp.dot(
                state[2], new_rows[:, 0:LAT], preferred_element_type=jnp.float32
            )
        else:
            part = part + mixed[...]
        if last < chunks:
            mixed[...] = part
            return
        part = part * (1.0 / jnp.sum(state[1], axis=1, keepdims=True))
        for i in range(per_block):
            s = b * per_block + i
            for d in range(heads // per_owner):
                column, side, t = d // (2 * depth), d // depth % 2, d % depth
                row = (side * steps + s) * per_owner
                first_row = i * heads + d * per_owner
                out_ref[places[column * depth + t], row : row + per_owner, :] = part[
                    first_row : first_row + per_owner, :
                ].astype(jnp.bfloat16)

    states = {}
    fetches = []
    turn(0)
    for stage in range(blocks + 2):
        mixing = stage - 2
        if mixing >= 0 and stage - 1 >= blocks:
            mix(mixing, 0, chunks, states[mixing])
            continue
        for c in range(chunks):
            if stage < blocks:
                if stage == 0:
                    kv_copies[c].wait()
                    if c == 0:
                        fetches = fetch(stored, held, sems, blocks + chunks + 1)
                score(stage, c)
                if c == 0 and stage + 1 < blocks:
                    turn(stage + 1)
            if 0 <= stage - 1 < blocks:
                soften(stage - 1, c, states[stage - 1])
            if mixing >= 0:
                mix(mixing, c, c + 1, states[mixing])
        if stage < blocks:
            states[stage] = peak(stage)
    for copy in fetches:
        copy.wait()


def attend(queries, kv_cache, new_kv, lengths, places, depth, ahead, chunk=1024):
    _, steps, heads, width = queries.shape
    positions = kv_cache.shape[1]
    rows = steps * heads
    lanes = 128
    block = 2 * heads
    chips = len(places)
    return pl.pallas_call(
        functools.partial(
            attend_kernel,
            chunk=chunk,
            block=block,
            depth=depth,
            places=places,
            ahead=len(ahead),
        ),
        out_shape=[jax.ShapeDtypeStruct((chips, rows // chips, LAT), jnp.bfloat16)]
        + [like(x) for x in ahead],
        in_specs=[SMEM] + [HBM] * (3 + len(ahead)),
        out_specs=[VMEM] * (1 + len(ahead)),
        scratch_shapes=[
            pltpu.VMEM((steps, width), jnp.bfloat16),
            pltpu.VMEM((steps, width, heads), jnp.bfloat16),
            pltpu.VMEM((rows, width), jnp.bfloat16),
            pltpu.VMEM((width, positions), jnp.bfloat16),
            pltpu.VMEM((lanes, width), jnp.bfloat16),
            pltpu.VMEM((rows, positions), jnp.float32),
            pltpu.VMEM((rows, positions), jnp.bfloat16),
            pltpu.VMEM((rows, lanes), jnp.float32),
            pltpu.VMEM((block, LAT), jnp.float32),
            pltpu.SemaphoreType.DMA((rows // block + positions // chunk + 1 + len(ahead),)),
        ],
        compiler_params=params(20),
        name="attend",
    )(
        lengths,
        in_hbm(jnp.swapaxes(queries[0], 1, 2)),
        in_hbm(jnp.swapaxes(kv_cache[0], 0, 1)),
        in_hbm(new_kv[0]),
        *[in_hbm(x) for x in ahead],
    )


def project_kernel(latent_ref, up_ref, up2_ref, down_ref, down2_ref, out_ref, latents, *, strip):
    sources, owned, _ = latent_ref.shape
    heads = up_ref.shape[0]
    owned = owned // 2
    steps = owned // heads
    items = sources * steps
    core = lax.axis_index("core")
    blocks = LAT // 128
    vals = []
    for side, w_ref in enumerate((up_ref, up2_ref)):
        start = pl.multiple_of((core if side == 0 else 1 - core) * owned, owned)
        for source in range(sources):
            block = latent_ref[source, pl.ds(start, owned), :].astype(jnp.float32)
            for j in range(blocks):
                latents[side * blocks + j, source * owned : (source + 1) * owned, :] = block[
                    :, j * 128 : (j + 1) * 128
                ]
        for h in range(heads):
            x = jnp.concatenate(
                [
                    latents[side * blocks + j, pl.ds(h, items, stride=heads), :]
                    for j in range(blocks)
                ],
                axis=1,
            ).astype(jnp.bfloat16)
            vals.append(
                jnp.dot(x, w_ref[h], preferred_element_type=jnp.float32).astype(jnp.bfloat16)
            )
    own = jnp.concatenate(vals[:heads], axis=1)
    partner = jnp.concatenate(vals[heads:], axis=1)
    width = down_ref.shape[1]
    for n in range(width // strip):
        cols = slice(n * strip, (n + 1) * strip)
        part = jnp.dot(own, down_ref[:, cols], preferred_element_type=jnp.float32)
        part = part + jnp.dot(partner, down2_ref[:, cols], preferred_element_type=jnp.float32)
        for j in range(sources):
            out_ref[j, :, cols] = part[j * steps : (j + 1) * steps].astype(jnp.bfloat16)


def project(by_head, value_up, value_up2, out_proj, out_proj2):
    sources, owned, _ = by_head.shape
    heads, _, value_width = value_up.shape
    width = out_proj.shape[2]
    flat = (heads * value_width, width)
    return pl.pallas_call(
        functools.partial(project_kernel, strip=512),
        out_shape=jax.ShapeDtypeStruct((sources, owned // (2 * heads), width), jnp.bfloat16),
        in_specs=[VMEM] * 5,
        out_specs=VMEM,
        scratch_shapes=[
            pltpu.VMEM((2 * LAT // 128, sources * owned // 2, 128), jnp.float32),
        ],
        compiler_params=params(8),
        name="project",
    )(by_head, value_up, value_up2, out_proj.reshape(flat), out_proj2.reshape(flat))


def norm_kernel(ids_ref, parts_ref, hidden_ref, gain_ref, router_ref, residual_ref, out_ref):
    chips, items, _ = parts_ref.shape
    width = hidden_ref.shape[1]
    experts = router_ref.shape[0]
    spare = out_ref.shape[2] - width
    place = lax.axis_index("tp")
    total = hidden_ref[...].astype(jnp.float32)
    attention = parts_ref[0].astype(jnp.float32)
    for j in range(1, chips):
        attention = attention + parts_ref[j].astype(jnp.float32)
    residual = total + attention
    residual_ref[...] = residual
    square = jnp.mean(residual * residual, axis=1, keepdims=True)
    normed = (residual * lax.rsqrt(square + norm_eps) * gain_ref[...].astype(jnp.float32).reshape(1, width)).astype(
        jnp.bfloat16
    )
    lane = lax.broadcasted_iota(jnp.int32, (items, experts), 1)
    exact = normed.astype(jnp.float32)
    logits = jnp.zeros((items, experts), jnp.float32)
    for e in range(experts):
        column = router_ref[e : e + 1, :].astype(jnp.float32)
        logits = jnp.where(lane == e, jnp.sum(exact * column, axis=1, keepdims=True), logits)
    affinity = 1.0 / (1.0 + jnp.exp(-logits))
    ids = ids_ref[place]
    own = lax.broadcasted_iota(jnp.int32, (items, items), 0) == lax.broadcasted_iota(
        jnp.int32, (items, items), 1
    )
    chosen = jnp.zeros((items, experts), jnp.float32)
    for k in range(ids.shape[0]):
        named = jnp.sum(jnp.where(own, ids[k : k + 1, :], 0), axis=1, keepdims=True)
        chosen = chosen + (lane == named).astype(jnp.float32)
    scored = chosen * affinity
    gates = route_scale * scored / jnp.sum(scored, axis=1, keepdims=True)
    high = gates.astype(jnp.bfloat16)
    low = (gates - high.astype(jnp.float32)).astype(jnp.bfloat16)
    tail = jnp.concatenate(
        [high.astype(jnp.float32), low.astype(jnp.float32),
         jnp.zeros((items, spare - 2 * experts), jnp.float32)], axis=1
    ).astype(jnp.bfloat16)
    for j in range(chips):
        out_ref[j, :, 0:width] = normed
        out_ref[j, :, width:] = tail


def norm_rows(ids, parts, hidden, gain, router):
    chips, items, width = parts.shape
    experts = router.shape[1]
    spare = -(-2 * experts // 128) * 128
    return pl.pallas_call(
        norm_kernel,
        out_shape=(
            jax.ShapeDtypeStruct((items, width), jnp.float32),
            jax.ShapeDtypeStruct((chips, items, width + spare), jnp.bfloat16),
        ),
        in_specs=[VMEM] * 5,
        out_specs=(VMEM, VMEM),
        compiler_params=params(8),
        name="norm_rows",
    )(ids, parts, hidden, gain, router.T)


def merge_kernel(kept_ref, got_ref, out_ref):
    chips, items, _ = out_ref.shape
    total = kept_ref[...] + got_ref[...].astype(jnp.float32)
    for j in range(chips):
        out_ref[j] = total[j * items : (j + 1) * items, :].astype(jnp.bfloat16)


def merge(kept, got, chips):
    rows, width = kept.shape
    return pl.pallas_call(
        merge_kernel,
        out_shape=jax.ShapeDtypeStruct((chips, rows // chips, width), jnp.bfloat16),
        in_specs=[VMEM, VMEM],
        out_specs=VMEM,
        compiler_params=params(4),
        name="merge",
    )(kept, got)


def silu_gate(g, u):
    return (g / (1.0 + jnp.exp(-g)) * u).astype(jnp.bfloat16)


def gather_rows(ref, first, tokens, tails):
    items = ref.shape[1]
    width = tokens.shape[1]
    for j in range(ref.shape[0]):
        rows = slice(first + j * items, first + (j + 1) * items)
        block = ref[j].astype(jnp.float32)
        tokens[rows, :] = block[:, :width]
        if tails is not None:
            tails[rows, :] = block[:, width:]


def shared_kernel(mine_ref, in_ref, out_w_ref, out_ref, tokens, *, strip, places):
    rows, width = out_ref.shape
    depth = rows // mine_ref.shape[1]
    column = lax.axis_index("epx")
    items = mine_ref.shape[1]
    for t in range(depth):
        place = sum(
            jnp.where(column == x, places[x * depth + t], 0)
            for x in range(len(places) // depth)
        )
        tokens[t * items : (t + 1) * items, :] = mine_ref[place].astype(jnp.float32)[:, :width]
    x = tokens[...].astype(jnp.bfloat16)
    g = jnp.dot(x, in_ref[0], preferred_element_type=jnp.float32)
    u = jnp.dot(x, in_ref[1], preferred_element_type=jnp.float32)
    act = silu_gate(g, u)
    for n in range(width // strip):
        cols = slice(n * strip, (n + 1) * strip)
        out_ref[:, cols] = jnp.dot(act, out_w_ref[:, cols], preferred_element_type=jnp.float32)


def run_shared(mine, shared_in, shared_out, places, depth):
    rows, width = depth * mine.shape[1], shared_out.shape[1]
    return pl.pallas_call(
        functools.partial(shared_kernel, strip=512, places=places),
        out_shape=jax.ShapeDtypeStruct((rows, width), jnp.float32),
        in_specs=[VMEM] * 3,
        out_specs=VMEM,
        scratch_shapes=[pltpu.VMEM((rows, width), jnp.float32)],
        compiler_params=params(6),
        name="shared",
    )(mine, shared_in, shared_out)


def routed_kernel(
    mine_ref, other_ref, in_ref, out_w_ref, sent_ref, act_ref, gate_ref, tokens, tails,
    *, experts, strip,
):
    half, width = sent_ref.shape
    core, column = lax.axis_index("core"), lax.axis_index("epx")
    gather_rows(mine_ref, 0, tokens, tails)
    gather_rows(other_ref, half, tokens, tails)
    x = tokens[...].astype(jnp.bfloat16)
    here = column * 2 + core
    lane = lax.broadcasted_iota(jnp.int32, tails.shape, 1)
    gate = jnp.sum(
        jnp.where((lane == here) | (lane == here + experts), tails[...], 0.0),
        axis=1, keepdims=True,
    )
    g = jnp.dot(x, in_ref[0], preferred_element_type=jnp.float32)
    u = jnp.dot(x, in_ref[1], preferred_element_type=jnp.float32)
    act = silu_gate(g, u)
    act_ref[...] = act[:half]
    gate_ref[...] = jnp.broadcast_to(gate[:half], gate_ref.shape)
    for n in range(width // strip):
        cols = slice(n * strip, (n + 1) * strip)
        y = gate[half:] * jnp.dot(
            act[half:], out_w_ref[:, cols], preferred_element_type=jnp.float32
        )
        sent_ref[:, cols] = y.astype(jnp.bfloat16)


def run_routed(mine, other, expert_in, expert_out, experts):
    chips, items, padded = mine.shape
    hidden, width = expert_out.shape
    half = chips * items
    return pl.pallas_call(
        functools.partial(routed_kernel, experts=experts, strip=512),
        out_shape=(
            jax.ShapeDtypeStruct((half, width), jnp.bfloat16),
            jax.ShapeDtypeStruct((half, hidden), jnp.bfloat16),
            jax.ShapeDtypeStruct((half, 128), jnp.float32),
        ),
        in_specs=[VMEM] * 4,
        out_specs=(VMEM, VMEM, VMEM),
        scratch_shapes=[
            pltpu.VMEM((2 * half, width), jnp.float32),
            pltpu.VMEM((2 * half, padded - width), jnp.float32),
        ],
        compiler_params=params(8),
        name="routed",
    )(mine, other, expert_in, expert_out)


def keep_kernel(act_ref, gate_ref, out_w_ref, shared_ref, kept_ref, *, strip, places):
    width = kept_ref.shape[1]
    rows = shared_ref.shape[0]
    items = kept_ref.shape[0] // len(places)
    depth = rows // items
    column = lax.axis_index("epx")
    gate = gate_ref[:, 0:1]
    for n in range(width // strip):
        cols = slice(n * strip, (n + 1) * strip)
        kept_ref[:, cols] = gate * jnp.dot(
            act_ref[...], out_w_ref[:, cols], preferred_element_type=jnp.float32
        )
    for x in range(len(places) // depth):
        for t in range(depth):
            first = places[x * depth + t] * items
            part = shared_ref[t * items : (t + 1) * items, :]
            kept_ref[first : first + items, :] = kept_ref[first : first + items, :] + jnp.where(
                column == x, part, 0.0
            )


def run_keep(act, gate, expert_out, shared, places):
    return pl.pallas_call(
        functools.partial(keep_kernel, strip=512, places=places),
        out_shape=jax.ShapeDtypeStruct((act.shape[0], expert_out.shape[1]), jnp.float32),
        in_specs=[VMEM] * 4,
        out_specs=VMEM,
        compiler_params=params(6),
        name="keep",
    )(act, gate, expert_out, shared)


def finish_kernel(parts_ref, residual_ref, out_ref):
    total = residual_ref[...]
    for j in range(parts_ref.shape[0]):
        total = total + parts_ref[j].astype(jnp.float32)
    out_ref[...] = total.astype(jnp.bfloat16)


def finish(parts, residual):
    return pl.pallas_call(
        finish_kernel,
        out_shape=jax.ShapeDtypeStruct(residual.shape, jnp.bfloat16),
        in_specs=[VMEM, VMEM],
        out_specs=VMEM,
        compiler_params=params(8),
        name="finish",
    )(parts, residual)


def swap_cores(x):
    return lax.ppermute(x, "core", [(0, 1), (1, 0)])


def chip_exchange(x):
    return lax.all_to_all(x, CHIPS, split_axis=0, concat_axis=0, tiled=True)


def order_of_chips(chips):
    return [int(chip) for chip in np.random.RandomState(98737).permutation(chips)]


def plane_exchange(x, order, depth):
    groups = [
        [(chip // depth * 2 + core) * depth + chip % depth for chip in order] for core in range(2)
    ]
    return lax.all_to_all(
        x, ALL, split_axis=0, concat_axis=0, axis_index_groups=groups, tiled=True
    )


def attend_block(queries, kv_cache, new_kv, lengths):
    rows_here, steps_here, heads_here, kv_width = queries.shape
    positions = kv_cache.shape[1]
    cached = (
        jnp.einsum("rshk,rck->rshc", queries, kv_cache, preferred_element_type=jnp.float32)
        * score_scale
    )
    recent = (
        jnp.einsum("rshk,rjk->rshj", queries, new_kv, preferred_element_type=jnp.float32)
        * score_scale
    )
    cache_live = lax.broadcasted_iota(jnp.int32, (rows_here, positions), 1) < lengths[:, None]
    causal = lax.broadcasted_iota(jnp.int32, (steps_here, steps_here), 1) <= lax.broadcasted_iota(
        jnp.int32, (steps_here, steps_here), 0
    )
    cached = jnp.where(cache_live[:, None, None, :], cached, -1e30)
    recent = jnp.where(causal[None, :, None, :], recent, -1e30)
    highest = jnp.maximum(cached.max(-1), recent.max(-1))[..., None]
    cached_exp = jnp.exp(cached - highest)
    recent_exp = jnp.exp(recent - highest)
    denominator = cached_exp.sum(-1, keepdims=True) + recent_exp.sum(-1, keepdims=True)
    cached_prob = (cached_exp / denominator).astype(jnp.bfloat16)
    recent_prob = (recent_exp / denominator).astype(jnp.bfloat16)
    combined = jnp.einsum(
        "rshc,rck->rshk", cached_prob, kv_cache, preferred_element_type=jnp.float32
    )
    combined = combined + jnp.einsum(
        "rshj,rjk->rshk", recent_prob, new_kv, preferred_element_type=jnp.float32
    )
    return combined[..., :LAT].astype(jnp.bfloat16)


def sum_at_rows(kept, sent, chips):
    half = kept + swap_cores(sent.astype(jnp.bfloat16)).astype(jnp.float32)
    width = half.shape[1]
    parts = chip_exchange(half.astype(jnp.bfloat16).reshape(chips, -1, width))
    return jnp.sum(parts.astype(jnp.float32), axis=0)


def plain_device(
    hidden_in,
    queries,
    kv_cache,
    new_kv,
    lengths,
    expert_ids,
    value_up,
    out_proj,
    norm_gain,
    router,
    expert_in,
    expert_out,
    shared_in,
    shared_out,
):
    rows_here, steps_here, model_width = hidden_in.shape
    items = rows_here * steps_here
    columns = lax.axis_size("epx")
    depth = lax.axis_size("tp")
    chips = columns * depth
    core = lax.axis_index("core")
    column = lax.axis_index("epx")
    place = lax.axis_index("tp")
    expert_count = router.shape[1]

    latent_out = attend_block(queries, kv_cache, new_kv, lengths)
    by_head = lax.all_to_all(latent_out, ALL, split_axis=2, concat_axis=0, tiled=True)
    head_vals = jnp.einsum(
        "rshl,hlv->rshv", by_head, value_up, preferred_element_type=jnp.float32
    ).astype(jnp.bfloat16)
    partial = jnp.einsum(
        "rshv,hvd->rsd", head_vals, out_proj, preferred_element_type=jnp.float32
    ).reshape(columns, 2, depth * items, model_width)
    kept = lax.dynamic_index_in_dim(partial, core, 1, keepdims=False)
    sent = lax.dynamic_index_in_dim(partial, 1 - core, 1, keepdims=False)
    attention = sum_at_rows(
        kept.reshape(-1, model_width), sent.reshape(-1, model_width), chips
    )
    residual = hidden_in.reshape(items, model_width).astype(jnp.float32) + attention
    mean_square = jnp.mean(residual * residual, axis=-1, keepdims=True)
    normed = (residual * lax.rsqrt(mean_square + norm_eps) * norm_gain.astype(jnp.float32)).astype(
        jnp.bfloat16
    )
    affinity = jax.nn.sigmoid(jnp.dot(normed, router, preferred_element_type=jnp.float32))
    picked = lax.dynamic_slice_in_dim(expert_ids, place * rows_here, rows_here, 0).reshape(
        items, expert_ids.shape[2]
    )
    expert_iota = lax.broadcasted_iota(jnp.int32, (1, 1, expert_count), 2)
    chosen = jnp.sum((picked[:, :, None] == expert_iota).astype(jnp.float32), axis=1)
    scored = chosen * affinity
    gate_weight = route_scale * scored / jnp.sum(scored, axis=-1, keepdims=True)
    gate_high = gate_weight.astype(jnp.bfloat16)
    gate_low = (gate_weight - gate_high.astype(jnp.float32)).astype(jnp.bfloat16)
    spare = -(2 * expert_count) % 128
    payload = jnp.concatenate(
        [normed, gate_high, gate_low, jnp.zeros((items, spare), jnp.bfloat16)], axis=1
    )
    mine = chip_exchange(jnp.broadcast_to(payload[None], (chips,) + payload.shape)).reshape(
        chips * items, -1
    )
    tokens = jnp.concatenate([mine, swap_cores(mine)], axis=0)
    block_items = tokens[:, :model_width]
    expert_here = column * 2 + core
    gate_pairs = tokens[:, model_width : model_width + 2 * expert_count].astype(jnp.float32)
    gates = gate_pairs[:, :expert_count] + gate_pairs[:, expert_count:]
    gate_here = lax.dynamic_slice_in_dim(gates, expert_here, 1, 1)

    gate_part = jnp.dot(block_items, expert_in[0, 0], preferred_element_type=jnp.float32)
    up_part = jnp.dot(block_items, expert_in[0, 1], preferred_element_type=jnp.float32)
    activated = (jax.nn.silu(gate_part) * up_part).astype(jnp.bfloat16)
    routed = gate_here * jnp.dot(activated, expert_out[0], preferred_element_type=jnp.float32)

    own = lax.dynamic_slice_in_dim(mine, column * depth * items, depth * items, 0)[
        :, :model_width
    ]
    shared_gate = jnp.dot(own, shared_in[0], preferred_element_type=jnp.float32)
    shared_up = jnp.dot(own, shared_in[1], preferred_element_type=jnp.float32)
    shared_act = (jax.nn.silu(shared_gate) * shared_up).astype(jnp.bfloat16)
    shared_part = jnp.dot(shared_act, shared_out, preferred_element_type=jnp.float32)

    kept = routed[: chips * items].reshape(columns, depth * items, model_width)
    at_column = lax.broadcasted_iota(jnp.int32, (columns, 1, 1), 0) == column
    kept = kept + jnp.where(at_column, shared_part[None], 0.0)
    expert_sum = sum_at_rows(
        kept.reshape(-1, model_width), routed[chips * items :], chips
    )
    layer_out = (residual + expert_sum).astype(jnp.bfloat16)
    return layer_out.reshape(rows_here, steps_here, model_width)


def on_device(
    hidden_in,
    queries,
    kv_cache,
    new_kv,
    lengths,
    expert_ids,
    value_up,
    out_proj,
    norm_gain,
    router,
    expert_in,
    expert_out,
    shared_in,
    shared_out,
):
    rows_here, steps_here, model_width = hidden_in.shape
    items = rows_here * steps_here
    columns = lax.axis_size("epx")
    depth = lax.axis_size("tp")
    chips = columns * depth
    order = order_of_chips(chips)
    places = [order.index(chip) for chip in range(chips)]
    experts = router.shape[1]

    value_up2 = swap_cores(value_up)
    out_proj2 = swap_cores(out_proj)
    expert_in, expert_out = expert_in[0], expert_out[0]
    latent_out, out_proj, value_up = attend(
        queries, kv_cache, new_kv, lengths, places, depth, [out_proj, value_up]
    )
    by_head = plane_exchange(latent_out, order, depth)
    parts = plane_exchange(
        project(by_head, value_up, value_up2, out_proj, out_proj2), order, depth
    )
    ids = jnp.swapaxes(expert_ids, 1, 2)
    residual, handed = norm_rows(
        ids, parts, hidden_in.reshape(items, model_width), norm_gain, router
    )
    mine = plane_exchange(handed, order, depth)
    other = swap_cores(mine)
    shared = run_shared(mine, shared_in, shared_out, places, depth)
    other, shared = lax.optimization_barrier((other, shared))
    sent, act, gate = run_routed(mine, other, expert_in, expert_out, experts)
    got = swap_cores(sent)
    kept = run_keep(act, gate, expert_out, shared, places)
    parts = plane_exchange(merge(kept, got, chips), order, depth)
    return finish(parts, residual).reshape(rows_here, steps_here, model_width)


def choose(*args):
    owners = 2 * lax.axis_size("epx") * lax.axis_size("tp")
    queries = args[1]
    whole_tiles = queries.shape[0] == 1 and queries.shape[2] % (8 * owners) == 0
    return on_device(*args) if whole_tiles else plain_device(*args)


def solution(mesh):
    sizes = mesh.shape
    fine = Mesh(
        mesh.devices.reshape(sizes["groups"], sizes["ep"] // 2, 2, sizes["tp"]),
        ("groups", "epx", "core", "tp"),
    )
    ep = ("epx", "core")
    rows = ("groups", "epx", "core", "tp")
    in_specs = (
        P(rows, None, None),
        P(rows, None, None, None),
        P(rows, None, None),
        P(rows, None, None),
        P(rows),
        P(("groups",) + ep, None, None),
        P(ALL, None, None),
        P(ALL, None, None),
        P(),
        P(),
        P(ep, None, None, "tp"),
        P(ep, "tp", None),
        P(None, None, "tp"),
        P("tp", None),
    )
    out_specs = P(rows, None, None)
    return jax.shard_map(
        choose, mesh=fine, in_specs=in_specs, out_specs=out_specs, check_vma=False
    )
```
